128 devices in a mesh: row: 16 (over y_hi, z, core), col: 8 (over y_lo, x).
Axes of the slice: x: 4, y: 4 (y_hi: 2, y_lo: 2; y = y_hi * 2 + y_lo), z: 4, core: 2. Of those that a mesh axis runs over, the one named last changes fastest.
Arguments:
- pair: bfloat16 [1024, 1024, 128], P('row', 'col'), may hold values from -6 to 6
- relpos: bfloat16 [128, 128], replicated, may hold values from -4 to 4
- pair_gain: float32 [128], replicated, may hold values from 0.1 to 1.9
- bias_weight: bfloat16 [128, 12], replicated, may hold values from -0.5 to 0.5
- single: float32 [1024, 384], P(('row', 'col')), may hold values from -6 to 6
- rotation_params: float32 [3, 1024], P(None, ('row', 'col')), may hold values from -4 to 4
- translation: float32 [3, 1024], P(None, ('row', 'col')), may hold values from -9 to 9
- residue_index: int32 [1024], P(('row', 'col')), may hold values from 0 to 203776, as said below
- residue_mask: int32 [1024], P(('row', 'col')), may hold values 0 or 1
- w_scalar: float32 [384, 576], replicated, may hold values from -0.3125 to 0.3125
- w_points: float32 [384, 576], replicated, may hold values from -0.3125 to 0.3125
- head_weights: float32 [12], replicated, may hold values from -2 to 1.5
- w_out: float32 [2112, 384], replicated, may hold values from -0.125 to 0.125
- w_hidden: float32 [384, 384], replicated, may hold values from -0.3125 to 0.3125
- w_back: float32 [384, 384], replicated, may hold values from -0.3125 to 0.3125
- w_frame: float32 [384, 6], replicated, may hold values from -0.078125 to 0.078125
Outputs:
- single_out: float32 [1024, 384], P(('row', 'col'))
- frames: float32 [12, 1024], P(None, ('row', 'col'))
The draws below stay inside these ranges and needn't reach their ends.
Inputs may be any that keep to these rules, and one draw needn't show every extreme that they name: residue_index is strictly increasing along the crop, begins at 0 and ends at exactly 203776.
All inputs are finite; a program needn't handle non-finite values. No bound on the sum of `residue_mask` on one device may be relied on, other than what follows from the above.
Results may differ from the reference program's by a relative error of at most 0.0025.
Values may be sent and summed in bfloat16 or wider, within the bound.
A program may use at most 64 MiB of HBM per device.

```python
import math
import jax
import jax.numpy as jnp
from jax import lax

D = 384
CZ = 128
H = 12
C = 16
PQ = 4
PV = 8
BINS = 128
ITERS = 3
N = 1024
OUT_F = 2112


def draw_residue_index(key, part):
    key_step, key_break, key_jump = jax.random.split(jax.random.fold_in(key, 17), 3)
    steps = jax.random.randint(key_step, (N,), 1, 3)
    breaks = jax.random.randint(key_break, (N,), 0, 64) == 0
    jumps = jax.random.randint(key_jump, (N,), 50, 200)
    steps = jnp.where(breaks, jumps, steps)
    numbers = (jnp.cumsum(steps) - steps[0]).astype(jnp.int32)
    position = jnp.arange(N, dtype=jnp.int32)
    return jnp.where(position == N - 1, jnp.int32(199 * N), numbers).astype(jnp.int32)


def plant(values, key, least, top_value):
    index_at = [jax.random.randint(jax.random.fold_in(key, axis), (), 0, length) for axis, length in enumerate(values.shape)]
    main_axis = values.shape.index(max(values.shape))
    next_to = index_at[:main_axis] + [(index_at[main_axis] + 1) % values.shape[main_axis]] + index_at[main_axis + 1:]
    return values.at[tuple(index_at)].set(least).at[tuple(next_to)].set(top_value)


def block_scale(stream_key, dims, pieces, least, high):
    loudness, own = 1.0, jax.random.fold_in(stream_key, 6)
    for axis_at, blocks in pieces:
        heights = jnp.exp(jax.random.uniform(jax.random.fold_in(own, axis_at), (blocks,), jnp.float32, least / len(pieces), high / len(pieces)))
        loudness = loudness * jnp.repeat(heights, dims[axis_at] // blocks).reshape([-1 if axis == axis_at else 1 for axis in range(len(dims))])
    return loudness


def bell_draw(own_key, shape, scale, most, pieces=(), kind=jnp.bfloat16):
    values = jax.random.normal(own_key, shape, jnp.float32) * scale
    if len(pieces) > 0:
        values = block_scale(own_key, shape, pieces, -0.22, 0.18) * values
    return jnp.clip(values, min=-most, max=most).astype(kind)


def setup_inputs(seed: int = 0) -> dict:
    key_of = jax.random.split(jax.random.key(seed), 17)
    pair = bell_draw(key_of[0], (N, N, CZ), 1.0, 6.0, ((0, 16), (1, 8)))
    relpos = bell_draw(key_of[1], (BINS, CZ), 0.7, 4.0)
    pair_gain = jnp.clip(1.0 + 0.18 * jax.random.normal(key_of[2], (CZ,), jnp.float32), 0.1, 1.9)
    bias_weight = bell_draw(key_of[3], (CZ, H), CZ ** -0.5, 0.5)
    single = bell_draw(key_of[4], (N, D), 1.0, 6.0, ((0, 128),), jnp.float32)
    rotation_params = bell_draw(key_of[5], (3, N), 0.7, 4.0, ((1, 128),), jnp.float32)
    translation = bell_draw(key_of[6], (3, N), 1.5, 9.0, ((1, 128),), jnp.float32)
    residue_index = draw_residue_index(jax.random.fold_in(key_of[16], 71), 0)
    residue_mask = plant((jax.random.randint(key_of[8], (N,), 0, 8) < 7).astype(jnp.int32), jax.random.fold_in(key_of[8], 1), 0, 1)
    w_scalar = bell_draw(key_of[9], (D, 3 * H * C), D ** -0.5, 0.3125, (), jnp.float32)
    w_points = bell_draw(key_of[10], (D, 3 * H * (2 * PQ + PV)), D ** -0.5, 0.3125, (), jnp.float32)
    head_weights = jnp.clip(jax.random.uniform(key_of[11], (H,), jnp.float32, -2.0, 1.5), -2.0, 1.5)
    w_out = bell_draw(key_of[12], (OUT_F, D), OUT_F ** -0.5, 0.125, (), jnp.float32)
    w_hidden = bell_draw(key_of[13], (D, D), D ** -0.5, 0.3125, (), jnp.float32)
    w_back = bell_draw(key_of[14], (D, D), D ** -0.5, 0.3125, (), jnp.float32)
    w_frame = bell_draw(key_of[15], (D, 6), (16 * D) ** -0.5, 0.078125, (), jnp.float32)
    return dict(pair=pair, relpos=relpos, pair_gain=pair_gain, bias_weight=bias_weight, single=single, rotation_params=rotation_params, translation=translation, residue_index=residue_index, residue_mask=residue_mask, w_scalar=w_scalar, w_points=w_points, head_weights=head_weights, w_out=w_out, w_hidden=w_hidden, w_back=w_back, w_frame=w_frame)


NORM_EPSILON = 1e-05
MASKED_LOGIT = -100000.0
NORM_FLOOR = 0.1
HIGHEST_PRECISION = lax.Precision.HIGHEST

def layer_norm(values):
    center = values - lax.optimization_barrier(jnp.mean(values, axis=-1, keepdims=True))
    spread = lax.optimization_barrier(jnp.mean(center * center, axis=-1, keepdims=True))
    return center * lax.rsqrt(spread + NORM_EPSILON)

def rotation_from(update):
    quat_b, quat_c, quat_d = (update[0], update[1], update[2])
    inverse = 1.0 / (1.0 + quat_b * quat_b + quat_c * quat_c + quat_d * quat_d)
    entries = [1.0 + quat_b * quat_b - quat_c * quat_c - quat_d * quat_d, 2.0 * (quat_b * quat_c - quat_d), 2.0 * (quat_b * quat_d + quat_c), 2.0 * (quat_b * quat_c + quat_d), 1.0 - quat_b * quat_b + quat_c * quat_c - quat_d * quat_d, 2.0 * (quat_c * quat_d - quat_b), 2.0 * (quat_b * quat_d - quat_c), 2.0 * (quat_c * quat_d + quat_b), 1.0 - quat_b * quat_b - quat_c * quat_c + quat_d * quat_d]
    return jnp.stack(entries) * inverse

def to_global(rotation, points, translation):
    return jnp.stack([rotation[3 * component] * points[0] + rotation[3 * component + 1] * points[1] + rotation[3 * component + 2] * points[2] + translation[component] for component in range(3)])

def to_local(rotation, points, translation):
    moved = [points[component] - translation[component] for component in range(3)]
    return jnp.stack([rotation[component] * moved[0] + rotation[3 + component] * moved[1] + rotation[6 + component] * moved[2] for component in range(3)])

def compose(rotation, translation, update):
    turn = rotation_from(update[:3])
    new_rotation = jnp.stack([rotation[3 * left] * turn[right] + rotation[3 * left + 1] * turn[3 + right] + rotation[3 * left + 2] * turn[6 + right] for left in range(3) for right in range(3)])
    new_translation = jnp.stack([rotation[3 * left] * update[3] + rotation[3 * left + 1] * update[4] + rotation[3 * left + 2] * update[5] + translation[left] for left in range(3)])
    return (new_rotation, new_translation)

def project(single, rotation, translation, w_scalar, w_points):
    count = single.shape[0]
    scalars = jnp.dot(single, w_scalar, precision=HIGHEST_PRECISION, preferred_element_type=jnp.float32).T
    scalars = scalars.reshape(3, H * C, count).astype(jnp.bfloat16)
    points = jnp.dot(single, w_points, precision=HIGHEST_PRECISION, preferred_element_type=jnp.float32).T
    query_local = points[:3 * H * PQ].reshape(3, H * PQ, count)
    key_local = points[3 * H * PQ:6 * H * PQ].reshape(3, H * PQ, count)
    value_local = points[6 * H * PQ:].reshape(3, H * PV, count)
    return (scalars, to_global(rotation, query_local, translation), to_global(rotation, key_local, translation), to_global(rotation, value_local, translation))

def advance(single, rotation, translation, scalar_out, point_out, pair_out, w_out, w_hidden, w_back, w_frame):
    count = single.shape[0]
    local = to_local(rotation, point_out, translation)
    lengths = jnp.sqrt(lax.optimization_barrier(jnp.sum(local * local, axis=0)) + NORM_FLOOR)
    features = jnp.concatenate([scalar_out, local.reshape(3 * H * PV, count), lengths, pair_out], axis=0)
    single = layer_norm(single + jnp.dot(features.T, w_out, precision=HIGHEST_PRECISION, preferred_element_type=jnp.float32))
    hidden = jax.nn.relu(jnp.dot(single, w_hidden, precision=HIGHEST_PRECISION, preferred_element_type=jnp.float32))
    single = layer_norm(single + jnp.dot(hidden, w_back, precision=HIGHEST_PRECISION, preferred_element_type=jnp.float32))
    update = jnp.dot(single, w_frame, precision=HIGHEST_PRECISION, preferred_element_type=jnp.float32).T
    rotation, translation = compose(rotation, translation, update)
    return (single, rotation, translation)

def reference(pair, relpos, pair_gain, bias_weight, single, rotation_params, translation, residue_index, residue_mask, w_scalar, w_points, head_weights, w_out, w_hidden, w_back, w_frame):
    span_rows = math.gcd(N, 128)
    count = N // span_rows
    live = residue_mask == 1
    table = relpos.astype(jnp.float32)
    point_scale = jax.nn.softplus(head_weights) * (math.sqrt(2.0 / (9.0 * PQ)) / 2.0)

    def prepare(index):
        start = index * span_rows
        rows = lax.dynamic_slice_in_dim(pair, start, span_rows, 0).astype(jnp.float32)
        near = lax.dynamic_slice_in_dim(residue_index, start, span_rows, 0)
        offset = jnp.clip(residue_index[None, :] - near[:, None], -(BINS // 2), BINS // 2 - 1) + BINS // 2
        normed = (layer_norm(rows + table[offset]) * pair_gain).astype(jnp.bfloat16)
        bias = jnp.einsum('ijc,ch->hij', normed.astype(jnp.float32), bias_weight.astype(jnp.float32), precision=HIGHEST_PRECISION)
        return (normed, bias)
    rotation = rotation_from(rotation_params)
    state = single
    for step in range(ITERS):
        scalars, query_points, key_points, value_points = project(state, rotation, translation, w_scalar, w_points)
        query = scalars[0].reshape(H, C, N)
        keys = scalars[1].reshape(H, C, N).astype(jnp.float32)
        values = scalars[2].reshape(H, C, N).astype(jnp.float32)
        query_grid = query_points.reshape(3, H, PQ, N)
        key_grid = key_points.reshape(3, H, PQ, N)
        value_grid = value_points.reshape(3, H, PV, N)
        key_square = lax.optimization_barrier(jnp.sum(key_grid * key_grid, axis=(0, 2)))

        def attend(index):
            normed, bias = prepare(index)
            start = index * span_rows
            query_block = lax.dynamic_slice_in_dim(query, start, span_rows, 2).astype(jnp.float32)
            query_block_points = lax.dynamic_slice_in_dim(query_grid, start, span_rows, 3)
            scores = jnp.einsum('hci,hcj->hij', query_block, keys, precision=HIGHEST_PRECISION) / math.sqrt(C)
            cross = jnp.einsum('ahpi,ahpj->hij', query_block_points, key_grid, precision=HIGHEST_PRECISION)
            distance = lax.optimization_barrier(jnp.sum(query_block_points * query_block_points, axis=(0, 2)))[:, :, None] + key_square[:, None, :] - 2.0 * cross
            logits = math.sqrt(1.0 / 3.0) * (scores + bias - point_scale[:, None, None] * distance)
            live_block = lax.dynamic_slice_in_dim(live, start, span_rows, 0)
            logits = jnp.where(live_block[None, :, None] & live[None, None, :], logits, MASKED_LOGIT)
            weights = jax.nn.softmax(logits, axis=-1)
            rounded = lax.optimization_barrier(weights.astype(jnp.bfloat16)).astype(jnp.float32)
            scalar_part = jnp.einsum('hij,hcj->hci', rounded, values, precision=HIGHEST_PRECISION)
            point_part = jnp.einsum('hij,ahpj->ahpi', weights, value_grid, precision=HIGHEST_PRECISION)
            pair_part = jnp.einsum('hij,ijc->hci', rounded, normed.astype(jnp.float32), precision=HIGHEST_PRECISION)
            return (scalar_part.reshape(H * C, span_rows), point_part.reshape(3 * H * PV, span_rows), pair_part.reshape(H * CZ, span_rows))
        scalar_part, point_part, pair_part = lax.map(attend, jnp.arange(count, dtype=jnp.int32))
        scalar_out = scalar_part.transpose(1, 0, 2).reshape(H * C, N)
        point_out = point_part.transpose(1, 0, 2).reshape(3, H * PV, N)
        pair_out = pair_part.transpose(1, 0, 2).reshape(H * CZ, N)
        state, rotation, translation = advance(state, rotation, translation, scalar_out, point_out, pair_out, w_out, w_hidden, w_back, w_frame)
    frames = jnp.concatenate([rotation, translation], axis=0)
    return (state, frames)
```

```python
import functools
import math

import jax
import jax.numpy as jnp
import numpy as np
from jax import lax
from jax.experimental import pallas as pl
from jax.experimental.pallas import tpu as pltpu
from jax.sharding import PartitionSpec as P

H = 12
C = 16
PQ = 4
PV = 8
BINS = 128
ITERS = 3
D = 384
HP = 16
ROWS = 64
COLS = 128
OWN = 8
NR = 16
NC = 8
SW = 512
RW = 768
QW = 640
FW = 1024
MIXW = 1792

NORM_EPSILON = 1e-05
MASKED_LOGIT = -100000.0
DEAD = -3e38
NORM_FLOOR = 0.1
THIRD = math.sqrt(1.0 / 3.0)
MESH = pl.DeviceIdType.MESH
F32 = jnp.float32
BF16 = jnp.bfloat16


def rotation_entries(b, c, d):
    inverse = 1.0 / (1.0 + b * b + c * c + d * d)
    entries = [
        1.0 + b * b - c * c - d * d,
        2.0 * (b * c - d),
        2.0 * (b * d + c),
        2.0 * (b * c + d),
        1.0 - b * b + c * c - d * d,
        2.0 * (c * d - b),
        2.0 * (b * d - c),
        2.0 * (c * d + b),
        1.0 - b * b - c * c + d * d,
    ]
    return [e * inverse for e in entries]


def layer_norm(values):
    center = values - jnp.mean(values, axis=-1, keepdims=True)
    spread = jnp.mean(center * center, axis=-1, keepdims=True)
    return center * lax.rsqrt(spread + NORM_EPSILON)


def column_maps():
    lane = np.arange(128)

    def scalars(at):
        f = np.arange(256)
        return np.where(f < H * C, at * H * C + f, -1)

    def points(base):
        comps = []
        for a in range(3):
            comps.append(np.where(lane < 96, base + a * H * PQ + lane % 48, -1))
        return np.concatenate(comps)

    values = np.concatenate(
        [np.where(lane < 96, 6 * H * PQ + a * H * PV + lane, -1) for a in range(3)]
    )
    scal = np.concatenate([scalars(0), scalars(1), scalars(2)])
    pts = np.concatenate([points(0), points(3 * H * PQ), values])
    return scal.reshape(1, -1).astype(np.int32), pts.reshape(1, -1).astype(np.int32)


def head_mask():
    f = np.arange(FW)
    lane = f % 128
    head = np.where(f < 256, f // C, np.where(lane < 96, (lane % 48) // PQ, lane - 96))
    ok = np.where(f < 256, f < H * C, lane < 96 + H)
    rows = np.arange(HP)[:, None]
    return ((rows == head[None]) & ok[None]).astype(np.float32)


def split2(x):
    hi = x.astype(BF16)
    return hi, (x - hi.astype(F32)).astype(BF16)


def mm(a, b):
    return jnp.dot(a, b, preferred_element_type=F32)


def dot3(x, w_hi, w_mid):
    hi, mid = split2(x)
    n = x.shape[0]
    both = mm(jnp.concatenate([hi, mid], axis=0), w_hi)
    return both[:n] + both[n:] + mm(hi, w_mid)


def lane_iota(rows):
    return lax.broadcasted_iota(jnp.int32, (rows, 128), 1)


def column(x, k):
    return jnp.broadcast_to(x[:, k : k + 1], (x.shape[0], 128))


def kernel(
    state0, pair_hbm, relpos, gain, wb_t, gamma, hmask, smap, pmap,
    wsc_hbm, wpt_hbm, wout_hbm, whid_hbm, wback_hbm, wframe,
    single_out, frames_out,
    pair_v, bias_v, wsc_f, wpt_f, wout_f, whid_f, wback_f,
    wp_hi, wp_mid, wmix_hi, wmix_mid, wloc_hi, wloc_mid, whid_hi, whid_mid, wback_hi, wback_mid,
    wfr_hi, wfr_mid,
    send_buf, row_recv, swap_recv, col_recv, sync_send, sync_recv, red_send, red_recv,
    qf, qmask, kf, vcat, idx_b, p_s, m_b, s_b, r_s, pair_s,
    copy_sem, row_ss, row_rs, swap_ss, swap_rs, col_ss, col_rs, sync_ss, sync_rs, red_ss, red_rs,
):
    r = lax.axis_index("row")
    c = lax.axis_index("col")
    swap_row = 2 * c + lax.rem(r, 2)
    swap_col = r // 2
    alone = swap_col == c
    slot = lax.rem(r, 2) * 8 + r // 2

    copies = [
        pltpu.make_async_copy(src, dst, copy_sem.at[k])
        for k, (src, dst) in enumerate(
            [
                (wsc_hbm, wsc_f),
                (wpt_hbm, wpt_f),
                (pair_hbm, pair_v),
                (wout_hbm, wout_f),
                (whid_hbm, whid_f),
                (wback_hbm, wback_f),
            ]
        )
    ]
    for cp in copies:
        cp.start()

    barrier = pltpu.get_barrier_semaphore()
    for d in range(1, NC):
        pl.semaphore_signal(
            barrier, inc=1, device_id=(r, lax.rem(c + d, NC)), device_id_type=MESH
        )
    for d in range(1, NR):
        pl.semaphore_signal(
            barrier, inc=1, device_id=(lax.rem(r + d, NR), c), device_id_type=MESH
        )

    @pl.when(jnp.logical_not(alone))
    def _():
        pl.semaphore_signal(barrier, inc=1, device_id=(swap_row, swap_col), device_id_type=MESH)
        pl.semaphore_wait(barrier, NC + NR - 1)

    @pl.when(alone)
    def _():
        pl.semaphore_wait(barrier, NC + NR - 2)

    send_buf[0] = state0[...]

    def row_copy(it, peer, at):
        return pltpu.make_async_remote_copy(
            src_ref=send_buf.at[it],
            dst_ref=row_recv.at[it, at],
            send_sem=row_ss.at[peer],
            recv_sem=row_rs.at[it, at],
            device_id=(r, peer),
            device_id_type=MESH,
        )

    def swap_copy(it):
        return pltpu.make_async_remote_copy(
            src_ref=send_buf.at[it],
            dst_ref=swap_recv.at[it],
            send_sem=swap_ss,
            recv_sem=swap_rs.at[it],
            device_id=(swap_row, swap_col),
            device_id_type=MESH,
        )

    def col_copy(it, peer, at):
        return pltpu.make_async_remote_copy(
            src_ref=swap_recv.at[it],
            dst_ref=col_recv.at[it, at],
            send_sem=col_ss.at[peer],
            recv_sem=col_rs.at[it, at],
            device_id=(peer, c),
            device_id_type=MESH,
        )

    def sync_copy(it, peer, at):
        return pltpu.make_async_remote_copy(
            src_ref=sync_send.at[it],
            dst_ref=sync_recv.at[it, at],
            send_sem=sync_ss.at[peer],
            recv_sem=sync_rs.at[it, at],
            device_id=(r, peer),
            device_id_type=MESH,
        )

    def red_copy(it, peer, at):
        return pltpu.make_async_remote_copy(
            src_ref=red_send.at[it, peer],
            dst_ref=red_recv.at[it, at],
            send_sem=red_ss.at[peer],
            recv_sem=red_rs.at[it, at],
            device_id=(r, peer),
            device_id_type=MESH,
        )

    def start_exchange(it):
        @pl.when(jnp.logical_not(alone))
        def _():
            swap_copy(it).start()

        for d in range(1, NC):
            row_copy(it, lax.rem(c + d, NC), c).start()
        row_recv[it, c] = send_buf[it]

    def prepare_weights():
        for cp in copies[:2]:
            cp.wait()
        for w_f, m_ref, widths, starts in (
            (wsc_f, smap, (256, 256, 256), (0, QW, 2 * QW)),
            (wpt_f, pmap, (384, 384, 384), (256, QW + 256, 2 * QW + 256)),
        ):
            hi, mid = split2(w_f[...])
            at = 0
            for width, start in zip(widths, starts):
                pick = (
                    lax.broadcasted_iota(jnp.int32, (w_f.shape[1], width), 0)
                    == m_ref[:, at : at + width]
                )
                pick = jnp.where(pick, 1.0, 0.0).astype(BF16)
                wp_hi[:, start : start + width] = mm(hi, pick).astype(BF16)
                wp_mid[:, start : start + width] = mm(mid, pick).astype(BF16)
                at += width
        for cp in copies[3:]:
            cp.wait()
        zeros64 = jnp.zeros((64, D), BF16)
        zeros32 = jnp.zeros((32, D), BF16)
        for part, (dst_mix, dst_loc) in enumerate(((wmix_hi, wloc_hi), (wmix_mid, wloc_mid))):
            dst_mix[0:192] = split2(wout_f[0:192])[part]
            dst_mix[192:256] = zeros64
            for k in range(4):
                dst_mix[256 + 384 * k : 640 + 384 * k] = split2(
                    wout_f[576 + 384 * k : 960 + 384 * k]
                )[part]
            for k in range(4):
                dst_loc[128 * k : 128 * k + 96] = split2(wout_f[192 + 96 * k : 288 + 96 * k])[part]
                dst_loc[128 * k + 96 : 128 * k + 128] = zeros32
        whid_hi[...], whid_mid[...] = split2(whid_f[...])
        wback_hi[...], wback_mid[...] = split2(wback_f[...])
        wfr_hi[...], wfr_mid[...] = split2(wframe[...])

    def to_global(f, y, width):
        comps = []
        x = [y[:, 128 * b : 128 * b + 128] for b in range(3)]
        keep = lane_iota(f.shape[0]) < width
        for a in range(3):
            g = (
                column(f, 3 * a) * x[0]
                + column(f, 3 * a + 1) * x[1]
                + column(f, 3 * a + 2) * x[2]
                + column(f, 9 + a)
            )
            comps.append(jnp.where(keep, g, 0.0))
        return comps

    def square_terms(comps):
        sq = comps[0] * comps[0] + comps[1] * comps[1] + comps[2] * comps[2]
        f = lax.broadcasted_iota(jnp.int32, (128, 128), 0)
        n = lax.broadcasted_iota(jnp.int32, (128, 128), 1)
        pick = jnp.where((f < 48) & (n == 96 + f // PQ), 1.0, 0.0).astype(BF16)
        hi, mid = split2(sq)
        lo = (sq - hi.astype(F32) - mid.astype(F32)).astype(BF16)
        total = (mm(hi, pick) + mm(mid, pick) + mm(lo, pick)) * gamma[...]
        hi, mid = split2(total)
        lo = (total - hi.astype(F32) - mid.astype(F32)).astype(BF16)
        return hi, mid, lo

    def query_features(it):
        s = row_recv[it].reshape(ROWS, SW)
        y = dot3(s[:, :D], wp_hi[:, :QW], wp_mid[:, :QW])
        qf[:, 0:256] = y[:, :256]
        comps = to_global(s[:, D:], y[:, 256:], 96)
        squares = square_terms(comps)
        lane = lane_iota(ROWS)
        for a in range(3):
            hi, mid = split2(comps[a] * gamma[...])
            ones = jnp.where(lane < 96 + H, 1.0, 0.0)
            qf[:, 256 + 128 * a : 384 + 128 * a] = jnp.where(lane < 96, hi.astype(F32), ones)
            qf[:, 640 + 128 * a : 768 + 128 * a] = jnp.where(
                lane < 48, mid.astype(F32), jnp.where(lane < 96, 0.0, squares[a].astype(F32))
            )

        mask = hmask[...]

        def spread(k, carry):
            for u in range(4):
                i = k * 4 + u
                row = jnp.broadcast_to(qf[pl.ds(i, 1), :], (HP, FW))
                at = pl.multiple_of(i * HP, HP)
                qmask[pl.ds(at, HP), :] = (row * mask).astype(BF16)
            return carry

        lax.fori_loop(0, ROWS // 4, spread, 0)

    def key_features(it):
        s = col_recv[it].reshape(COLS, SW)
        hi, mid = split2(s[:, :D])
        w_hi, w_mid = wp_hi[:, QW:], wp_mid[:, QW:]
        y = mm(hi, w_hi) + mm(mid, w_hi) + mm(hi, w_mid)
        kf[:, 0:256] = y[:, :256].astype(BF16)
        f = s[:, D:]
        comps = to_global(f, y[:, 256:QW], 96)
        squares = square_terms(comps)
        lane = lane_iota(COLS)
        zero = jnp.zeros((COLS, 128), F32)
        for a in range(3):
            hi, mid = split2(comps[a])
            hi, mid = hi.astype(F32), mid.astype(F32)
            sq = squares[a].astype(F32)
            kf[:, 256 + 128 * a : 384 + 128 * a] = jnp.where(
                lane < 48, hi, jnp.where(lane < 96, mid, sq)
            ).astype(BF16)
            ones = jnp.where((lane >= 96) & (lane < 96 + H), 1.0, zero)
            kf[:, 640 + 128 * a : 768 + 128 * a] = jnp.where(lane < 48, hi, ones).astype(BF16)
        v = y[:, QW : QW + 256].astype(BF16)
        vcat[0:COLS, 0:256] = v
        vcat[COLS : 2 * COLS, 0:256] = v
        vcat[2 * COLS :, 0:256] = jnp.zeros((COLS, 256), BF16)
        values = to_global(f, y[:, QW + 256 :], 96)
        for a in range(3):
            hi, mid = split2(values[a])
            at = 256 + 128 * a
            vcat[0:COLS, at : at + 128] = hi
            vcat[COLS : 2 * COLS, at : at + 128] = hi
            vcat[2 * COLS :, at : at + 128] = mid

    def prepare_pair():
        copies[2].wait()
        fq = row_recv[0].reshape(ROWS, SW)[:, D:]
        fk = col_recv[0].reshape(COLS, SW)[:, D:]
        idx_b[0:ROWS] = column(fq, 12)
        idx_b[ROWS:] = column(fq, 13)
        key_index = column(fk, 12)
        key_live = fk.T[13:14, :]
        lane = lax.broadcasted_iota(jnp.int32, (COLS, 128), 1).astype(F32)
        table = relpos[...]
        gains = gain[...]
        project = wb_t[...]

        def prepare(k, carry):
            for u in range(2):
                i = k * 2 + u
                offset = jnp.clip(key_index - idx_b[pl.ds(i, 1), :], -64.0, 63.0) + 64.0
                onehot = jnp.where(offset == lane, 1.0, 0.0).astype(BF16)
                x = pair_v[i].astype(F32) + mm(onehot, table)
                normed = (layer_norm(x) * gains).astype(BF16)
                pair_v[i] = normed
                bias = lax.dot_general(
                    project, normed, (((1,), (1,)), ((), ())), preferred_element_type=F32
                )
                live = key_live * idx_b[pl.ds(ROWS + i, 1), :] > 0.5
                at = pl.multiple_of(i * HP, HP)
                bias_v[pl.ds(at, HP), :] = jnp.where(live, bias * THIRD, DEAD)
            return carry

        lax.fori_loop(0, ROWS // 2, prepare, 0)

    def attend(it):
        keys = kf[...]
        rows = 128

        def logits_of(k, carry):
            at = pl.multiple_of(k * rows, rows)
            part = pl.ds(at, rows)
            acc = lax.dot_general(
                qmask[part, :], keys, (((1,), (1,)), ((), ())), preferred_element_type=F32
            )
            bias = bias_v[part, :]
            logits = jnp.where(bias > -1e38, acc * (THIRD / math.sqrt(C)) + bias, MASKED_LOGIT)
            top = jnp.max(logits, axis=-1, keepdims=True)
            p = jnp.exp(logits - top)
            m_b[part, :] = jnp.broadcast_to(top, (rows, 128))
            s_b[part, :] = jnp.broadcast_to(jnp.sum(p, axis=-1, keepdims=True), (rows, 128))
            hi, mid = split2(p)
            p_s[part, 0:128] = hi
            p_s[part, 128:256] = mid
            p_s[part, 256:384] = hi
            return carry

        lax.fori_loop(0, ROWS * HP // rows, logits_of, 0)

        lane = lane_iota(8)
        tops = jnp.zeros((8, 128), F32)
        sums = jnp.zeros((8, 128), F32)
        for g in range(8):
            for h in range(HP):
                src = pl.ds(8 * HP * g + h, 8, stride=HP)
                tops = jnp.where(lane == g * HP + h, m_b[src, :], tops)
                sums = jnp.where(lane == g * HP + h, s_b[src, :], sums)
        sync_send[it, 0:8] = tops
        sync_send[it, 8:16] = sums
        for d in range(1, NC):
            sync_copy(it, lax.rem(c + d, NC), c).start()
        sync_recv[it, c] = sync_send[it]

        def pair_sum(k, carry):
            for u in range(8):
                i = k * 8 + u
                at = pl.multiple_of(i * HP, HP)
                pair_s[pl.ds(at, HP), :] = mm(p_s[pl.ds(at, HP), 0:128], pair_v[i])
            return carry

        lax.fori_loop(0, ROWS // 8, pair_sum, 0)
        values = vcat[...]

        def value_sum(k, carry):
            at = pl.multiple_of(k * 256, 256)
            part = pl.ds(at, 256)
            y = mm(p_s[part, :], values)
            for t in range(5):
                r_s[t, part, :] = y[:, 128 * t : 128 * t + 128]
            return carry

        lax.fori_loop(0, ROWS * HP // 256, value_sum, 0)

        for d in range(1, NC):
            peer = lax.rem(c + d, NC)
            sync_copy(it, peer, peer).wait_recv()
        all_tops = [sync_recv[it, k, 0:8] for k in range(NC)]
        top = functools.reduce(jnp.maximum, all_tops)
        total = jnp.zeros((8, 128), F32)
        for k in range(NC):
            total = total + sync_recv[it, k, 8:16] * jnp.exp(all_tops[k] - top)
        factor = jnp.exp(tops - top) / total

        scale = []
        for h in range(H):
            scale.append(
                jnp.concatenate([column(factor, g * HP + h) for g in range(8)], axis=0)
            )

        wide = lane_iota(ROWS)
        tiles = []
        for t in range(5):
            out = jnp.zeros((ROWS, 128), F32)
            if t == 0:
                heads, first, size = range(0, 8), 0, C
            elif t == 1:
                heads, first, size = range(8, 12), 8, C
            else:
                heads, first, size = range(0, H), 0, PV
            for h in heads:
                part = r_s[t, pl.ds(h, ROWS, stride=HP), :] * scale[h]
                lo = (h - first) * size
                out = jnp.where((wide >= lo) & (wide < lo + size), part, out)
            tiles.append(out)
        pairs = [pair_s[pl.ds(h, ROWS, stride=HP), :] * scale[h] for h in range(H)]
        mixed_in = jnp.concatenate(tiles[:2] + pairs, axis=1)
        mixed = dot3(mixed_in, wmix_hi[...], wmix_mid[...])
        red_send[it, :, :, 0:D] = mixed.reshape(NC, OWN, D)
        for a in range(3):
            red_send[it, :, :, D + 128 * a : D + 128 * a + 128] = tiles[2 + a].reshape(NC, OWN, 128)
        for d in range(1, NC):
            red_copy(it, lax.rem(c + d, NC), c).start()
        red_recv[it, c] = red_send[it, c]

    def advance(it):
        for d in range(1, NC):
            peer = lax.rem(c + d, NC)
            red_copy(it, peer, peer).wait_recv()
        acc = red_recv[it, 0]
        for k in range(1, NC):
            acc = acc + red_recv[it, k]
        state = send_buf[it]
        frames = state[:, D:]
        single = state[:, :D]
        moved = [acc[:, D + 128 * a : D + 128 * a + 128] - column(frames, 9 + a) for a in range(3)]
        local = [
            column(frames, a) * moved[0]
            + column(frames, 3 + a) * moved[1]
            + column(frames, 6 + a) * moved[2]
            for a in range(3)
        ]
        lengths = jnp.sqrt(
            local[0] * local[0] + local[1] * local[1] + local[2] * local[2] + NORM_FLOOR
        )
        keep = lane_iota(OWN) < H * PV
        feats = jnp.concatenate([jnp.where(keep, x, 0.0) for x in local + [lengths]], axis=1)
        single = layer_norm(single + acc[:, :D] + dot3(feats, wloc_hi[...], wloc_mid[...]))
        hidden = jnp.maximum(dot3(single, whid_hi[...], whid_mid[...]), 0.0)
        single = layer_norm(single + dot3(hidden, wback_hi[...], wback_mid[...]))
        update = dot3(single, wfr_hi[...], wfr_mid[...])
        turn = rotation_entries(column(update, 0), column(update, 1), column(update, 2))
        rot = [column(frames, k) for k in range(9)]
        step = [column(update, 3 + k) for k in range(3)]
        new = [
            rot[3 * left] * turn[right]
            + rot[3 * left + 1] * turn[3 + right]
            + rot[3 * left + 2] * turn[6 + right]
            for left in range(3)
            for right in range(3)
        ] + [
            rot[3 * left] * step[0]
            + rot[3 * left + 1] * step[1]
            + rot[3 * left + 2] * step[2]
            + column(frames, 9 + left)
            for left in range(3)
        ]
        lane = lane_iota(OWN)
        out = frames
        for k, value in enumerate(new):
            out = jnp.where(lane == k, value, out)
        return single, out

    def iteration(it, carry):
        start_exchange(it)

        @pl.when(it == 0)
        def _():
            prepare_weights()

        @pl.when(alone)
        def _():
            swap_recv[it] = send_buf[it]

        @pl.when(jnp.logical_not(alone))
        def _():
            swap_copy(it).wait_recv()

        for d in range(1, NR):
            col_copy(it, lax.rem(r + d, NR), slot).start()
        col_recv[it, slot] = swap_recv[it]

        for d in range(1, NC):
            peer = lax.rem(c + d, NC)
            row_copy(it, peer, peer).wait_recv()
        query_features(it)
        for d in range(1, NR):
            peer = lax.rem(r + d, NR)
            col_copy(it, peer, lax.rem(peer, 2) * 8 + peer // 2).wait_recv()
        key_features(it)

        @pl.when(it == 0)
        def _():
            prepare_pair()

        attend(it)
        single, frames = advance(it)

        @pl.when(it < ITERS - 1)
        def _():
            send_buf[it + 1, :, 0:D] = single
            send_buf[it + 1, :, D:] = frames

        @pl.when(it == ITERS - 1)
        def _():
            single_out[...] = single
            frames_out[...] = frames

        @pl.when(jnp.logical_not(alone))
        def _():
            swap_copy(it).wait_send()

        for d in range(1, NC):
            peer = lax.rem(c + d, NC)
            row_copy(it, peer, c).wait_send()
            sync_copy(it, peer, c).wait_send()
            red_copy(it, peer, c).wait_send()
        for d in range(1, NR):
            col_copy(it, lax.rem(r + d, NR), slot).wait_send()
        return carry

    lax.fori_loop(0, ITERS, iteration, 0)


def body(
    pair, relpos, pair_gain, bias_weight, single, rotation_params, translation, residue_index,
    residue_mask, w_scalar, w_points, head_weights, w_out, w_hidden, w_back, w_frame,
):
    frames = jnp.stack(
        rotation_entries(rotation_params[0], rotation_params[1], rotation_params[2])
        + [translation[0], translation[1], translation[2]]
        + [residue_index.astype(F32), (residue_mask == 1).astype(F32)]
    )
    state0 = jnp.concatenate([single, frames.T, jnp.zeros((OWN, SW - D - 14), F32)], axis=1)
    scale = jax.nn.softplus(head_weights) * (math.sqrt(2.0 / (9.0 * PQ)) / 2.0)
    lane = np.arange(128)
    head = np.where(lane < 96, (lane % 48) // PQ, lane - 96)
    weight = np.where(lane < 96, 8.0, np.where(lane < 96 + H, -4.0, 0.0))
    expand = ((np.arange(H)[:, None] == head[None]) * weight[None]).astype(np.float32)
    gamma = jnp.sum(scale[:, None] * expand, axis=0, keepdims=True)
    wb_t = jnp.pad(bias_weight.T, ((0, HP - H), (0, 0)))
    wframe = jnp.pad(w_frame, ((0, 0), (0, 122)))
    smap, pmap = column_maps()

    vmem = pl.BlockSpec(memory_space=pltpu.VMEM)
    anyspace = pl.BlockSpec(memory_space=pl.ANY)
    V = pltpu.VMEM
    dma = pltpu.SemaphoreType.DMA
    scratch = [
        V((ROWS, COLS, 128), BF16),
        V((ROWS * HP, 128), F32),
        V((D, 576), F32),
        V((D, 576), F32),
        V((2112, D), F32),
        V((D, D), F32),
        V((D, D), F32),
        V((D, 3 * QW), BF16),
        V((D, 3 * QW), BF16),
        V((MIXW, D), BF16),
        V((MIXW, D), BF16),
        V((512, D), BF16),
        V((512, D), BF16),
        V((D, D), BF16),
        V((D, D), BF16),
        V((D, D), BF16),
        V((D, D), BF16),
        V((D, 128), BF16),
        V((D, 128), BF16),
        V((ITERS, OWN, SW), F32),
        V((ITERS, NC, OWN, SW), F32),
        V((ITERS, OWN, SW), F32),
        V((ITERS, NR, OWN, SW), F32),
        V((ITERS, 16, 128), F32),
        V((ITERS, NC, 16, 128), F32),
        V((ITERS, NC, OWN, RW), F32),
        V((ITERS, NC, OWN, RW), F32),
        V((ROWS, FW), F32),
        V((ROWS * HP, FW), BF16),
        V((COLS, FW), BF16),
        V((3 * COLS, QW), BF16),
        V((2 * ROWS, 128), F32),
        V((ROWS * HP, 384), BF16),
        V((ROWS * HP, 128), F32),
        V((ROWS * HP, 128), F32),
        V((5, ROWS * HP, 128), F32),
        V((ROWS * HP, 128), F32),
        dma((6,)),
        dma((NC,)),
        dma((ITERS, NC)),
        dma,
        dma((ITERS,)),
        dma((NR,)),
        dma((ITERS, NR)),
        dma((NC,)),
        dma((ITERS, NC)),
        dma((NC,)),
        dma((ITERS, NC)),
    ]
    state, tile = pl.pallas_call(
        kernel,
        out_shape=(
            jax.ShapeDtypeStruct((OWN, D), F32),
            jax.ShapeDtypeStruct((OWN, 128), F32),
        ),
        in_specs=[vmem, anyspace] + [vmem] * 7 + [anyspace] * 5 + [vmem],
        out_specs=(vmem, vmem),
        scratch_shapes=scratch,
        compiler_params=pltpu.CompilerParams(
            collective_id=0, has_side_effects=True, vmem_limit_bytes=60 * 1024 * 1024
        ),
        name="structure",
    )(
        state0, pair, relpos, pair_gain.reshape(1, 128), wb_t, gamma, head_mask(), smap, pmap,
        w_scalar, w_points, w_out, w_hidden, w_back, wframe,
    )
    return state, tile[:, :12].T


def solution(mesh):
    placed = (
        P("row", "col", None),
        P(),
        P(),
        P(),
        P(("row", "col"), None),
        P(None, ("row", "col")),
        P(None, ("row", "col")),
        P(("row", "col")),
        P(("row", "col")),
        P(),
        P(),
        P(),
        P(),
        P(),
        P(),
        P(),
    )
    return jax.shard_map(
        body,
        mesh=mesh,
        in_specs=placed,
        out_specs=(P(("row", "col"), None), P(None, ("row", "col"))),
        check_vma=False,
    )
```

```python
import functools
import math

import jax
import jax.numpy as jnp
from jax import lax
from jax.experimental import pallas as pl
from jax.experimental.pallas import tpu as pltpu
from jax.sharding import PartitionSpec as P

H = 12
C = 16
PQ = 4
PV = 8
BINS = 128
ITERS = 3
D = 384
HP = 16
ROWS = 64
COLS = 128
OWN = 8
NR = 16
NC = 8
SW = 512
RW = 768
QW = 640
FW = 1024
MIXW = 1792

NORM_EPSILON = 1e-05
MASKED_LOGIT = -100000.0
DEAD = -3e38
NORM_FLOOR = 0.1
THIRD = math.sqrt(1.0 / 3.0)
MESH = pl.DeviceIdType.MESH
F32 = jnp.float32
BF16 = jnp.bfloat16


def rotation_entries(b, c, d):
    inverse = 1.0 / (1.0 + b * b + c * c + d * d)
    entries = [
        1.0 + b * b - c * c - d * d,
        2.0 * (b * c - d),
        2.0 * (b * d + c),
        2.0 * (b * c + d),
        1.0 - b * b + c * c - d * d,
        2.0 * (c * d - b),
        2.0 * (b * d - c),
        2.0 * (c * d + b),
        1.0 - b * b - c * c + d * d,
    ]
    return [e * inverse for e in entries]


def layer_norm(values):
    center = values - jnp.mean(values, axis=-1, keepdims=True)
    spread = jnp.mean(center * center, axis=-1, keepdims=True)
    return center * lax.rsqrt(spread + NORM_EPSILON)


def split2(x):
    hi = x.astype(BF16)
    return hi, (x - hi.astype(F32)).astype(BF16)


def mm(a, b):
    return jnp.dot(a, b, preferred_element_type=F32)


def dot3(x, w_hi, w_mid):
    hi, mid = split2(x)
    n = x.shape[0]
    both = mm(jnp.concatenate([hi, mid], axis=0), w_hi)
    return both[:n] + both[n:] + mm(hi, w_mid)


def lane_iota(rows):
    return lax.broadcasted_iota(jnp.int32, (rows, 128), 1)


def pad_lanes(x):
    return jnp.concatenate([x, jnp.zeros((x.shape[0], 128 - x.shape[1]), x.dtype)], axis=1)


def column(x, k):
    return jnp.broadcast_to(x[:, k : k + 1], (x.shape[0], 128))


def kernel(
    single_in, rotation_in, translation_in, index_in, live_in, head_in, relpos, gain, wb_in, wframe,
    pair_hbm, wsc_hbm, wpt_hbm, wout_hbm, whid_hbm, wback_hbm,
    single_out, frames_out,
    pair_v, bias_v, wsc_f, wpt_f, wout_f, whid_f, wback_f, wfr_f,
    wp_hi, wp_mid, wmix_hi, wmix_mid, wloc_hi, wloc_mid, whid_hi, whid_mid, wback_hi, wback_mid,
    wfr_hi, wfr_mid, wb_s, small, gamma, hmask, centre,
    send_buf, row_recv, swap_recv, col_recv, sync_send, sync_recv, mix_send, mix_recv,
    pts_send, pts_recv,
    qf, qmask, kf, vcat, idx_b, p_s, m_b, s_b, r_s, pair_s,
    copy_sem, row_ss, row_rs, swap_ss, swap_rs, col_ss, col_rs, sync_ss, sync_rs,
    mix_ss, mix_rs, pts_ss, pts_rs,
):
    r = lax.axis_index("row")
    c = lax.axis_index("col")
    core = lax.rem(r, 2)
    z = lax.rem(r // 2, 4)
    y_hi = r // 8
    x = lax.rem(c, 4)
    y_lo = c // 4
    to_row = y_lo * 8 + lax.rem(2 * z + 6 - x, 4) * 2 + core
    to_col = y_hi * 4 + z
    from_row = y_lo * 8 + x * 2 + core
    from_col = y_hi * 4 + lax.rem(2 * x + 6 - z, 4)

    def slot_of(row):
        return lax.rem(row, 2) * 8 + (row // 8) * 4 + lax.rem(2 * x + 6 - lax.rem(row // 2, 4), 4)

    slot = slot_of(r)

    copies = [
        pltpu.make_async_copy(src, dst, copy_sem.at[k])
        for k, (src, dst) in enumerate(
            [
                (wsc_hbm, wsc_f),
                (wpt_hbm, wpt_f),
                (pair_hbm, pair_v),
                (wout_hbm, wout_f),
                (whid_hbm, whid_f),
                (wback_hbm, wback_f),
            ]
        )
    ]
    for cp in copies:
        cp.start()

    barrier = pltpu.get_barrier_semaphore()
    for d in range(1, NC):
        pl.semaphore_signal(
            barrier, inc=1, device_id=(r, lax.rem(c + d, NC)), device_id_type=MESH
        )
    for d in range(1, NR):
        pl.semaphore_signal(
            barrier, inc=1, device_id=(lax.rem(r + d, NR), c), device_id_type=MESH
        )
    pl.semaphore_signal(barrier, inc=1, device_id=(from_row, from_col), device_id_type=MESH)

    small[...] = jnp.zeros_like(small)
    entries = rotation_entries(rotation_in[0:1], rotation_in[1:2], rotation_in[2:3])
    for k, row in enumerate(
        entries
        + [translation_in[k : k + 1] for k in range(3)]
        + [index_in[...].astype(F32), jnp.where(live_in[...] == 1, 1.0, 0.0)]
    ):
        small[k : k + 1, 0:OWN] = row
    head = head_in[...]
    positive = jnp.maximum(head, 0.0) + jnp.log1p(jnp.exp(-jnp.abs(head)))
    small[14:15, 0:H] = positive * (math.sqrt(2.0 / (9.0 * PQ)) / 2.0)
    turned = small[...].T
    send_buf[0, :, 0:D] = single_in[...]
    send_buf[0, :, D:] = jnp.where(lane_iota(OWN) < 14, pad_lanes(turned[0:OWN]), 0.0)

    lane = lane_iota(HP)
    head_row = lax.broadcasted_iota(jnp.int32, (HP, 128), 0)
    low = lane < 96
    owner = jnp.where(low, lax.rem(lane, 48) // PQ, lane - 96)
    own = (owner == head_row) & (lane < 96 + H)
    spread_scale = jnp.where(own, jnp.where(low, 8.0, -4.0), 0.0)
    gamma[...] = jnp.sum(
        jnp.broadcast_to(turned[0:HP, 14:15], (HP, 128)) * spread_scale, axis=0, keepdims=True
    )
    for t in range(2):
        own_scalar = (lane + 128 * t) // C == head_row
        hmask[:, 128 * t : 128 * t + 128] = jnp.where(own_scalar & (head_row < H), 1.0, 0.0)
    for t in range(2, 8):
        hmask[:, 128 * t : 128 * t + 128] = jnp.where(own & (head_row < H), 1.0, 0.0)

    with jax.named_scope("barrier"):
        pl.semaphore_wait(barrier, NC + NR - 1)

    def row_copy(it, peer, at):
        return pltpu.make_async_remote_copy(
            src_ref=send_buf.at[it],
            dst_ref=row_recv.at[it, at],
            send_sem=row_ss.at[peer],
            recv_sem=row_rs.at[it, at],
            device_id=(r, peer),
            device_id_type=MESH,
        )

    def swap_copy(it):
        return pltpu.make_async_remote_copy(
            src_ref=send_buf.at[it],
            dst_ref=swap_recv.at[it],
            send_sem=swap_ss,
            recv_sem=swap_rs.at[it],
            device_id=(to_row, to_col),
            device_id_type=MESH,
        )

    def col_copy(it, peer, at):
        return pltpu.make_async_remote_copy(
            src_ref=swap_recv.at[it],
            dst_ref=col_recv.at[it, at],
            send_sem=col_ss.at[peer],
            recv_sem=col_rs.at[it, at],
            device_id=(peer, c),
            device_id_type=MESH,
        )

    def sync_copy(it, peer, at):
        return pltpu.make_async_remote_copy(
            src_ref=sync_send.at[it],
            dst_ref=sync_recv.at[it, at],
            send_sem=sync_ss.at[peer],
            recv_sem=sync_rs.at[it, at],
            device_id=(r, peer),
            device_id_type=MESH,
        )

    def mix_copy(it, peer, at):
        return pltpu.make_async_remote_copy(
            src_ref=mix_send.at[it, peer],
            dst_ref=mix_recv.at[it, at],
            send_sem=mix_ss.at[peer],
            recv_sem=mix_rs.at[it, at],
            device_id=(r, peer),
            device_id_type=MESH,
        )

    def pts_copy(it, peer, at):
        return pltpu.make_async_remote_copy(
            src_ref=pts_send.at[it, peer],
            dst_ref=pts_recv.at[it, at],
            send_sem=pts_ss.at[peer],
            recv_sem=pts_rs.at[it, at],
            device_id=(r, peer),
            device_id_type=MESH,
        )

    def start_exchange(it):
        swap_copy(it).start()
        for d in range(1, NC):
            row_copy(it, lax.rem(c + d, NC), c).start()
        row_recv[it, c] = send_buf[it]

    def prepare_projection():
        for cp in copies[:2]:
            cp.wait()
        zeros64 = jnp.zeros((64, D), F32)
        zeros32 = jnp.zeros((32, D), F32)

        def place(block, rows):
            hi, mid = split2(rows.T)
            wp_hi[:, 128 * block : 128 * block + 128] = hi
            wp_mid[:, 128 * block : 128 * block + 128] = mid

        for g in range(3):
            at = g * H * C
            place(5 * g, wsc_f[at : at + 128])
            place(5 * g + 1, jnp.concatenate([wsc_f[at + 128 : at + 192], zeros64], axis=0))
            for a in range(3):
                if g < 2:
                    first = g * 144 + 48 * a
                    part = wpt_f[first : first + 48]
                    rows = jnp.concatenate([part, part, zeros32], axis=0)
                else:
                    rows = jnp.concatenate(
                        [wpt_f[288 + 96 * a : 384 + 96 * a], zeros32], axis=0
                    )
                place(5 * g + 2 + a, rows)

    def prepare_weights():
        for cp in copies[3:]:
            cp.wait()
        zeros64 = jnp.zeros((64, D), BF16)
        zeros32 = jnp.zeros((32, D), BF16)
        for part, (dst_mix, dst_loc) in enumerate(((wmix_hi, wloc_hi), (wmix_mid, wloc_mid))):
            dst_mix[0:192] = split2(wout_f[0:192])[part]
            dst_mix[192:256] = zeros64
            for k in range(4):
                dst_mix[256 + 384 * k : 640 + 384 * k] = split2(
                    wout_f[576 + 384 * k : 960 + 384 * k]
                )[part]
            for k in range(4):
                dst_loc[128 * k : 128 * k + 96] = split2(wout_f[192 + 96 * k : 288 + 96 * k])[part]
                dst_loc[128 * k + 96 : 128 * k + 128] = zeros32
        whid_hi[...], whid_mid[...] = split2(whid_f[...])
        wback_hi[...], wback_mid[...] = split2(wback_f[...])
        wfr_f[...] = jnp.zeros_like(wfr_f)
        wfr_f[0:6] = wframe[...]
        wfr_hi[...], wfr_mid[...] = split2(wfr_f[...].T)

    def to_global(f, y, width):
        comps = []
        x = [y[:, 128 * b : 128 * b + 128] for b in range(3)]
        keep = lane_iota(f.shape[0]) < width
        for a in range(3):
            g = (
                column(f, 3 * a) * x[0]
                + column(f, 3 * a + 1) * x[1]
                + column(f, 3 * a + 2) * x[2]
                + column(f, 9 + a)
            )
            comps.append(jnp.where(keep, g, 0.0))
        return comps

    def square_terms(comps):
        sq = comps[0] * comps[0] + comps[1] * comps[1] + comps[2] * comps[2]
        f = lax.broadcasted_iota(jnp.int32, (128, 128), 0)
        n = lax.broadcasted_iota(jnp.int32, (128, 128), 1)
        pick = jnp.where((f < 48) & (n == 96 + f // PQ), 1.0, 0.0).astype(BF16)
        hi, mid = split2(sq)
        lo = (sq - hi.astype(F32) - mid.astype(F32)).astype(BF16)
        total = (mm(hi, pick) + mm(mid, pick) + mm(lo, pick)) * gamma[...]
        hi, mid = split2(total)
        lo = (total - hi.astype(F32) - mid.astype(F32)).astype(BF16)
        return hi, mid, lo

    def query_features(it):
        s = row_recv[it].reshape(ROWS, SW)
        y = dot3(s[:, :D], wp_hi[:, :QW], wp_mid[:, :QW])
        qf[:, 0:256] = y[:, :256]
        comps = to_global(s[:, D:], y[:, 256:], 96)
        squares = square_terms(comps)
        lane = lane_iota(ROWS)
        for a in range(3):
            hi, mid = split2(comps[a] * gamma[...])
            ones = jnp.where(lane < 96 + H, 1.0, 0.0)
            qf[:, 256 + 128 * a : 384 + 128 * a] = jnp.where(lane < 96, hi.astype(F32), ones)
            qf[:, 640 + 128 * a : 768 + 128 * a] = jnp.where(
                lane < 48, mid.astype(F32), jnp.where(lane < 96, 0.0, squares[a].astype(F32))
            )

        mask = hmask[...]

        def spread(k, carry):
            for u in range(4):
                i = k * 4 + u
                row = jnp.broadcast_to(qf[pl.ds(i, 1), :], (HP, FW))
                at = pl.multiple_of(i * HP, HP)
                qmask[pl.ds(at, HP), :] = (row * mask).astype(BF16)
            return carry

        lax.fori_loop(0, ROWS // 4, spread, 0)

    def key_features(it):
        s = col_recv[it].reshape(COLS, SW)
        hi, mid = split2(s[:, :D])
        w_hi, w_mid = wp_hi[:, QW:], wp_mid[:, QW:]
        y = mm(hi, w_hi) + mm(mid, w_hi) + mm(hi, w_mid)
        kf[:, 0:256] = y[:, :256].astype(BF16)
        f = s[:, D:]
        comps = to_global(f, y[:, 256:QW], 96)
        squares = square_terms(comps)
        lane = lane_iota(COLS)
        zero = jnp.zeros((COLS, 128), F32)
        for a in range(3):
            hi, mid = split2(comps[a])
            hi, mid = hi.astype(F32), mid.astype(F32)
            sq = squares[a].astype(F32)
            kf[:, 256 + 128 * a : 384 + 128 * a] = jnp.where(
                lane < 48, hi, jnp.where(lane < 96, mid, sq)
            ).astype(BF16)
            ones = jnp.where((lane >= 96) & (lane < 96 + H), 1.0, zero)
            kf[:, 640 + 128 * a : 768 + 128 * a] = jnp.where(lane < 48, hi, ones).astype(BF16)
        vcat[0:COLS, 0:256] = y[:, QW : QW + 256].astype(BF16)
        vcat[COLS:, 0:256] = jnp.zeros((COLS, 256), BF16)
        values = to_global(f, y[:, QW + 256 :], 96)
        for a in range(3):
            hi, mid = split2(values[a])
            at = 256 + 128 * a
            vcat[0:COLS, at : at + 128] = hi
            vcat[COLS:, at : at + 128] = mid

    def prepare_pair():
        copies[2].wait()
        fq = row_recv[0].reshape(ROWS, SW)[:, D:]
        fk = col_recv[0].reshape(COLS, SW)[:, D:]
        idx_b[0:ROWS] = column(fq, 12)
        idx_b[ROWS:] = column(fq, 13)
        key_index = column(fk, 12)
        key_live = fk.T[13:14, :]
        shape = (COLS, 128)
        lane = lax.broadcasted_iota(jnp.int32, shape, 1).astype(F32) - 64.0
        same = lax.broadcasted_iota(jnp.int32, shape, 0) == lax.broadcasted_iota(jnp.int32, shape, 1)
        table = relpos[...].astype(F32)
        hi, mid = split2(table - jnp.mean(table, axis=-1, keepdims=True))
        centre[0:128] = jnp.where(same, 1.0 - 1.0 / 128.0, -1.0 / 128.0).astype(BF16)
        centre[128:256] = hi
        centre[256:384] = mid
        wb_s[...] = jnp.zeros_like(wb_s)
        wb_s[0:H] = wb_in[...].astype(F32)
        project = wb_s[...].astype(BF16)
        gains = gain[...]
        step = 8

        def prepare(k, carry):
            first = k * step
            centres = []
            for u in range(step):
                offset = jnp.clip(key_index - idx_b[pl.ds(first + u, 1), :], -64.0, 63.0)
                onehot = jnp.where(offset == lane, 1.0, 0.0).astype(BF16)
                both = jnp.concatenate([pair_v[first + u], onehot, onehot], axis=1)
                centres.append(mm(both, centre[...]))
            for u in range(step):
                spread = jnp.mean(centres[u] * centres[u], axis=-1, keepdims=True)
                normed = (centres[u] * lax.rsqrt(spread + NORM_EPSILON) * gains).astype(BF16)
                pair_v[first + u] = normed
                bias = lax.dot_general(
                    project, normed, (((1,), (1,)), ((), ())), preferred_element_type=F32
                )
                live = key_live * idx_b[pl.ds(ROWS + first + u, 1), :] > 0.5
                at = pl.multiple_of((first + u) * HP, HP)
                bias_v[pl.ds(at, HP), :] = jnp.where(live, bias * THIRD, DEAD)
            return carry

        lax.fori_loop(0, ROWS // step, prepare, 0)

    def attend(it):
        keys = kf[...]
        rows = 256
        for k in range(ROWS * HP // rows):
            part = pl.ds(k * rows, rows)
            acc = lax.dot_general(
                qmask[part, :], keys, (((1,), (1,)), ((), ())), preferred_element_type=F32
            )
            bias = bias_v[part, :]
            logits = jnp.where(bias > -1e38, acc * (THIRD / math.sqrt(C)) + bias, MASKED_LOGIT)
            top = jnp.max(logits, axis=-1, keepdims=True)
            p = jnp.exp(logits - top).astype(BF16)
            m_b[part, :] = jnp.broadcast_to(top, (rows, 128))
            total = jnp.sum(p.astype(F32), axis=-1, keepdims=True)
            s_b[part, :] = jnp.broadcast_to(total, (rows, 128))
            p_s[part, 0:128] = p
            p_s[part, 128:256] = p

        lane = lane_iota(8)
        tops = jnp.zeros((8, 128), F32)
        sums = jnp.zeros((8, 128), F32)
        for g in range(8):
            for h in range(HP):
                src = pl.ds(8 * HP * g + h, 8, stride=HP)
                tops = jnp.where(lane == g * HP + h, m_b[src, :], tops)
                sums = jnp.where(lane == g * HP + h, s_b[src, :], sums)
        sync_send[it, 0:8] = tops
        sync_send[it, 8:16] = sums
        for d in range(1, NC):
            sync_copy(it, lax.rem(c + d, NC), c).start()
        sync_recv[it, c] = sync_send[it]

        for i in range(ROWS):
            part = pl.ds(i * HP, HP)
            pair_s[part, :] = mm(p_s[part, 0:128], pair_v[i])
        values = vcat[...]
        for k in range(4):
            part = pl.ds(k * 256, 256)
            y = mm(p_s[part, :], values)
            for t in range(5):
                r_s[t, part, :] = y[:, 128 * t : 128 * t + 128]

        with jax.named_scope("wait_sync"):
            for d in range(1, NC):
                peer = lax.rem(c + d, NC)
                sync_copy(it, peer, peer).wait_recv()
        all_tops = [sync_recv[it, k, 0:8] for k in range(NC)]
        top = functools.reduce(jnp.maximum, all_tops)
        total = jnp.zeros((8, 128), F32)
        for k in range(NC):
            total = total + sync_recv[it, k, 8:16] * jnp.exp(all_tops[k] - top)
        factor = jnp.exp(tops - top) / total

        scale = []
        for h in range(H):
            scale.append(
                jnp.concatenate([column(factor, g * HP + h) for g in range(8)], axis=0)
            )

        wide = lane_iota(ROWS)
        tiles = {}
        for t in (2, 3, 4, 0, 1):
            out = jnp.zeros((ROWS, 128), F32)
            if t == 0:
                heads, first, size = range(0, 8), 0, C
            elif t == 1:
                heads, first, size = range(8, 12), 8, C
            else:
                heads, first, size = range(0, H), 0, PV
            for h in heads:
                part = r_s[t, pl.ds(h, ROWS, stride=HP), :] * scale[h]
                lo = (h - first) * size
                out = jnp.where((wide >= lo) & (wide < lo + size), part, out)
            tiles[t] = out
        for a in range(3):
            pts_send[it, :, :, 128 * a : 128 * a + 128] = tiles[2 + a].reshape(NC, OWN, 128)
        for d in range(1, NC):
            pts_copy(it, lax.rem(c + d, NC), c).start()
        pairs = [pair_s[pl.ds(h, ROWS, stride=HP), :] * scale[h] for h in range(H)]
        mixed_in = jnp.concatenate([tiles[0], tiles[1]] + pairs, axis=1)
        mixed = dot3(mixed_in, wmix_hi[...], wmix_mid[...])
        mix_send[it] = mixed.reshape(NC, OWN, D)
        for d in range(1, NC):
            mix_copy(it, lax.rem(c + d, NC), c).start()
        pts_recv[it, c] = pts_send[it, c]
        mix_recv[it, c] = mix_send[it, c]

    def advance(it):
        with jax.named_scope("wait_pts"):
            for d in range(1, NC):
                peer = lax.rem(c + d, NC)
                pts_copy(it, peer, peer).wait_recv()
        points = pts_recv[it, 0]
        for k in range(1, NC):
            points = points + pts_recv[it, k]
        state = send_buf[it]
        frames = state[:, D:]
        single = state[:, :D]
        moved = [points[:, 128 * a : 128 * a + 128] - column(frames, 9 + a) for a in range(3)]
        local = [
            column(frames, a) * moved[0]
            + column(frames, 3 + a) * moved[1]
            + column(frames, 6 + a) * moved[2]
            for a in range(3)
        ]
        lengths = jnp.sqrt(
            local[0] * local[0] + local[1] * local[1] + local[2] * local[2] + NORM_FLOOR
        )
        keep = lane_iota(OWN) < H * PV
        feats = jnp.concatenate([jnp.where(keep, x, 0.0) for x in local + [lengths]], axis=1)
        single = single + dot3(feats, wloc_hi[...], wloc_mid[...])
        with jax.named_scope("wait_mix"):
            for d in range(1, NC):
                peer = lax.rem(c + d, NC)
                mix_copy(it, peer, peer).wait_recv()
        for k in range(NC):
            single = single + mix_recv[it, k]
        single = layer_norm(single)
        hidden = jnp.maximum(dot3(single, whid_hi[...], whid_mid[...]), 0.0)
        single = layer_norm(single + dot3(hidden, wback_hi[...], wback_mid[...]))
        update = dot3(single, wfr_hi[...], wfr_mid[...])
        turn = rotation_entries(column(update, 0), column(update, 1), column(update, 2))
        rot = [column(frames, k) for k in range(9)]
        step = [column(update, 3 + k) for k in range(3)]
        new = [
            rot[3 * left] * turn[right]
            + rot[3 * left + 1] * turn[3 + right]
            + rot[3 * left + 2] * turn[6 + right]
            for left in range(3)
            for right in range(3)
        ] + [
            rot[3 * left] * step[0]
            + rot[3 * left + 1] * step[1]
            + rot[3 * left + 2] * step[2]
            + column(frames, 9 + left)
            for left in range(3)
        ]
        lane = lane_iota(OWN)
        out = frames
        for k, value in enumerate(new):
            out = jnp.where(lane == k, value, out)
        return single, out

    def iteration(it, carry):
        with jax.named_scope("start"):
            start_exchange(it)

            @pl.when(it == 0)
            def _():
                prepare_projection()

        with jax.named_scope("wait_swap"):
            swap_copy(it).wait_recv()
        with jax.named_scope("send_col"):
            for d in range(1, NR):
                col_copy(it, lax.rem(r + d, NR), slot).start()
            col_recv[it, slot] = swap_recv[it]

            @pl.when(it == 0)
            def _():
                prepare_weights()

        with jax.named_scope("wait_row"):
            for d in range(1, NC):
                peer = lax.rem(c + d, NC)
                row_copy(it, peer, peer).wait_recv()
        with jax.named_scope("query"):
            query_features(it)
        with jax.named_scope("wait_col"):
            for d in range(1, NR):
                peer = lax.rem(r + d, NR)
                col_copy(it, peer, slot_of(peer)).wait_recv()
        with jax.named_scope("key"):
            key_features(it)
        with jax.named_scope("prep_pair"):

            @pl.when(it == 0)
            def _():
                prepare_pair()

        with jax.named_scope("attend"):
            attend(it)
        with jax.named_scope("advance"):
            single, frames = advance(it)

            @pl.when(it < ITERS - 1)
            def _():
                send_buf[it + 1, :, 0:D] = single
                send_buf[it + 1, :, D:] = frames

            @pl.when(it == ITERS - 1)
            def _():
                single_out[...] = single
                frames_out[...] = frames[:, 0:12]

        with jax.named_scope("wait_send"):
            swap_copy(it).wait_send()
            for d in range(1, NC):
                peer = lax.rem(c + d, NC)
                row_copy(it, peer, c).wait_send()
                sync_copy(it, peer, c).wait_send()
                pts_copy(it, peer, c).wait_send()
                mix_copy(it, peer, c).wait_send()
            for d in range(1, NR):
                col_copy(it, lax.rem(r + d, NR), slot).wait_send()
        return carry

    lax.fori_loop(0, ITERS, iteration, 0)


def body(
    pair, relpos, pair_gain, bias_weight, single, rotation_params, translation, residue_index,
    residue_mask, w_scalar, w_points, head_weights, w_out, w_hidden, w_back, w_frame,
):
    vmem = pl.BlockSpec(memory_space=pltpu.VMEM)
    anyspace = pl.BlockSpec(memory_space=pl.ANY)
    V = pltpu.VMEM
    dma = pltpu.SemaphoreType.DMA
    scratch = [
        V((ROWS, COLS, 128), BF16),
        V((ROWS * HP, 128), F32),
        V((576, D), F32),
        V((576, D), F32),
        V((2112, D), F32),
        V((D, D), F32),
        V((D, D), F32),
        V((128, D), F32),
        V((D, 3 * QW), BF16),
        V((D, 3 * QW), BF16),
        V((MIXW, D), BF16),
        V((MIXW, D), BF16),
        V((512, D), BF16),
        V((512, D), BF16),
        V((D, D), BF16),
        V((D, D), BF16),
        V((D, D), BF16),
        V((D, D), BF16),
        V((D, 128), BF16),
        V((D, 128), BF16),
        V((HP, 128), F32),
        V((HP, 128), F32),
        V((1, 128), F32),
        V((HP, FW), F32),
        V((3 * 128, 128), BF16),
        V((ITERS, OWN, SW), F32),
        V((ITERS, NC, OWN, SW), F32),
        V((ITERS, OWN, SW), F32),
        V((ITERS, NR, OWN, SW), F32),
        V((ITERS, 16, 128), F32),
        V((ITERS, NC, 16, 128), F32),
        V((ITERS, NC, OWN, D), F32),
        V((ITERS, NC, OWN, D), F32),
        V((ITERS, NC, OWN, D), F32),
        V((ITERS, NC, OWN, D), F32),
        V((ROWS, FW), F32),
        V((ROWS * HP, FW), BF16),
        V((COLS, FW), BF16),
        V((2 * COLS, QW), BF16),
        V((2 * ROWS, 128), F32),
        V((ROWS * HP, 256), BF16),
        V((ROWS * HP, 128), F32),
        V((ROWS * HP, 128), F32),
        V((5, ROWS * HP, 128), F32),
        V((ROWS * HP, 128), F32),
        dma((6,)),
        dma((NC,)),
        dma((ITERS, NC)),
        dma,
        dma((ITERS,)),
        dma((NR,)),
        dma((ITERS, NR)),
        dma((NC,)),
        dma((ITERS, NC)),
        dma((NC,)),
        dma((ITERS, NC)),
        dma((NC,)),
        dma((ITERS, NC)),
    ]
    state, frames = pl.pallas_call(
        kernel,
        out_shape=(
            jax.ShapeDtypeStruct((OWN, D), F32),
            jax.ShapeDtypeStruct((OWN, 12), F32),
        ),
        in_specs=[vmem] * 10 + [anyspace] * 6,
        out_specs=(vmem, vmem),
        scratch_shapes=scratch,
        compiler_params=pltpu.CompilerParams(
            collective_id=0, has_side_effects=True, vmem_limit_bytes=60 * 1024 * 1024
        ),
        name="structure",
    )(
        single, rotation_params, translation, residue_index.reshape(1, OWN),
        residue_mask.reshape(1, OWN), head_weights.reshape(1, H), relpos,
        pair_gain.reshape(1, 128), bias_weight.T, w_frame.T,
        pair, w_scalar.T, w_points.T, w_out, w_hidden, w_back,
    )
    return state, frames.T


def solution(mesh):
    placed = (
        P("row", "col", None),
        P(),
        P(),
        P(),
        P(("row", "col"), None),
        P(None, ("row", "col")),
        P(None, ("row", "col")),
        P(("row", "col")),
        P(("row", "col")),
        P(),
        P(),
        P(),
        P(),
        P(),
        P(),
        P(),
    )
    return jax.shard_map(
        body,
        mesh=mesh,
        in_specs=placed,
        out_specs=(P(("row", "col"), None), P(None, ("row", "col"))),
        check_vma=False,
    )
```

```python
import functools
import math

import jax
import jax.numpy as jnp
from jax import lax
from jax.experimental import pallas as pl
from jax.experimental.pallas import tpu as pltpu
from jax.sharding import PartitionSpec as P

H = 12
C = 16
PQ = 4
PV = 8
BINS = 128
ITERS = 3
D = 384
HP = 16
ROWS = 64
COLS = 128
OWN = 8
NR = 16
NC = 8
SW = 512
RW = 768
QW = 640
FW = 1024
MIXW = 1792

NORM_EPSILON = 1e-05
MASKED_LOGIT = -100000.0
DEAD = -3e38
NORM_FLOOR = 0.1
THIRD = math.sqrt(1.0 / 3.0)
MESH = pl.DeviceIdType.MESH
F32 = jnp.float32
BF16 = jnp.bfloat16


def rotation_entries(b, c, d):
    inverse = 1.0 / (1.0 + b * b + c * c + d * d)
    entries = [
        1.0 + b * b - c * c - d * d,
        2.0 * (b * c - d),
        2.0 * (b * d + c),
        2.0 * (b * c + d),
        1.0 - b * b + c * c - d * d,
        2.0 * (c * d - b),
        2.0 * (b * d - c),
        2.0 * (c * d + b),
        1.0 - b * b - c * c + d * d,
    ]
    return [e * inverse for e in entries]


def layer_norm(values):
    center = values - jnp.mean(values, axis=-1, keepdims=True)
    spread = jnp.mean(center * center, axis=-1, keepdims=True)
    return center * lax.rsqrt(spread + NORM_EPSILON)


def split2(x):
    hi = x.astype(BF16)
    return hi, (x - hi.astype(F32)).astype(BF16)


def mm(a, b):
    return jnp.dot(a, b, preferred_element_type=F32)


def dot3(x, w_hi, w_mid):
    hi, mid = split2(x)
    n = x.shape[0]
    both = mm(jnp.concatenate([hi, mid], axis=0), w_hi)
    return both[:n] + both[n:] + mm(hi, w_mid)


def lane_iota(rows):
    return lax.broadcasted_iota(jnp.int32, (rows, 128), 1)


def pad_lanes(x):
    return jnp.concatenate([x, jnp.zeros((x.shape[0], 128 - x.shape[1]), x.dtype)], axis=1)


def column(x, k):
    return jnp.broadcast_to(x[:, k : k + 1], (x.shape[0], 128))


def kernel(
    single_hbm, rotation_hbm, translation_hbm, index_hbm, live_hbm, head_hbm, relpos_hbm, gain_hbm,
    wb_hbm, wframe_hbm, pair_hbm, wsc_hbm, wpt_hbm, wout_hbm, whid_hbm, wback_hbm,
    single_out, frames_out,
    single_in, rotation_in, translation_in, index_in, live_in, head_in, relpos, gain, wb_in, wframe,
    pair_v, bias_v, wsc_f, wpt_f, wout_f, whid_f, wback_f, wfr_f,
    wp_hi, wp_mid, wmix_hi, wmix_mid, wloc_hi, wloc_mid, whid_hi, whid_mid, wback_hi, wback_mid,
    wfr_hi, wfr_mid, wb_s, small, gamma, hmask, centre,
    state_f, send_buf, row_recv, swap_recv, col_recv, sync_send, sync_recv, mix_send, mix_recv,
    pts_send, pts_recv,
    qf, qmask, kf, vcat, idx_b, p_s, m_b, s_b, r_s, sums_s, pair_s,
    copy_sem, row_ss, row_rs, swap_ss, swap_rs, col_ss, col_rs, sync_ss, sync_rs,
    mix_ss, mix_rs, pts_ss, pts_rs,
):
    r = lax.axis_index("row")
    c = lax.axis_index("col")
    core = lax.rem(r, 2)
    z = lax.rem(r // 2, 4)
    y_hi = r // 8
    x = lax.rem(c, 4)
    y_lo = c // 4
    to_row = y_lo * 8 + lax.rem(2 * z + 6 - x, 4) * 2 + core
    to_col = y_hi * 4 + z
    from_row = y_lo * 8 + x * 2 + core
    from_col = y_hi * 4 + lax.rem(2 * x + 6 - z, 4)

    def slot_of(row):
        return lax.rem(row, 2) * 8 + (row // 8) * 4 + lax.rem(2 * x + 6 - lax.rem(row // 2, 4), 4)

    slot = slot_of(r)

    barrier = pltpu.get_barrier_semaphore()
    for d in range(1, NC):
        pl.semaphore_signal(
            barrier, inc=1, device_id=(r, lax.rem(c + d, NC)), device_id_type=MESH
        )
    for d in range(1, NR):
        pl.semaphore_signal(
            barrier, inc=1, device_id=(lax.rem(r + d, NR), c), device_id_type=MESH
        )
    pl.semaphore_signal(barrier, inc=1, device_id=(from_row, from_col), device_id_type=MESH)

    small_copies = [
        pltpu.make_async_copy(src, dst, copy_sem.at[6 + k])
        for k, (src, dst) in enumerate(
            [
                (single_hbm, single_in),
                (rotation_hbm, rotation_in),
                (translation_hbm, translation_in),
                (index_hbm, index_in),
                (live_hbm, live_in),
                (head_hbm, head_in),
                (relpos_hbm, relpos),
                (gain_hbm, gain),
                (wb_hbm, wb_in),
                (wframe_hbm, wframe),
            ]
        )
    ]
    copies = [
        pltpu.make_async_copy(src, dst, copy_sem.at[k])
        for k, (src, dst) in enumerate(
            [
                (wsc_hbm, wsc_f),
                (wpt_hbm, wpt_f),
                (pair_hbm, pair_v),
                (wout_hbm, wout_f),
                (whid_hbm, whid_f),
                (wback_hbm, wback_f),
            ]
        )
    ]
    for cp in small_copies + copies:
        cp.start()
    for cp in small_copies:
        cp.wait()

    small[...] = jnp.zeros_like(small)
    entries = rotation_entries(rotation_in[0:1], rotation_in[1:2], rotation_in[2:3])
    for k, row in enumerate(
        entries
        + [translation_in[k : k + 1] for k in range(3)]
        + [index_in[...].astype(F32), jnp.where(live_in[...] == 1, 1.0, 0.0)]
    ):
        small[k : k + 1, 0:OWN] = row
    head = head_in[...]
    positive = jnp.maximum(head, 0.0) + jnp.log1p(jnp.exp(-jnp.abs(head)))
    small[14:15, 0:H] = positive * (math.sqrt(2.0 / (9.0 * PQ)) / 2.0)
    turned = small[...].T
    state_f[:, 0:D] = single_in[...]
    state_f[:, D:] = pad_lanes(jnp.concatenate([turned[0:OWN]] * 3, axis=1))

    def pack(single, frames):
        at = lane_iota(OWN)
        hi, mid = split2(frames)
        lo = (frames - hi.astype(F32) - mid.astype(F32)).astype(BF16)
        pieces = jnp.where(
            at < 16,
            hi.astype(F32),
            jnp.where(at < 32, mid.astype(F32), jnp.where(at < 48, lo.astype(F32), 0.0)),
        )
        return jnp.concatenate([single.astype(BF16), pieces.astype(BF16)], axis=1)

    def unpack(blocks):
        rows = blocks.astype(F32).reshape(blocks.shape[0] * OWN, SW)
        f = rows[:, D:]
        f = f + pltpu.roll(f, 112, 1) + pltpu.roll(f, 96, 1)
        return rows[:, :D].astype(BF16), f

    send_buf[0] = pack(state_f[:, 0:D], state_f[:, D:])

    lane = lane_iota(HP)
    head_row = lax.broadcasted_iota(jnp.int32, (HP, 128), 0)
    low = lane < 96
    owner = jnp.where(low, lax.rem(lane, 48) // PQ, lane - 96)
    own = (owner == head_row) & (lane < 96 + H)
    spread_scale = jnp.where(own, jnp.where(low, 8.0, -4.0), 0.0)
    gamma[...] = jnp.sum(
        jnp.broadcast_to(turned[0:HP, 14:15], (HP, 128)) * spread_scale, axis=0, keepdims=True
    )
    for t in range(2):
        own_scalar = (lane + 128 * t) // C == head_row
        hmask[:, 128 * t : 128 * t + 128] = jnp.where(own_scalar & (head_row < H), 1.0, 0.0)
    for t in range(2, 8):
        hmask[:, 128 * t : 128 * t + 128] = jnp.where(own & (head_row < H), 1.0, 0.0)

    with jax.named_scope("barrier"):
        pl.semaphore_wait(barrier, NC + NR - 1)

    def row_copy(it, peer, at):
        return pltpu.make_async_remote_copy(
            src_ref=send_buf.at[it],
            dst_ref=row_recv.at[it, at],
            send_sem=row_ss.at[peer],
            recv_sem=row_rs.at[it, at],
            device_id=(r, peer),
            device_id_type=MESH,
        )

    def swap_copy(it):
        return pltpu.make_async_remote_copy(
            src_ref=send_buf.at[it],
            dst_ref=swap_recv.at[it],
            send_sem=swap_ss,
            recv_sem=swap_rs.at[it],
            device_id=(to_row, to_col),
            device_id_type=MESH,
        )

    def col_copy(it, peer, at):
        return pltpu.make_async_remote_copy(
            src_ref=swap_recv.at[it],
            dst_ref=col_recv.at[it, at],
            send_sem=col_ss.at[peer],
            recv_sem=col_rs.at[it, at],
            device_id=(peer, c),
            device_id_type=MESH,
        )

    def sync_copy(it, peer, at):
        return pltpu.make_async_remote_copy(
            src_ref=sync_send.at[it],
            dst_ref=sync_recv.at[it, at],
            send_sem=sync_ss.at[peer],
            recv_sem=sync_rs.at[it, at],
            device_id=(r, peer),
            device_id_type=MESH,
        )

    def mix_copy(it, peer, at):
        return pltpu.make_async_remote_copy(
            src_ref=mix_send.at[it, peer],
            dst_ref=mix_recv.at[it, at],
            send_sem=mix_ss.at[peer],
            recv_sem=mix_rs.at[it, at],
            device_id=(r, peer),
            device_id_type=MESH,
        )

    def pts_copy(it, peer, at):
        return pltpu.make_async_remote_copy(
            src_ref=pts_send.at[it, peer],
            dst_ref=pts_recv.at[it, at],
            send_sem=pts_ss.at[peer],
            recv_sem=pts_rs.at[it, at],
            device_id=(r, peer),
            device_id_type=MESH,
        )

    def start_exchange(it):
        swap_copy(it).start()
        for d in range(1, NC):
            row_copy(it, lax.rem(c + d, NC), c).start()
        row_recv[it, c] = send_buf[it]

    def prepare_projection():
        for cp in copies[:2]:
            cp.wait()
        zeros64 = jnp.zeros((64, D), F32)
        zeros32 = jnp.zeros((32, D), F32)

        def place(block, rows):
            hi, mid = split2(rows.T)
            wp_hi[:, 128 * block : 128 * block + 128] = hi
            wp_mid[:, 128 * block : 128 * block + 128] = mid

        for g in range(3):
            at = g * H * C
            place(5 * g, wsc_f[at : at + 128])
            place(5 * g + 1, jnp.concatenate([wsc_f[at + 128 : at + 192], zeros64], axis=0))
            for a in range(3):
                if g < 2:
                    first = g * 144 + 48 * a
                    part = wpt_f[first : first + 48]
                    rows = jnp.concatenate([part, part, zeros32], axis=0)
                else:
                    rows = jnp.concatenate(
                        [wpt_f[288 + 96 * a : 384 + 96 * a], zeros32], axis=0
                    )
                place(5 * g + 2 + a, rows)

    def prepare_weights():
        for cp in copies[3:]:
            cp.wait()
        zeros64 = jnp.zeros((64, D), BF16)
        zeros32 = jnp.zeros((32, D), BF16)
        for part, (dst_mix, dst_loc) in enumerate(((wmix_hi, wloc_hi), (wmix_mid, wloc_mid))):
            dst_mix[0:192] = split2(wout_f[0:192])[part]
            dst_mix[192:256] = zeros64
            for k in range(4):
                dst_mix[256 + 384 * k : 640 + 384 * k] = split2(
                    wout_f[576 + 384 * k : 960 + 384 * k]
                )[part]
            for k in range(4):
                dst_loc[128 * k : 128 * k + 96] = split2(wout_f[192 + 96 * k : 288 + 96 * k])[part]
                dst_loc[128 * k + 96 : 128 * k + 128] = zeros32
        whid_hi[...], whid_mid[...] = split2(whid_f[...])
        wback_hi[...], wback_mid[...] = split2(wback_f[...])
        wfr_f[...] = jnp.zeros_like(wfr_f)
        wfr_f[0:6] = wframe[...]
        wfr_hi[...], wfr_mid[...] = split2(wfr_f[...].T)

    def to_global(f, y, width):
        comps = []
        x = [y[:, 128 * b : 128 * b + 128] for b in range(3)]
        keep = lane_iota(f.shape[0]) < width
        for a in range(3):
            g = (
                column(f, 3 * a) * x[0]
                + column(f, 3 * a + 1) * x[1]
                + column(f, 3 * a + 2) * x[2]
                + column(f, 9 + a)
            )
            comps.append(jnp.where(keep, g, 0.0))
        return comps

    def square_terms(comps):
        sq = comps[0] * comps[0] + comps[1] * comps[1] + comps[2] * comps[2]
        f = lax.broadcasted_iota(jnp.int32, (128, 128), 0)
        n = lax.broadcasted_iota(jnp.int32, (128, 128), 1)
        pick = jnp.where((f < 48) & (n == 96 + f // PQ), 1.0, 0.0).astype(BF16)
        hi, mid = split2(sq)
        lo = (sq - hi.astype(F32) - mid.astype(F32)).astype(BF16)
        total = (mm(hi, pick) + mm(mid, pick) + mm(lo, pick)) * gamma[...]
        hi, mid = split2(total)
        lo = (total - hi.astype(F32) - mid.astype(F32)).astype(BF16)
        return hi, mid, lo

    def query_features(it):
        s, f = unpack(row_recv[it])
        y = mm(s, wp_hi[:, :QW]) + mm(s, wp_mid[:, :QW])
        qf[:, 0:256] = y[:, :256]
        comps = to_global(f, y[:, 256:], 96)
        squares = square_terms(comps)
        lane = lane_iota(ROWS)
        for a in range(3):
            hi, mid = split2(comps[a] * gamma[...])
            ones = jnp.where(lane < 96 + H, 1.0, 0.0)
            qf[:, 256 + 128 * a : 384 + 128 * a] = jnp.where(lane < 96, hi.astype(F32), ones)
            qf[:, 640 + 128 * a : 768 + 128 * a] = jnp.where(
                lane < 48, mid.astype(F32), jnp.where(lane < 96, 0.0, squares[a].astype(F32))
            )

        mask = hmask[...]

        def spread(k, carry):
            for u in range(4):
                i = k * 4 + u
                row = jnp.broadcast_to(qf[pl.ds(i, 1), :], (HP, FW))
                at = pl.multiple_of(i * HP, HP)
                qmask[pl.ds(at, HP), :] = (row * mask).astype(BF16)
            return carry

        lax.fori_loop(0, ROWS // 4, spread, 0)

    def key_features(it):
        s, f = unpack(col_recv[it])
        y = mm(s, wp_hi[:, QW : 2 * QW]) + mm(s, wp_mid[:, QW : 2 * QW])
        kf[:, 0:256] = y[:, :256].astype(BF16)
        comps = to_global(f, y[:, 256:QW], 96)
        squares = square_terms(comps)
        lane = lane_iota(COLS)
        zero = jnp.zeros((COLS, 128), F32)
        for a in range(3):
            hi, mid = split2(comps[a])
            hi, mid = hi.astype(F32), mid.astype(F32)
            sq = squares[a].astype(F32)
            kf[:, 256 + 128 * a : 384 + 128 * a] = jnp.where(
                lane < 48, hi, jnp.where(lane < 96, mid, sq)
            ).astype(BF16)
            ones = jnp.where((lane >= 96) & (lane < 96 + H), 1.0, zero)
            kf[:, 640 + 128 * a : 768 + 128 * a] = jnp.where(lane < 48, hi, ones).astype(BF16)

    def value_features(it):
        s, f = unpack(col_recv[it])
        y = mm(s, wp_hi[:, 2 * QW :]) + mm(s, wp_mid[:, 2 * QW :])
        vcat[0:COLS, 0:256] = y[:, :256].astype(BF16)
        vcat[COLS:, 0:256] = jnp.zeros((COLS, 256), BF16)
        values = to_global(f, y[:, 256:], 96)
        for a in range(3):
            hi, mid = split2(values[a])
            at = 256 + 128 * a
            vcat[0:COLS, at : at + 128] = hi
            vcat[COLS:, at : at + 128] = mid

    def prepare_pair():
        copies[2].wait()
        fq = unpack(row_recv[0])[1]
        fk = unpack(col_recv[0])[1]
        idx_b[0:ROWS] = column(fq, 12)
        idx_b[ROWS:] = column(fq, 13)
        key_index = column(fk, 12)
        key_live = fk.T[13:14, :]
        shape = (COLS, 128)
        lane = lax.broadcasted_iota(jnp.int32, shape, 1).astype(F32) - 64.0
        same = lax.broadcasted_iota(jnp.int32, shape, 0) == lax.broadcasted_iota(jnp.int32, shape, 1)
        table = relpos[...].astype(F32)
        hi, mid = split2(table - jnp.mean(table, axis=-1, keepdims=True))
        centre[0:128] = jnp.where(same, 1.0 - 1.0 / 128.0, -1.0 / 128.0).astype(BF16)
        centre[128:256] = hi
        centre[256:384] = mid
        wb_s[...] = jnp.zeros_like(wb_s)
        wb_s[0:H] = wb_in[...].astype(F32)
        project = wb_s[...].astype(BF16)
        gains = gain[...]
        step = 8

        def prepare(k, carry):
            first = k * step
            centres = []
            for u in range(step):
                offset = jnp.clip(key_index - idx_b[pl.ds(first + u, 1), :], -64.0, 63.0)
                onehot = jnp.where(offset == lane, 1.0, 0.0).astype(BF16)
                both = jnp.concatenate([pair_v[first + u], onehot, onehot], axis=1)
                centres.append(mm(both, centre[...]))
            for u in range(step):
                spread = jnp.mean(centres[u] * centres[u], axis=-1, keepdims=True)
                normed = (centres[u] * lax.rsqrt(spread + NORM_EPSILON) * gains).astype(BF16)
                pair_v[first + u] = normed
                bias = lax.dot_general(
                    project, normed, (((1,), (1,)), ((), ())), preferred_element_type=F32
                )
                live = key_live * idx_b[pl.ds(ROWS + first + u, 1), :] > 0.5
                at = pl.multiple_of((first + u) * HP, HP)
                bias_v[pl.ds(at, HP), :] = jnp.where(live, bias * THIRD, DEAD)
            return carry

        lax.fori_loop(0, ROWS // step, prepare, 0)

    def attend(it):
        keys = kf[...]
        rows = 256
        for k in range(ROWS * HP // rows):
            part = pl.ds(k * rows, rows)
            acc = lax.dot_general(
                qmask[part, :], keys, (((1,), (1,)), ((), ())), preferred_element_type=F32
            )
            bias = bias_v[part, :]
            logits = jnp.where(bias > -1e38, acc * (THIRD / math.sqrt(C)) + bias, MASKED_LOGIT)
            top = jnp.max(logits, axis=-1, keepdims=True)
            p = jnp.exp(logits - top).astype(BF16)
            m_b[part, :] = jnp.broadcast_to(top, (rows, 128))
            total = jnp.sum(p.astype(F32), axis=-1, keepdims=True)
            s_b[part, :] = jnp.broadcast_to(total, (rows, 128))
            p_s[part, 0:128] = p
            p_s[part, 128:256] = p

        lane = lane_iota(8)
        tops = jnp.zeros((8, 128), F32)
        sums = jnp.zeros((8, 128), F32)
        for g in range(8):
            for h in range(HP):
                src = pl.ds(8 * HP * g + h, 8, stride=HP)
                tops = jnp.where(lane == g * HP + h, m_b[src, :], tops)
                sums = jnp.where(lane == g * HP + h, s_b[src, :], sums)
        sync_send[it, 0:8] = tops
        sync_send[it, 8:16] = sums
        for d in range(1, NC):
            sync_copy(it, lax.rem(c + d, NC), c).start()
        sync_recv[it, c] = sync_send[it]

        @pl.when(it == 0)
        def _():
            prepare_weights()

        value_features(it)
        for i in range(ROWS):
            part = pl.ds(i * HP, HP)
            pair_s[part, :] = mm(p_s[part, 0:128], pair_v[i])
        values = vcat[...]
        for k in range(4):
            part = pl.ds(k * 256, 256)
            y = mm(p_s[part, :], values)
            for t in range(5):
                r_s[t, part, :] = y[:, 128 * t : 128 * t + 128]

        wide = lane_iota(ROWS)

        def layout_of(t):
            if t == 0:
                return range(0, 8), 0, C
            if t == 1:
                return range(8, 12), 8, C
            return range(0, H), 0, PV

        def by_head(t, piece):
            heads, first, size = layout_of(t)
            out = jnp.zeros((ROWS, 128), F32)
            for h in heads:
                lo = (h - first) * size
                out = jnp.where((wide >= lo) & (wide < lo + size), piece(h), out)
            return out

        for t in range(5):
            sums_s[t] = by_head(t, lambda h: r_s[t, pl.ds(h, ROWS, stride=HP), :])

        with jax.named_scope("wait_sync"):
            for d in range(1, NC):
                peer = lax.rem(c + d, NC)
                sync_copy(it, peer, peer).wait_recv()
        all_tops = [sync_recv[it, k, 0:8] for k in range(NC)]
        top = functools.reduce(jnp.maximum, all_tops)
        total = jnp.zeros((8, 128), F32)
        for k in range(NC):
            total = total + sync_recv[it, k, 8:16] * jnp.exp(all_tops[k] - top)
        factor = jnp.exp(tops - top) / total

        scale = []
        for h in range(H):
            scale.append(
                jnp.concatenate([column(factor, g * HP + h) for g in range(8)], axis=0)
            )

        scale_points = by_head(2, lambda h: scale[h])
        for a in range(3):
            pts_send[it, :, :, 128 * a : 128 * a + 128] = (sums_s[2 + a] * scale_points).reshape(
                NC, OWN, 128
            )
        for d in range(1, NC):
            pts_copy(it, lax.rem(c + d, NC), c).start()
        pairs = [pair_s[pl.ds(h, ROWS, stride=HP), :] * scale[h] for h in range(H)]
        scalars = [sums_s[t] * by_head(t, lambda h: scale[h]) for t in range(2)]
        mixed_in = jnp.concatenate(scalars + pairs, axis=1)
        mixed = dot3(mixed_in, wmix_hi[...], wmix_mid[...])
        mix_send[it] = mixed.reshape(NC, OWN, D)
        for d in range(1, NC):
            mix_copy(it, lax.rem(c + d, NC), c).start()
        pts_recv[it, c] = pts_send[it, c]
        mix_recv[it, c] = mix_send[it, c]

    def advance(it):
        with jax.named_scope("wait_pts"):
            for d in range(1, NC):
                peer = lax.rem(c + d, NC)
                pts_copy(it, peer, peer).wait_recv()
        points = pts_recv[it, 0]
        for k in range(1, NC):
            points = points + pts_recv[it, k]
        frames = state_f[:, D:]
        single = state_f[:, :D]
        moved = [points[:, 128 * a : 128 * a + 128] - column(frames, 9 + a) for a in range(3)]
        local = [
            column(frames, a) * moved[0]
            + column(frames, 3 + a) * moved[1]
            + column(frames, 6 + a) * moved[2]
            for a in range(3)
        ]
        lengths = jnp.sqrt(
            local[0] * local[0] + local[1] * local[1] + local[2] * local[2] + NORM_FLOOR
        )
        keep = lane_iota(OWN) < H * PV
        feats = jnp.concatenate([jnp.where(keep, x, 0.0) for x in local + [lengths]], axis=1)
        single = single + dot3(feats, wloc_hi[...], wloc_mid[...])
        with jax.named_scope("wait_mix"):
            for d in range(1, NC):
                peer = lax.rem(c + d, NC)
                mix_copy(it, peer, peer).wait_recv()
        for k in range(NC):
            single = single + mix_recv[it, k]
        single = layer_norm(single)
        hidden = jnp.maximum(dot3(single, whid_hi[...], whid_mid[...]), 0.0)
        single = layer_norm(single + dot3(hidden, wback_hi[...], wback_mid[...]))
        update = dot3(single, wfr_hi[...], wfr_mid[...])
        turn = rotation_entries(column(update, 0), column(update, 1), column(update, 2))
        rot = [column(frames, k) for k in range(9)]
        step = [column(update, 3 + k) for k in range(3)]
        new = [
            rot[3 * left] * turn[right]
            + rot[3 * left + 1] * turn[3 + right]
            + rot[3 * left + 2] * turn[6 + right]
            for left in range(3)
            for right in range(3)
        ] + [
            rot[3 * left] * step[0]
            + rot[3 * left + 1] * step[1]
            + rot[3 * left + 2] * step[2]
            + column(frames, 9 + left)
            for left in range(3)
        ]
        lane = lax.rem(lane_iota(OWN), 16)
        out = frames
        for k, value in enumerate(new):
            out = jnp.where(lane == k, value, out)
        return single, out

    def iteration(it, carry):
        with jax.named_scope("start"):
            start_exchange(it)

            @pl.when(it == 0)
            def _():
                prepare_projection()

        with jax.named_scope("wait_swap"):
            swap_copy(it).wait_recv()
        with jax.named_scope("send_col"):
            for d in range(1, NR):
                col_copy(it, lax.rem(r + d, NR), slot).start()
            col_recv[it, slot] = swap_recv[it]

        with jax.named_scope("wait_row"):
            for d in range(1, NC):
                peer = lax.rem(c + d, NC)
                row_copy(it, peer, peer).wait_recv()
        with jax.named_scope("query"):
            query_features(it)
        with jax.named_scope("wait_col"):
            for d in range(1, NR):
                peer = lax.rem(r + d, NR)
                col_copy(it, peer, slot_of(peer)).wait_recv()
        with jax.named_scope("key"):
            key_features(it)
        with jax.named_scope("prep_pair"):

            @pl.when(it == 0)
            def _():
                prepare_pair()

        with jax.named_scope("attend"):
            attend(it)
        with jax.named_scope("advance"):
            single, frames = advance(it)

            @pl.when(it < ITERS - 1)
            def _():
                send_buf[it + 1] = pack(single, frames)
                state_f[:, 0:D] = single
                state_f[:, D:] = frames

            @pl.when(it == ITERS - 1)
            def _():
                single_out[...] = single
                frames_out[...] = frames[:, 0:12]

        with jax.named_scope("wait_send"):
            swap_copy(it).wait_send()
            for d in range(1, NC):
                peer = lax.rem(c + d, NC)
                row_copy(it, peer, c).wait_send()
                sync_copy(it, peer, c).wait_send()
                pts_copy(it, peer, c).wait_send()
                mix_copy(it, peer, c).wait_send()
            for d in range(1, NR):
                col_copy(it, lax.rem(r + d, NR), slot).wait_send()
        return carry

    lax.fori_loop(0, ITERS, iteration, 0)


def hand_over(state, frames, state_out, frames_out):
    state_out[...] = state[...]
    frames_out[...] = frames[...]


def body(
    pair, relpos, pair_gain, bias_weight, single, rotation_params, translation, residue_index,
    residue_mask, w_scalar, w_points, head_weights, w_out, w_hidden, w_back, w_frame,
):
    vmem = pl.BlockSpec(memory_space=pltpu.VMEM)
    anyspace = pl.BlockSpec(memory_space=pl.ANY)
    V = pltpu.VMEM
    dma = pltpu.SemaphoreType.DMA
    scratch = [
        V((OWN, D), F32),
        V((3, OWN), F32),
        V((3, OWN), F32),
        V((1, OWN), jnp.int32),
        V((1, OWN), jnp.int32),
        V((1, H), F32),
        V((128, 128), BF16),
        V((1, 128), F32),
        V((H, 128), BF16),
        V((6, D), F32),
        V((ROWS, COLS, 128), BF16),
        V((ROWS * HP, 128), F32),
        V((576, D), F32),
        V((576, D), F32),
        V((2112, D), F32),
        V((D, D), F32),
        V((D, D), F32),
        V((128, D), F32),
        V((D, 3 * QW), BF16),
        V((D, 3 * QW), BF16),
        V((MIXW, D), BF16),
        V((MIXW, D), BF16),
        V((512, D), BF16),
        V((512, D), BF16),
        V((D, D), BF16),
        V((D, D), BF16),
        V((D, D), BF16),
        V((D, D), BF16),
        V((D, 128), BF16),
        V((D, 128), BF16),
        V((HP, 128), F32),
        V((HP, 128), F32),
        V((1, 128), F32),
        V((HP, FW), F32),
        V((3 * 128, 128), BF16),
        V((OWN, SW), F32),
        V((ITERS, OWN, SW), BF16),
        V((ITERS, NC, OWN, SW), BF16),
        V((ITERS, OWN, SW), BF16),
        V((ITERS, NR, OWN, SW), BF16),
        V((ITERS, 16, 128), F32),
        V((ITERS, NC, 16, 128), F32),
        V((ITERS, NC, OWN, D), F32),
        V((ITERS, NC, OWN, D), F32),
        V((ITERS, NC, OWN, D), F32),
        V((ITERS, NC, OWN, D), F32),
        V((ROWS, FW), F32),
        V((ROWS * HP, FW), BF16),
        V((COLS, FW), BF16),
        V((2 * COLS, QW), BF16),
        V((2 * ROWS, 128), F32),
        V((ROWS * HP, 256), BF16),
        V((ROWS * HP, 128), F32),
        V((ROWS * HP, 128), F32),
        V((5, ROWS * HP, 128), F32),
        V((5, ROWS, 128), F32),
        V((ROWS * HP, 128), F32),
        dma((16,)),
        dma((NC,)),
        dma((ITERS, NC)),
        dma,
        dma((ITERS,)),
        dma((NR,)),
        dma((ITERS, NR)),
        dma((NC,)),
        dma((ITERS, NC)),
        dma((NC,)),
        dma((ITERS, NC)),
        dma((NC,)),
        dma((ITERS, NC)),
    ]
    state, frames = pl.pallas_call(
        kernel,
        out_shape=(
            jax.ShapeDtypeStruct((OWN, D), F32),
            jax.ShapeDtypeStruct((OWN, 12), F32),
        ),
        in_specs=[anyspace] * 16,
        out_specs=(vmem, vmem),
        scratch_shapes=scratch,
        compiler_params=pltpu.CompilerParams(
            collective_id=0, has_side_effects=True, vmem_limit_bytes=60 * 1024 * 1024
        ),
        name="structure",
    )(
        single, rotation_params, translation, residue_index.reshape(1, OWN),
        residue_mask.reshape(1, OWN), head_weights.reshape(1, H), relpos,
        pair_gain.reshape(1, 128), bias_weight.T, w_frame.T,
        pair, w_scalar.T, w_points.T, w_out, w_hidden, w_back,
    )
    state, frames = pl.pallas_call(
        hand_over,
        out_shape=(
            jax.ShapeDtypeStruct((OWN, D), F32),
            jax.ShapeDtypeStruct((OWN, 12), F32),
        ),
        in_specs=[vmem, vmem],
        out_specs=(vmem, vmem),
        compiler_params=pltpu.CompilerParams(vmem_limit_bytes=1024 * 1024),
        name="hand_over",
    )(state, frames)
    return state, frames.T


def solution(mesh):
    placed = (
        P("row", "col", None),
        P(),
        P(),
        P(),
        P(("row", "col"), None),
        P(None, ("row", "col")),
        P(None, ("row", "col")),
        P(("row", "col")),
        P(("row", "col")),
        P(),
        P(),
        P(),
        P(),
        P(),
        P(),
        P(),
    )
    return jax.shard_map(
        body,
        mesh=mesh,
        in_specs=placed,
        out_specs=(P(("row", "col"), None), P(None, ("row", "col"))),
        check_vma=False,
    )
```

```python
import functools
import math

import jax
import jax.numpy as jnp
from jax import lax
from jax.experimental import pallas as pl
from jax.experimental.pallas import tpu as pltpu
from jax.sharding import PartitionSpec as P

H = 12
C = 16
PQ = 4
PV = 8
BINS = 128
ITERS = 3
D = 384
HP = 16
ROWS = 64
COLS = 128
OWN = 8
NR = 16
NC = 8
SW = 512
RW = 768
QW = 640
FW = 1024
MIXW = 1792

NORM_EPSILON = 1e-05
MASKED_LOGIT = -100000.0
DEAD = -3e38
NORM_FLOOR = 0.1
THIRD = math.sqrt(1.0 / 3.0)
MESH = pl.DeviceIdType.MESH
F32 = jnp.float32
BF16 = jnp.bfloat16


def rotation_entries(b, c, d):
    inverse = 1.0 / (1.0 + b * b + c * c + d * d)
    entries = [
        1.0 + b * b - c * c - d * d,
        2.0 * (b * c - d),
        2.0 * (b * d + c),
        2.0 * (b * c + d),
        1.0 - b * b + c * c - d * d,
        2.0 * (c * d - b),
        2.0 * (b * d - c),
        2.0 * (c * d + b),
        1.0 - b * b - c * c + d * d,
    ]
    return [e * inverse for e in entries]


def layer_norm(values):
    center = values - jnp.mean(values, axis=-1, keepdims=True)
    spread = jnp.mean(center * center, axis=-1, keepdims=True)
    return center * lax.rsqrt(spread + NORM_EPSILON)


def split2(x):
    hi = x.astype(BF16)
    return hi, (x - hi.astype(F32)).astype(BF16)


def mm(a, b):
    return jnp.dot(a, b, preferred_element_type=F32)


def dot3(x, w_hi, w_mid):
    hi, mid = split2(x)
    n = x.shape[0]
    both = mm(jnp.concatenate([hi, mid], axis=0), w_hi)
    return both[:n] + both[n:] + mm(hi, w_mid)


def lane_iota(rows):
    return lax.broadcasted_iota(jnp.int32, (rows, 128), 1)


def pad_lanes(x):
    return jnp.concatenate([x, jnp.zeros((x.shape[0], 128 - x.shape[1]), x.dtype)], axis=1)


def column(x, k):
    return jnp.broadcast_to(x[:, k : k + 1], (x.shape[0], 128))


def kernel(
    single_hbm, rotation_hbm, translation_hbm, index_hbm, live_hbm, head_hbm, relpos_hbm, gain_hbm,
    wb_hbm, wframe_hbm, pair_hbm, wsc_hbm, wpt_hbm, wout_hbm, whid_hbm, wback_hbm,
    single_out, frames_out,
    single_in, rotation_in, translation_in, index_in, live_in, head_in, relpos, gain, wb_in, wframe,
    pair_v, bias_v, wsc_f, wpt_f, wout_f, whid_f, wback_f, wfr_f,
    wp_hi, wp_mid, wmix_hi, wmix_mid, wloc_hi, wloc_mid, whid_hi, whid_mid, wback_hi, wback_mid,
    wfr_hi, wfr_mid, wb_s, small, gamma, hmask, centre,
    state_f, send_buf, row_recv, swap_recv, col_recv, sync_send, sync_recv, mix_send, mix_recv,
    pts_send, pts_recv, idx_recv, key_idx,
    qf, qmask, kf, vcat, idx_b, p_s, m_b, s_b, r_s, sums_s, pair_s,
    copy_sem, row_ss, row_rs, swap_ss, swap_rs, col_ss, col_rs, sync_ss, sync_rs,
    mix_ss, mix_rs, pts_ss, pts_rs, idx_ss, idx_rs,
):
    r = lax.axis_index("row")
    c = lax.axis_index("col")
    core = lax.rem(r, 2)
    z = lax.rem(r // 2, 4)
    y_hi = r // 8
    x = lax.rem(c, 4)
    y_lo = c // 4
    to_row = y_lo * 8 + lax.rem(2 * z + 6 - x, 4) * 2 + core
    to_col = y_hi * 4 + z
    from_row = y_lo * 8 + x * 2 + core
    from_col = y_hi * 4 + lax.rem(2 * x + 6 - z, 4)

    def slot_of(row):
        return lax.rem(row, 2) * 8 + (row // 8) * 4 + lax.rem(2 * x + 6 - lax.rem(row // 2, 4), 4)

    slot = slot_of(r)
    near = (r >= 2 * c - 1) & (r <= 2 * c + 2)
    diagonal = r // 2 == c

    row_peers = [
        lax.rem(y_lo + dy, 2) * 4 + lax.rem(x + dx, 4)
        for dy, dx in ((1, 2), (1, 1), (1, 3), (0, 2), (1, 0), (0, 1), (0, 3))
    ]
    col_peers = [
        lax.rem(y_hi + dy, 2) * 8 + lax.rem(z + dz, 4) * 2 + lax.rem(core + dc, 2)
        for dy, dz in ((1, 2), (1, 1), (1, 3), (1, 0), (0, 2), (0, 1), (0, 3), (0, 0))
        for dc in (0, 1)
        if (dy, dz, dc) != (0, 0, 0)
    ]

    barrier = pltpu.get_barrier_semaphore()
    for peer in col_peers:
        pl.semaphore_signal(barrier, inc=1, device_id=(peer, c), device_id_type=MESH)
    for peer in row_peers:
        pl.semaphore_signal(barrier, inc=1, device_id=(r, peer), device_id_type=MESH)
    pl.semaphore_signal(barrier, inc=1, device_id=(from_row, from_col), device_id_type=MESH)

    small_copies = [
        pltpu.make_async_copy(src, dst, copy_sem.at[6 + k])
        for k, (src, dst) in enumerate(
            [
                (single_hbm, single_in),
                (rotation_hbm, rotation_in),
                (translation_hbm, translation_in),
                (index_hbm, index_in),
                (live_hbm, live_in),
                (head_hbm, head_in),
                (relpos_hbm, relpos),
                (gain_hbm, gain),
                (wb_hbm, wb_in),
                (wframe_hbm, wframe),
            ]
        )
    ]
    copies = [
        pltpu.make_async_copy(src, dst, copy_sem.at[k])
        for k, (src, dst) in enumerate(
            [
                (wsc_hbm, wsc_f),
                (wpt_hbm, wpt_f),
                (pair_hbm, pair_v),
                (wout_hbm, wout_f),
                (whid_hbm, whid_f),
                (wback_hbm, wback_f),
            ]
        )
    ]
    for cp in small_copies + copies:
        cp.start()
    for cp in small_copies:
        cp.wait()

    small[...] = jnp.zeros_like(small)
    entries = rotation_entries(rotation_in[0:1], rotation_in[1:2], rotation_in[2:3])
    for k, row in enumerate(
        entries
        + [translation_in[k : k + 1] for k in range(3)]
        + [index_in[...].astype(F32), jnp.where(live_in[...] == 1, 1.0, 0.0)]
    ):
        small[k : k + 1, 0:OWN] = row
    head = head_in[...]
    positive = jnp.maximum(head, 0.0) + jnp.log1p(jnp.exp(-jnp.abs(head)))
    small[14:15, 0:H] = positive * (math.sqrt(2.0 / (9.0 * PQ)) / 2.0)
    turned = small[...].T
    state_f[:, 0:D] = single_in[...]
    state_f[:, D:] = pad_lanes(jnp.concatenate([turned[0:OWN]] * 3, axis=1))

    def pack(single, frames):
        at = lane_iota(OWN)
        hi, mid = split2(frames)
        lo = (frames - hi.astype(F32) - mid.astype(F32)).astype(BF16)
        pieces = jnp.where(
            at < 16,
            hi.astype(F32),
            jnp.where(at < 32, mid.astype(F32), jnp.where(at < 48, lo.astype(F32), 0.0)),
        )
        return jnp.concatenate([single.astype(BF16), pieces.astype(BF16)], axis=1)

    def unpack(blocks):
        rows = blocks.astype(F32).reshape(blocks.shape[0] * OWN, SW)
        f = rows[:, D:]
        f = f + pltpu.roll(f, 112, 1) + pltpu.roll(f, 96, 1)
        return rows[:, :D].astype(BF16), f

    send_buf[0] = pack(state_f[:, 0:D], state_f[:, D:])

    lane = lane_iota(HP)
    head_row = lax.broadcasted_iota(jnp.int32, (HP, 128), 0)
    low = lane < 96
    owner = jnp.where(low, lax.rem(lane, 48) // PQ, lane - 96)
    own = (owner == head_row) & (lane < 96 + H)
    spread_scale = jnp.where(own, jnp.where(low, 8.0, -4.0), 0.0)
    gamma[...] = jnp.sum(
        jnp.broadcast_to(turned[0:HP, 14:15], (HP, 128)) * spread_scale, axis=0, keepdims=True
    )
    for t in range(2):
        own_scalar = (lane + 128 * t) // C == head_row
        hmask[:, 128 * t : 128 * t + 128] = jnp.where(own_scalar & (head_row < H), 1.0, 0.0)
    for t in range(2, 8):
        hmask[:, 128 * t : 128 * t + 128] = jnp.where(own & (head_row < H), 1.0, 0.0)

    with jax.named_scope("barrier"):
        pl.semaphore_wait(barrier, NC + NR - 1)

    def row_copy(it, peer, at):
        return pltpu.make_async_remote_copy(
            src_ref=send_buf.at[it],
            dst_ref=row_recv.at[it, at],
            send_sem=row_ss.at[peer],
            recv_sem=row_rs.at[it, at],
            device_id=(r, peer),
            device_id_type=MESH,
        )

    def swap_copy(it):
        return pltpu.make_async_remote_copy(
            src_ref=send_buf.at[it],
            dst_ref=swap_recv.at[it],
            send_sem=swap_ss,
            recv_sem=swap_rs.at[it],
            device_id=(to_row, to_col),
            device_id_type=MESH,
        )

    def col_copy(it, peer, at):
        return pltpu.make_async_remote_copy(
            src_ref=swap_recv.at[it],
            dst_ref=col_recv.at[it, at],
            send_sem=col_ss.at[peer],
            recv_sem=col_rs.at[it, at],
            device_id=(peer, c),
            device_id_type=MESH,
        )

    def idx_copy(peer, k, at):
        return pltpu.make_async_remote_copy(
            src_ref=row_recv.at[0, :, :, D:SW],
            dst_ref=idx_recv.at[at],
            send_sem=idx_ss.at[k],
            recv_sem=idx_rs.at[at],
            device_id=(peer, c),
            device_id_type=MESH,
        )

    idx_targets = (
        (diagonal, r + 1 - 2 * core),
        (diagonal & (c > 0), lax.rem(2 * c + 15, 16)),
        (diagonal & (c < NC - 1), lax.rem(2 * c + 2, 16)),
    )

    def send_numbers():
        for k, (needed, peer) in enumerate(idx_targets):

            @pl.when(needed)
            def _(k=k, peer=peer):
                idx_copy(peer, k, core).start()

        @pl.when(diagonal)
        def _():
            idx_recv[core] = row_recv[0, :, :, D:SW]

    def key_numbers():
        @pl.when(diagonal)
        def _():
            idx_copy(r, 0, 1 - core).wait_recv()

        @pl.when(near & jnp.logical_not(diagonal))
        def _():
            idx_copy(r, 0, 0).wait_recv()
            idx_copy(r, 0, 1).wait_recv()

        @pl.when(near)
        def _():
            f = idx_recv[...].astype(F32).reshape(COLS, 128)
            f = f + pltpu.roll(f, 112, 1) + pltpu.roll(f, 96, 1)
            key_idx[...] = column(f, 12)

        @pl.when(jnp.logical_not(near) & (c > r // 2))
        def _():
            key_idx[...] = jnp.full((COLS, 128), 1e6, F32)

        @pl.when(jnp.logical_not(near) & (c < r // 2))
        def _():
            key_idx[...] = jnp.full((COLS, 128), -1e6, F32)

    def sync_copy(it, peer, at):
        return pltpu.make_async_remote_copy(
            src_ref=sync_send.at[it],
            dst_ref=sync_recv.at[it, at],
            send_sem=sync_ss.at[peer],
            recv_sem=sync_rs.at[it, at],
            device_id=(r, peer),
            device_id_type=MESH,
        )

    def mix_copy(it, peer, at):
        return pltpu.make_async_remote_copy(
            src_ref=mix_send.at[it, peer],
            dst_ref=mix_recv.at[it, at],
            send_sem=mix_ss.at[peer],
            recv_sem=mix_rs.at[it, at],
            device_id=(r, peer),
            device_id_type=MESH,
        )

    def pts_copy(it, peer, at):
        return pltpu.make_async_remote_copy(
            src_ref=pts_send.at[it, peer],
            dst_ref=pts_recv.at[it, at],
            send_sem=pts_ss.at[peer],
            recv_sem=pts_rs.at[it, at],
            device_id=(r, peer),
            device_id_type=MESH,
        )

    def start_exchange(it):
        swap_copy(it).start()
        for peer in row_peers:
            row_copy(it, peer, c).start()
        row_recv[it, c] = send_buf[it]

    def prepare_projection():
        for cp in copies[:2]:
            cp.wait()
        zeros64 = jnp.zeros((64, D), F32)
        zeros32 = jnp.zeros((32, D), F32)

        def place(block, rows):
            hi, mid = split2(rows.T)
            wp_hi[:, 128 * block : 128 * block + 128] = hi
            wp_mid[:, 128 * block : 128 * block + 128] = mid

        for g in range(3):
            at = g * H * C
            place(5 * g, wsc_f[at : at + 128])
            place(5 * g + 1, jnp.concatenate([wsc_f[at + 128 : at + 192], zeros64], axis=0))
            for a in range(3):
                if g < 2:
                    first = g * 144 + 48 * a
                    part = wpt_f[first : first + 48]
                    rows = jnp.concatenate([part, part, zeros32], axis=0)
                else:
                    rows = jnp.concatenate(
                        [wpt_f[288 + 96 * a : 384 + 96 * a], zeros32], axis=0
                    )
                place(5 * g + 2 + a, rows)

    def prepare_weights():
        for cp in copies[3:]:
            cp.wait()
        zeros64 = jnp.zeros((64, D), BF16)
        zeros32 = jnp.zeros((32, D), BF16)
        for part, (dst_mix, dst_loc) in enumerate(((wmix_hi, wloc_hi), (wmix_mid, wloc_mid))):
            dst_mix[0:192] = split2(wout_f[0:192])[part]
            dst_mix[192:256] = zeros64
            for k in range(4):
                dst_mix[256 + 384 * k : 640 + 384 * k] = split2(
                    wout_f[576 + 384 * k : 960 + 384 * k]
                )[part]
            for k in range(4):
                dst_loc[128 * k : 128 * k + 96] = split2(wout_f[192 + 96 * k : 288 + 96 * k])[part]
                dst_loc[128 * k + 96 : 128 * k + 128] = zeros32
        whid_hi[...], whid_mid[...] = split2(whid_f[...])
        wback_hi[...], wback_mid[...] = split2(wback_f[...])
        wfr_f[...] = jnp.zeros_like(wfr_f)
        wfr_f[0:6] = wframe[...]
        wfr_hi[...], wfr_mid[...] = split2(wfr_f[...].T)

    def to_global(f, y, width):
        comps = []
        x = [y[:, 128 * b : 128 * b + 128] for b in range(3)]
        keep = lane_iota(f.shape[0]) < width
        for a in range(3):
            g = (
                column(f, 3 * a) * x[0]
                + column(f, 3 * a + 1) * x[1]
                + column(f, 3 * a + 2) * x[2]
                + column(f, 9 + a)
            )
            comps.append(jnp.where(keep, g, 0.0))
        return comps

    def square_terms(comps):
        sq = comps[0] * comps[0] + comps[1] * comps[1] + comps[2] * comps[2]
        f = lax.broadcasted_iota(jnp.int32, (128, 128), 0)
        n = lax.broadcasted_iota(jnp.int32, (128, 128), 1)
        pick = jnp.where((f < 48) & (n == 96 + f // PQ), 1.0, 0.0).astype(BF16)
        hi, mid = split2(sq)
        lo = (sq - hi.astype(F32) - mid.astype(F32)).astype(BF16)
        total = (mm(hi, pick) + mm(mid, pick) + mm(lo, pick)) * gamma[...]
        hi, mid = split2(total)
        lo = (total - hi.astype(F32) - mid.astype(F32)).astype(BF16)
        return hi, mid, lo

    def query_features(it):
        s, f = unpack(row_recv[it])
        y = mm(s, wp_hi[:, :QW]) + mm(s, wp_mid[:, :QW])
        qf[:, 0:256] = y[:, :256]
        comps = to_global(f, y[:, 256:], 96)
        squares = square_terms(comps)
        lane = lane_iota(ROWS)
        for a in range(3):
            hi, mid = split2(comps[a] * gamma[...])
            ones = jnp.where(lane < 96 + H, 1.0, 0.0)
            qf[:, 256 + 128 * a : 384 + 128 * a] = jnp.where(lane < 96, hi.astype(F32), ones)
            qf[:, 640 + 128 * a : 768 + 128 * a] = jnp.where(
                lane < 48, mid.astype(F32), jnp.where(lane < 96, 0.0, squares[a].astype(F32))
            )

        mask = hmask[...]

        def spread(k, carry):
            for u in range(4):
                i = k * 4 + u
                row = jnp.broadcast_to(qf[pl.ds(i, 1), :], (HP, FW))
                at = pl.multiple_of(i * HP, HP)
                qmask[pl.ds(at, HP), :] = (row * mask).astype(BF16)
            return carry

        lax.fori_loop(0, ROWS // 4, spread, 0)

    def key_features(it):
        s, f = unpack(col_recv[it])
        y = mm(s, wp_hi[:, QW : 2 * QW]) + mm(s, wp_mid[:, QW : 2 * QW])
        kf[:, 0:256] = y[:, :256].astype(BF16)
        comps = to_global(f, y[:, 256:QW], 96)
        squares = square_terms(comps)
        lane = lane_iota(COLS)
        zero = jnp.zeros((COLS, 128), F32)
        for a in range(3):
            hi, mid = split2(comps[a])
            hi, mid = hi.astype(F32), mid.astype(F32)
            sq = squares[a].astype(F32)
            kf[:, 256 + 128 * a : 384 + 128 * a] = jnp.where(
                lane < 48, hi, jnp.where(lane < 96, mid, sq)
            ).astype(BF16)
            ones = jnp.where((lane >= 96) & (lane < 96 + H), 1.0, zero)
            kf[:, 640 + 128 * a : 768 + 128 * a] = jnp.where(lane < 48, hi, ones).astype(BF16)

    def value_features(it):
        s, f = unpack(col_recv[it])
        y = mm(s, wp_hi[:, 2 * QW :]) + mm(s, wp_mid[:, 2 * QW :])
        vcat[0:COLS, 0:256] = y[:, :256].astype(BF16)
        vcat[COLS:, 0:256] = jnp.zeros((COLS, 256), BF16)
        values = to_global(f, y[:, 256:], 96)
        for a in range(3):
            hi, mid = split2(values[a])
            at = 256 + 128 * a
            vcat[0:COLS, at : at + 128] = hi
            vcat[COLS:, at : at + 128] = mid

    def prepare_pair():
        copies[2].wait()
        fq = unpack(row_recv[0])[1]
        idx_b[0:ROWS] = column(fq, 12)
        idx_b[ROWS:] = column(fq, 13)
        key_index = key_idx[...]
        shape = (COLS, 128)
        lane = lax.broadcasted_iota(jnp.int32, shape, 1).astype(F32) - 64.0
        same = lax.broadcasted_iota(jnp.int32, shape, 0) == lax.broadcasted_iota(jnp.int32, shape, 1)
        table = relpos[...].astype(F32)
        hi, mid = split2(table - jnp.mean(table, axis=-1, keepdims=True))
        centre[0:128] = jnp.where(same, 1.0 - 1.0 / 128.0, -1.0 / 128.0).astype(BF16)
        centre[128:256] = hi
        centre[256:384] = mid
        wb_s[...] = jnp.zeros_like(wb_s)
        wb_s[0:H] = wb_in[...].astype(F32)
        project = wb_s[...].astype(BF16)
        gains = gain[...]
        step = 8

        def prepare(k, carry):
            first = k * step
            centres = []
            for u in range(step):
                offset = jnp.clip(key_index - idx_b[pl.ds(first + u, 1), :], -64.0, 63.0)
                onehot = jnp.where(offset == lane, 1.0, 0.0).astype(BF16)
                both = jnp.concatenate([pair_v[first + u], onehot, onehot], axis=1)
                centres.append(mm(both, centre[...]))
            for u in range(step):
                spread = jnp.mean(centres[u] * centres[u], axis=-1, keepdims=True)
                normed = (centres[u] * lax.rsqrt(spread + NORM_EPSILON) * gains).astype(BF16)
                pair_v[first + u] = normed
                bias = lax.dot_general(
                    project, normed, (((1,), (1,)), ((), ())), preferred_element_type=F32
                )
                live = idx_b[pl.ds(ROWS + first + u, 1), :] > 0.5
                at = pl.multiple_of((first + u) * HP, HP)
                bias_v[pl.ds(at, HP), :] = jnp.where(live, bias * THIRD, DEAD)
            return carry

        lax.fori_loop(0, ROWS // step, prepare, 0)

    def mask_keys():
        live = unpack(col_recv[0])[1].T[13:14, :] > 0.5
        for k in range(4):
            part = pl.ds(k * 256, 256)
            bias_v[part, :] = jnp.where(live, bias_v[part, :], DEAD)

    def attend(it):
        with jax.named_scope("logits"):
            keys = kf[...]
            rows = 256
            for k in range(ROWS * HP // rows):
                part = pl.ds(k * rows, rows)
                acc = lax.dot_general(
                    qmask[part, :], keys, (((1,), (1,)), ((), ())), preferred_element_type=F32
                )
                bias = bias_v[part, :]
                logits = jnp.where(bias > -1e38, acc * (THIRD / math.sqrt(C)) + bias, MASKED_LOGIT)
                top = jnp.max(logits, axis=-1, keepdims=True)
                p = jnp.exp(logits - top).astype(BF16)
                m_b[part, :] = jnp.broadcast_to(top, (rows, 128))
                total = jnp.sum(p.astype(F32), axis=-1, keepdims=True)
                s_b[part, :] = jnp.broadcast_to(total, (rows, 128))
                p_s[part, 0:128] = p
                p_s[part, 128:256] = p

        with jax.named_scope("pack"):
            lane = lane_iota(8)
            tops = jnp.zeros((8, 128), F32)
            sums = jnp.zeros((8, 128), F32)
            for g in range(8):
                for h in range(HP):
                    src = pl.ds(8 * HP * g + h, 8, stride=HP)
                    tops = jnp.where(lane == g * HP + h, m_b[src, :], tops)
                    sums = jnp.where(lane == g * HP + h, s_b[src, :], sums)
            sync_send[it, 0:8] = tops
            sync_send[it, 8:16] = sums
            for peer in row_peers:
                sync_copy(it, peer, c).start()
            sync_recv[it, c] = sync_send[it]

        with jax.named_scope("values"):
            @pl.when(it == 0)
            def _():
                prepare_weights()

            value_features(it)
        with jax.named_scope("sums"):
            for i in range(ROWS):
                part = pl.ds(i * HP, HP)
                pair_s[part, :] = mm(p_s[part, 0:128], pair_v[i])
            values = vcat[...]
            for k in range(4):
                part = pl.ds(k * 256, 256)
                y = mm(p_s[part, :], values)
                for t in range(5):
                    r_s[t, part, :] = y[:, 128 * t : 128 * t + 128]

        wide = lane_iota(ROWS)

        def layout_of(t):
            if t == 0:
                return range(0, 8), 0, C
            if t == 1:
                return range(8, 12), 8, C
            return range(0, H), 0, PV

        def by_head(t, piece):
            heads, first, size = layout_of(t)
            out = jnp.zeros((ROWS, 128), F32)
            for h in heads:
                lo = (h - first) * size
                out = jnp.where((wide >= lo) & (wide < lo + size), piece(h), out)
            return out

        with jax.named_scope("select"):
            for t in range(5):
                sums_s[t] = by_head(t, lambda h: r_s[t, pl.ds(h, ROWS, stride=HP), :])

        with jax.named_scope("wait_sync"):
            for peer in row_peers:
                sync_copy(it, peer, peer).wait_recv()
        all_tops = [sync_recv[it, k, 0:8] for k in range(NC)]
        top = functools.reduce(jnp.maximum, all_tops)
        total = jnp.zeros((8, 128), F32)
        for k in range(NC):
            total = total + sync_recv[it, k, 8:16] * jnp.exp(all_tops[k] - top)
        factor = jnp.exp(tops - top) / total

        with jax.named_scope("factor"):
            scale = []
            for h in range(H):
                scale.append(
                    jnp.concatenate([column(factor, g * HP + h) for g in range(8)], axis=0)
                )

            scale_points = by_head(2, lambda h: scale[h])
            for a in range(3):
                pts_send[it, :, :, 128 * a : 128 * a + 128] = (sums_s[2 + a] * scale_points).reshape(
                    NC, OWN, 128
                )
            for peer in row_peers:
                pts_copy(it, peer, c).start()
        with jax.named_scope("mix"):
            pairs = [pair_s[pl.ds(h, ROWS, stride=HP), :] * scale[h] for h in range(H)]
            scalars = [sums_s[t] * by_head(t, lambda h: scale[h]) for t in range(2)]
            mixed_in = jnp.concatenate(scalars + pairs, axis=1)
            mixed = dot3(mixed_in, wmix_hi[...], wmix_mid[...])
            mix_send[it] = mixed.reshape(NC, OWN, D)
            for peer in row_peers:
                mix_copy(it, peer, c).start()
            pts_recv[it, c] = pts_send[it, c]
            mix_recv[it, c] = mix_send[it, c]

    def advance(it):
        with jax.named_scope("wait_pts"):
            for peer in row_peers:
                pts_copy(it, peer, peer).wait_recv()
        points = pts_recv[it, 0]
        for k in range(1, NC):
            points = points + pts_recv[it, k]
        frames = state_f[:, D:]
        single = state_f[:, :D]
        moved = [points[:, 128 * a : 128 * a + 128] - column(frames, 9 + a) for a in range(3)]
        local = [
            column(frames, a) * moved[0]
            + column(frames, 3 + a) * moved[1]
            + column(frames, 6 + a) * moved[2]
            for a in range(3)
        ]
        lengths = jnp.sqrt(
            local[0] * local[0] + local[1] * local[1] + local[2] * local[2] + NORM_FLOOR
        )
        keep = lane_iota(OWN) < H * PV
        feats = jnp.concatenate([jnp.where(keep, x, 0.0) for x in local + [lengths]], axis=1)
        single = single + dot3(feats, wloc_hi[...], wloc_mid[...])
        with jax.named_scope("wait_mix"):
            for peer in row_peers:
                mix_copy(it, peer, peer).wait_recv()
        for k in range(NC):
            single = single + mix_recv[it, k]
        single = layer_norm(single)
        hidden = jnp.maximum(dot3(single, whid_hi[...], whid_mid[...]), 0.0)
        single = layer_norm(single + dot3(hidden, wback_hi[...], wback_mid[...]))
        update = dot3(single, wfr_hi[...], wfr_mid[...])
        turn = rotation_entries(column(update, 0), column(update, 1), column(update, 2))
        rot = [column(frames, k) for k in range(9)]
        step = [column(update, 3 + k) for k in range(3)]
        new = [
            rot[3 * left] * turn[right]
            + rot[3 * left + 1] * turn[3 + right]
            + rot[3 * left + 2] * turn[6 + right]
            for left in range(3)
            for right in range(3)
        ] + [
            rot[3 * left] * step[0]
            + rot[3 * left + 1] * step[1]
            + rot[3 * left + 2] * step[2]
            + column(frames, 9 + left)
            for left in range(3)
        ]
        lane = lax.rem(lane_iota(OWN), 16)
        out = frames
        for k, value in enumerate(new):
            out = jnp.where(lane == k, value, out)
        return single, out

    def iteration(it, carry):
        with jax.named_scope("start"):
            start_exchange(it)

            @pl.when(it == 0)
            def _():
                prepare_projection()

        with jax.named_scope("wait_swap"):
            swap_copy(it).wait_recv()
        with jax.named_scope("send_col"):
            for peer in col_peers:
                col_copy(it, peer, slot).start()
            col_recv[it, slot] = swap_recv[it]

        with jax.named_scope("wait_row"):
            for peer in row_peers:
                row_copy(it, peer, peer).wait_recv()
        with jax.named_scope("query"):

            @pl.when(it == 0)
            def _():
                send_numbers()

            query_features(it)
        with jax.named_scope("prep_pair"):

            @pl.when(it == 0)
            def _():
                key_numbers()
                prepare_pair()

        with jax.named_scope("wait_col"):
            for peer in col_peers:
                col_copy(it, peer, slot_of(peer)).wait_recv()
        with jax.named_scope("key"):
            key_features(it)

            @pl.when(it == 0)
            def _():
                mask_keys()

        attend(it)
        with jax.named_scope("advance"):
            single, frames = advance(it)

            @pl.when(it < ITERS - 1)
            def _():
                send_buf[it + 1] = pack(single, frames)
                state_f[:, 0:D] = single
                state_f[:, D:] = frames

            @pl.when(it == ITERS - 1)
            def _():
                single_out[...] = single
                frames_out[...] = frames[:, 0:12]

        with jax.named_scope("wait_send"):
            swap_copy(it).wait_send()
            for peer in row_peers:
                row_copy(it, peer, c).wait_send()
                sync_copy(it, peer, c).wait_send()
                pts_copy(it, peer, c).wait_send()
                mix_copy(it, peer, c).wait_send()
            for peer in col_peers:
                col_copy(it, peer, slot).wait_send()
        return carry

    lax.fori_loop(0, ITERS, iteration, 0)
    for k, (needed, peer) in enumerate(idx_targets):

        @pl.when(needed)
        def _(k=k, peer=peer):
            idx_copy(peer, k, core).wait_send()


def hand_over(state, frames, state_out, frames_out):
    state_out[...] = state[...]
    frames_out[...] = frames[...]


def body(
    pair, relpos, pair_gain, bias_weight, single, rotation_params, translation, residue_index,
    residue_mask, w_scalar, w_points, head_weights, w_out, w_hidden, w_back, w_frame,
):
    vmem = pl.BlockSpec(memory_space=pltpu.VMEM)
    anyspace = pl.BlockSpec(memory_space=pl.ANY)
    V = pltpu.VMEM
    dma = pltpu.SemaphoreType.DMA
    scratch = [
        V((OWN, D), F32),
        V((3, OWN), F32),
        V((3, OWN), F32),
        V((1, OWN), jnp.int32),
        V((1, OWN), jnp.int32),
        V((1, H), F32),
        V((128, 128), BF16),
        V((1, 128), F32),
        V((H, 128), BF16),
        V((6, D), F32),
        V((ROWS, COLS, 128), BF16),
        V((ROWS * HP, 128), F32),
        V((576, D), F32),
        V((576, D), F32),
        V((2112, D), F32),
        V((D, D), F32),
        V((D, D), F32),
        V((128, D), F32),
        V((D, 3 * QW), BF16),
        V((D, 3 * QW), BF16),
        V((MIXW, D), BF16),
        V((MIXW, D), BF16),
        V((512, D), BF16),
        V((512, D), BF16),
        V((D, D), BF16),
        V((D, D), BF16),
        V((D, D), BF16),
        V((D, D), BF16),
        V((D, 128), BF16),
        V((D, 128), BF16),
        V((HP, 128), F32),
        V((HP, 128), F32),
        V((1, 128), F32),
        V((HP, FW), F32),
        V((3 * 128, 128), BF16),
        V((OWN, SW), F32),
        V((ITERS, OWN, SW), BF16),
        V((ITERS, NC, OWN, SW), BF16),
        V((ITERS, OWN, SW), BF16),
        V((ITERS, NR, OWN, SW), BF16),
        V((ITERS, 16, 128), F32),
        V((ITERS, NC, 16, 128), F32),
        V((ITERS, NC, OWN, D), F32),
        V((ITERS, NC, OWN, D), F32),
        V((ITERS, NC, OWN, D), F32),
        V((ITERS, NC, OWN, D), F32),
        V((2, NC, OWN, 128), BF16),
        V((COLS, 128), F32),
        V((ROWS, FW), F32),
        V((ROWS * HP, FW), BF16),
        V((COLS, FW), BF16),
        V((2 * COLS, QW), BF16),
        V((2 * ROWS, 128), F32),
        V((ROWS * HP, 256), BF16),
        V((ROWS * HP, 128), F32),
        V((ROWS * HP, 128), F32),
        V((5, ROWS * HP, 128), F32),
        V((5, ROWS, 128), F32),
        V((ROWS * HP, 128), F32),
        dma((16,)),
        dma((NC,)),
        dma((ITERS, NC)),
        dma,
        dma((ITERS,)),
        dma((NR,)),
        dma((ITERS, NR)),
        dma((NC,)),
        dma((ITERS, NC)),
        dma((NC,)),
        dma((ITERS, NC)),
        dma((NC,)),
        dma((ITERS, NC)),
        dma((3,)),
        dma((2,)),
    ]
    state, frames = pl.pallas_call(
        kernel,
        out_shape=(
            jax.ShapeDtypeStruct((OWN, D), F32),
            jax.ShapeDtypeStruct((OWN, 12), F32),
        ),
        in_specs=[anyspace] * 16,
        out_specs=(vmem, vmem),
        scratch_shapes=scratch,
        compiler_params=pltpu.CompilerParams(
            collective_id=0, has_side_effects=True, vmem_limit_bytes=62 * 1024 * 1024
        ),
        name="structure",
    )(
        single, rotation_params, translation, residue_index.reshape(1, OWN),
        residue_mask.reshape(1, OWN), head_weights.reshape(1, H), relpos,
        pair_gain.reshape(1, 128), bias_weight.T, w_frame.T,
        pair, w_scalar.T, w_points.T, w_out, w_hidden, w_back,
    )
    state, frames = pl.pallas_call(
        hand_over,
        out_shape=(
            jax.ShapeDtypeStruct((OWN, D), F32),
            jax.ShapeDtypeStruct((OWN, 12), F32),
        ),
        in_specs=[vmem, vmem],
        out_specs=(vmem, vmem),
        compiler_params=pltpu.CompilerParams(vmem_limit_bytes=62 * 1024 * 1024),
        name="hand_over",
    )(state, frames)
    return state, frames.T


def solution(mesh):
    placed = (
        P("row", "col", None),
        P(),
        P(),
        P(),
        P(("row", "col"), None),
        P(None, ("row", "col")),
        P(None, ("row", "col")),
        P(("row", "col")),
        P(("row", "col")),
        P(),
        P(),
        P(),
        P(),
        P(),
        P(),
        P(),
    )
    return jax.shard_map(
        body,
        mesh=mesh,
        in_specs=placed,
        out_specs=(P(("row", "col"), None), P(None, ("row", "col"))),
        check_vma=False,
    )
```

```python
import functools
import math

import jax
import jax.numpy as jnp
from jax import lax
from jax.experimental import pallas as pl
from jax.experimental.pallas import tpu as pltpu
from jax.sharding import PartitionSpec as P

H = 12
C = 16
PQ = 4
PV = 8
BINS = 128
ITERS = 3
D = 384
HP = 16
ROWS = 64
COLS = 128
OWN = 8
NR = 16
NC = 8
SW = 512
QW = 640
FW = 1024

NORM_EPSILON = 1e-05
MASKED_LOGIT = -100000.0
DEAD = -3e38
NORM_FLOOR = 0.1
THIRD = math.sqrt(1.0 / 3.0)
MESH = pl.DeviceIdType.MESH
F32 = jnp.float32
BF16 = jnp.bfloat16


def rotation_entries(b, c, d):
    inverse = 1.0 / (1.0 + b * b + c * c + d * d)
    entries = [
        1.0 + b * b - c * c - d * d,
        2.0 * (b * c - d),
        2.0 * (b * d + c),
        2.0 * (b * c + d),
        1.0 - b * b + c * c - d * d,
        2.0 * (c * d - b),
        2.0 * (b * d - c),
        2.0 * (c * d + b),
        1.0 - b * b - c * c + d * d,
    ]
    return [e * inverse for e in entries]


def layer_norm(values):
    center = values - jnp.mean(values, axis=-1, keepdims=True)
    spread = jnp.mean(center * center, axis=-1, keepdims=True)
    return center * lax.rsqrt(spread + NORM_EPSILON)


def split2(x):
    hi = x.astype(BF16)
    return hi, (x - hi.astype(F32)).astype(BF16)


def mm(a, b):
    return jnp.dot(a, b, preferred_element_type=F32)


def dot3(x, w_hi, w_mid):
    hi, mid = split2(x)
    n = x.shape[0]
    both = mm(jnp.concatenate([hi, mid], axis=0), w_hi)
    return both[:n] + both[n:] + mm(hi, w_mid)


def lane_iota(rows):
    return lax.broadcasted_iota(jnp.int32, (rows, 128), 1)


def pad_lanes(x):
    return jnp.concatenate([x, jnp.zeros((x.shape[0], 128 - x.shape[1]), x.dtype)], axis=1)


def column(x, k):
    return jnp.broadcast_to(x[:, k : k + 1], (x.shape[0], 128))


def kernel(
    single_hbm, rotation_hbm, translation_hbm, index_hbm, live_hbm, head_hbm, relpos_hbm, gain_hbm,
    wb_hbm, wframe_hbm, pair_hbm, wsc_hbm, wpt_hbm, wout_hbm, whid_hbm, wback_hbm,
    single_out, frames_out,
    single_in, rotation_in, translation_in, index_in, live_in, head_in, relpos, gain, wb_in, wframe,
    pair_v, bias_v, wsc_f, wpt_f, wout_f, whid_f, wback_f, wfr_f,
    wp_hi, wp_mid, wmix_hi, wmix_mid, wloc_hi, wloc_mid, whid_hi, whid_mid, wback_hi, wback_mid,
    wfr_hi, wfr_mid, wb_s, small, gamma, hmask, centre,
    state_f, send_buf, row_recv, swap_recv, col_recv, top_send, top_recv, pair_send, pair_recv,
    val_send, val_recv, idx_recv, key_idx,
    qf, qmask, kf, vcat, idx_b, p_s, m_b, s_b, r_s, pair_s,
    copy_sem, row_ss, row_rs, swap_ss, swap_rs, col_ss, col_rs, top_ss, top_rs,
    pair_ss, pair_rs, val_ss, val_rs, idx_ss, idx_rs,
):
    r = lax.axis_index("row")
    c = lax.axis_index("col")
    core = lax.rem(r, 2)
    z = lax.rem(r // 2, 4)
    y_hi = r // 8
    x = lax.rem(c, 4)
    y_lo = c // 4
    to_row = y_lo * 8 + lax.rem(2 * z + 6 - x, 4) * 2 + core
    to_col = y_hi * 4 + z
    from_row = y_lo * 8 + x * 2 + core
    from_col = y_hi * 4 + lax.rem(2 * x + 6 - z, 4)

    def slot_of(row):
        return lax.rem(row, 2) * 8 + (row // 8) * 4 + lax.rem(2 * x + 6 - lax.rem(row // 2, 4), 4)

    slot = slot_of(r)
    near = (r >= 2 * c - 1) & (r <= 2 * c + 2)
    diagonal = r // 2 == c

    row_peers = [
        lax.rem(y_lo + dy, 2) * 4 + lax.rem(x + dx, 4)
        for dy, dx in ((1, 2), (1, 1), (1, 3), (0, 2), (1, 0), (0, 1), (0, 3))
    ]
    col_peers = [
        lax.rem(y_hi + dy, 2) * 8 + lax.rem(z + dz, 4) * 2 + lax.rem(core + dc, 2)
        for dy, dz in ((1, 2), (1, 1), (1, 3), (1, 0), (0, 2), (0, 1), (0, 3), (0, 0))
        for dc in (0, 1)
        if (dy, dz, dc) != (0, 0, 0)
    ]

    barrier = pltpu.get_barrier_semaphore()
    for peer in col_peers:
        pl.semaphore_signal(barrier, inc=1, device_id=(peer, c), device_id_type=MESH)
    for peer in row_peers:
        pl.semaphore_signal(barrier, inc=1, device_id=(r, peer), device_id_type=MESH)
    pl.semaphore_signal(barrier, inc=1, device_id=(from_row, from_col), device_id_type=MESH)

    small_copies = [
        pltpu.make_async_copy(src, dst, copy_sem.at[6 + k])
        for k, (src, dst) in enumerate(
            [
                (single_hbm, single_in),
                (rotation_hbm, rotation_in),
                (translation_hbm, translation_in),
                (index_hbm, index_in),
                (live_hbm, live_in),
                (head_hbm, head_in),
                (relpos_hbm, relpos),
                (gain_hbm, gain),
                (wb_hbm, wb_in),
                (wframe_hbm, wframe),
            ]
        )
    ]
    copies = [
        pltpu.make_async_copy(src, dst, copy_sem.at[k])
        for k, (src, dst) in enumerate(
            [
                (wsc_hbm, wsc_f),
                (wpt_hbm, wpt_f),
                (pair_hbm, pair_v),
                (wout_hbm, wout_f),
                (whid_hbm, whid_f),
                (wback_hbm, wback_f),
            ]
        )
    ]
    for cp in small_copies + copies:
        cp.start()
    for cp in small_copies:
        cp.wait()

    small[...] = jnp.zeros_like(small)
    entries = rotation_entries(rotation_in[0:1], rotation_in[1:2], rotation_in[2:3])
    for k, row in enumerate(
        entries
        + [translation_in[k : k + 1] for k in range(3)]
        + [index_in[...].astype(F32), jnp.where(live_in[...] == 1, 1.0, 0.0)]
    ):
        small[k : k + 1, 0:OWN] = row
    head = head_in[...]
    positive = jnp.maximum(head, 0.0) + jnp.log1p(jnp.exp(-jnp.abs(head)))
    small[14:15, 0:H] = positive * (math.sqrt(2.0 / (9.0 * PQ)) / 2.0)
    turned = small[...].T
    state_f[:, 0:D] = single_in[...]
    state_f[:, D:] = pad_lanes(jnp.concatenate([turned[0:OWN]] * 3, axis=1))

    def pack(single, frames):
        at = lane_iota(OWN)
        hi, mid = split2(frames)
        lo = (frames - hi.astype(F32) - mid.astype(F32)).astype(BF16)
        pieces = jnp.where(
            at < 16,
            hi.astype(F32),
            jnp.where(at < 32, mid.astype(F32), jnp.where(at < 48, lo.astype(F32), 0.0)),
        )
        return jnp.concatenate([single.astype(BF16), pieces.astype(BF16)], axis=1)

    def unpack(blocks):
        rows = blocks.astype(F32).reshape(blocks.shape[0] * OWN, SW)
        f = rows[:, D:]
        f = f + pltpu.roll(f, 112, 1) + pltpu.roll(f, 96, 1)
        return rows[:, :D].astype(BF16), f

    send_buf[0] = pack(state_f[:, 0:D], state_f[:, D:])

    lane = lane_iota(HP)
    head_row = lax.broadcasted_iota(jnp.int32, (HP, 128), 0)
    low = lane < 96
    owner = jnp.where(low, lax.rem(lane, 48) // PQ, lane - 96)
    own = (owner == head_row) & (lane < 96 + H)
    spread_scale = jnp.where(own, jnp.where(low, 8.0, -4.0), 0.0)
    gamma[...] = jnp.sum(
        jnp.broadcast_to(turned[0:HP, 14:15], (HP, 128)) * spread_scale, axis=0, keepdims=True
    )
    for t in range(2):
        own_scalar = (lane + 128 * t) // C == head_row
        hmask[:, 128 * t : 128 * t + 128] = jnp.where(own_scalar & (head_row < H), 1.0, 0.0)
    for t in range(2, 8):
        hmask[:, 128 * t : 128 * t + 128] = jnp.where(own & (head_row < H), 1.0, 0.0)

    with jax.named_scope("barrier"):
        pl.semaphore_wait(barrier, NC + NR - 1)

    def row_copy(it, peer, at):
        return pltpu.make_async_remote_copy(
            src_ref=send_buf.at[it],
            dst_ref=row_recv.at[it, at],
            send_sem=row_ss.at[peer],
            recv_sem=row_rs.at[it, at],
            device_id=(r, peer),
            device_id_type=MESH,
        )

    def swap_copy(it):
        return pltpu.make_async_remote_copy(
            src_ref=send_buf.at[it],
            dst_ref=swap_recv.at[it],
            send_sem=swap_ss,
            recv_sem=swap_rs.at[it],
            device_id=(to_row, to_col),
            device_id_type=MESH,
        )

    def col_copy(it, peer, at):
        return pltpu.make_async_remote_copy(
            src_ref=swap_recv.at[it],
            dst_ref=col_recv.at[it, at],
            send_sem=col_ss.at[peer],
            recv_sem=col_rs.at[it, at],
            device_id=(peer, c),
            device_id_type=MESH,
        )

    def idx_copy(peer, k, at):
        return pltpu.make_async_remote_copy(
            src_ref=row_recv.at[0, :, :, D:SW],
            dst_ref=idx_recv.at[at],
            send_sem=idx_ss.at[k],
            recv_sem=idx_rs.at[at],
            device_id=(peer, c),
            device_id_type=MESH,
        )

    idx_targets = (
        (diagonal, r + 1 - 2 * core),
        (diagonal & (c > 0), lax.rem(2 * c + 15, 16)),
        (diagonal & (c < NC - 1), lax.rem(2 * c + 2, 16)),
    )

    def send_numbers():
        for k, (needed, peer) in enumerate(idx_targets):

            @pl.when(needed)
            def _(k=k, peer=peer):
                idx_copy(peer, k, core).start()

        @pl.when(diagonal)
        def _():
            idx_recv[core] = row_recv[0, :, :, D:SW]

    def key_numbers():
        @pl.when(diagonal)
        def _():
            idx_copy(r, 0, 1 - core).wait_recv()

        @pl.when(near & jnp.logical_not(diagonal))
        def _():
            idx_copy(r, 0, 0).wait_recv()
            idx_copy(r, 0, 1).wait_recv()

        @pl.when(near)
        def _():
            f = idx_recv[...].astype(F32).reshape(COLS, 128)
            f = f + pltpu.roll(f, 112, 1) + pltpu.roll(f, 96, 1)
            key_idx[...] = column(f, 12)

        @pl.when(jnp.logical_not(near) & (c > r // 2))
        def _():
            key_idx[...] = jnp.full((COLS, 128), 1e6, F32)

        @pl.when(jnp.logical_not(near) & (c < r // 2))
        def _():
            key_idx[...] = jnp.full((COLS, 128), -1e6, F32)

    def top_copy(it, peer, at):
        return pltpu.make_async_remote_copy(
            src_ref=top_send.at[it, peer],
            dst_ref=top_recv.at[it, at],
            send_sem=top_ss.at[peer],
            recv_sem=top_rs.at[it, at],
            device_id=(r, peer),
            device_id_type=MESH,
        )

    def pair_copy(it, peer, at):
        return pltpu.make_async_remote_copy(
            src_ref=pair_send.at[it, peer],
            dst_ref=pair_recv.at[it, at],
            send_sem=pair_ss.at[peer],
            recv_sem=pair_rs.at[it, at],
            device_id=(r, peer),
            device_id_type=MESH,
        )

    def val_copy(it, peer, at):
        return pltpu.make_async_remote_copy(
            src_ref=val_send.at[it, peer],
            dst_ref=val_recv.at[it, at],
            send_sem=val_ss.at[peer],
            recv_sem=val_rs.at[it, at],
            device_id=(r, peer),
            device_id_type=MESH,
        )

    def start_exchange(it):
        swap_copy(it).start()
        for peer in row_peers:
            row_copy(it, peer, c).start()
        row_recv[it, c] = send_buf[it]

    def prepare_projection():
        for cp in copies[:2]:
            cp.wait()
        zeros64 = jnp.zeros((64, D), F32)
        zeros32 = jnp.zeros((32, D), F32)

        def place(block, rows):
            hi, mid = split2(rows.T)
            wp_hi[:, 128 * block : 128 * block + 128] = hi
            wp_mid[:, 128 * block : 128 * block + 128] = mid

        for g in range(3):
            at = g * H * C
            place(5 * g, wsc_f[at : at + 128])
            place(5 * g + 1, jnp.concatenate([wsc_f[at + 128 : at + 192], zeros64], axis=0))
            for a in range(3):
                if g < 2:
                    first = g * 144 + 48 * a
                    part = wpt_f[first : first + 48]
                    rows = jnp.concatenate([part, part, zeros32], axis=0)
                else:
                    rows = jnp.concatenate(
                        [wpt_f[288 + 96 * a : 384 + 96 * a], zeros32], axis=0
                    )
                place(5 * g + 2 + a, rows)

    def prepare_weights():
        for cp in copies[3:]:
            cp.wait()
        zeros64 = jnp.zeros((64, D), BF16)
        zeros32 = jnp.zeros((32, D), BF16)
        for part, (dst_mix, dst_loc) in enumerate(((wmix_hi, wloc_hi), (wmix_mid, wloc_mid))):
            for k in range(4):
                dst_mix[384 * k : 384 * k + 384] = split2(wout_f[576 + 384 * k : 960 + 384 * k])[
                    part
                ]
            dst_loc[0:192] = split2(wout_f[0:192])[part]
            dst_loc[192:256] = zeros64
            for k in range(4):
                at = 256 + 128 * k
                dst_loc[at : at + 96] = split2(wout_f[192 + 96 * k : 288 + 96 * k])[part]
                dst_loc[at + 96 : at + 128] = zeros32
        whid_hi[...], whid_mid[...] = split2(whid_f[...])
        wback_hi[...], wback_mid[...] = split2(wback_f[...])
        wfr_f[...] = jnp.zeros_like(wfr_f)
        wfr_f[0:6] = wframe[...]
        wfr_hi[...], wfr_mid[...] = split2(wfr_f[...].T)

    def to_global(f, y, width):
        comps = []
        x = [y[:, 128 * b : 128 * b + 128] for b in range(3)]
        keep = lane_iota(f.shape[0]) < width
        for a in range(3):
            g = (
                column(f, 3 * a) * x[0]
                + column(f, 3 * a + 1) * x[1]
                + column(f, 3 * a + 2) * x[2]
                + column(f, 9 + a)
            )
            comps.append(jnp.where(keep, g, 0.0))
        return comps

    def square_terms(comps):
        sq = comps[0] * comps[0] + comps[1] * comps[1] + comps[2] * comps[2]
        f = lax.broadcasted_iota(jnp.int32, (128, 128), 0)
        n = lax.broadcasted_iota(jnp.int32, (128, 128), 1)
        pick = jnp.where((f < 48) & (n == 96 + f // PQ), 1.0, 0.0).astype(BF16)
        hi, mid = split2(sq)
        lo = (sq - hi.astype(F32) - mid.astype(F32)).astype(BF16)
        total = (mm(hi, pick) + mm(mid, pick) + mm(lo, pick)) * gamma[...]
        hi, mid = split2(total)
        lo = (total - hi.astype(F32) - mid.astype(F32)).astype(BF16)
        return hi, mid, lo

    def query_features(it):
        s, f = unpack(row_recv[it])
        y = mm(s, wp_hi[:, :QW]) + mm(s, wp_mid[:, :QW])
        qf[:, 0:256] = y[:, :256]
        comps = to_global(f, y[:, 256:], 96)
        squares = square_terms(comps)
        lane = lane_iota(ROWS)
        for a in range(3):
            hi, mid = split2(comps[a] * gamma[...])
            ones = jnp.where(lane < 96 + H, 1.0, 0.0)
            qf[:, 256 + 128 * a : 384 + 128 * a] = jnp.where(lane < 96, hi.astype(F32), ones)
            qf[:, 640 + 128 * a : 768 + 128 * a] = jnp.where(
                lane < 48, mid.astype(F32), jnp.where(lane < 96, 0.0, squares[a].astype(F32))
            )

        mask = hmask[...]

        def spread(k, carry):
            for u in range(4):
                i = k * 4 + u
                row = jnp.broadcast_to(qf[pl.ds(i, 1), :], (HP, FW))
                at = pl.multiple_of(i * HP, HP)
                qmask[pl.ds(at, HP), :] = (row * mask).astype(BF16)
            return carry

        lax.fori_loop(0, ROWS // 4, spread, 0)

    def key_features(it):
        s, f = unpack(col_recv[it])
        y = mm(s, wp_hi[:, QW : 2 * QW]) + mm(s, wp_mid[:, QW : 2 * QW])
        kf[:, 0:256] = y[:, :256].astype(BF16)
        comps = to_global(f, y[:, 256:QW], 96)
        squares = square_terms(comps)
        lane = lane_iota(COLS)
        zero = jnp.zeros((COLS, 128), F32)
        for a in range(3):
            hi, mid = split2(comps[a])
            hi, mid = hi.astype(F32), mid.astype(F32)
            sq = squares[a].astype(F32)
            kf[:, 256 + 128 * a : 384 + 128 * a] = jnp.where(
                lane < 48, hi, jnp.where(lane < 96, mid, sq)
            ).astype(BF16)
            ones = jnp.where((lane >= 96) & (lane < 96 + H), 1.0, zero)
            kf[:, 640 + 128 * a : 768 + 128 * a] = jnp.where(lane < 48, hi, ones).astype(BF16)

    def value_features(it):
        s, f = unpack(col_recv[it])
        y = mm(s, wp_hi[:, 2 * QW :]) + mm(s, wp_mid[:, 2 * QW :])
        vcat[0:COLS, 0:256] = y[:, :256].astype(BF16)
        vcat[COLS:, 0:256] = jnp.zeros((COLS, 256), BF16)
        values = to_global(f, y[:, 256:], 96)
        for a in range(3):
            hi, mid = split2(values[a])
            at = 256 + 128 * a
            vcat[0:COLS, at : at + 128] = hi
            vcat[COLS:, at : at + 128] = mid

    def prepare_pair():
        copies[2].wait()
        fq = unpack(row_recv[0])[1]
        idx_b[0:ROWS] = column(fq, 12)
        idx_b[ROWS:] = column(fq, 13)
        key_index = key_idx[...]
        shape = (COLS, 128)
        lane = lax.broadcasted_iota(jnp.int32, shape, 1).astype(F32) - 64.0
        same = lax.broadcasted_iota(jnp.int32, shape, 0) == lax.broadcasted_iota(jnp.int32, shape, 1)
        table = relpos[...].astype(F32)
        hi, mid = split2(table - jnp.mean(table, axis=-1, keepdims=True))
        centre[0:128] = jnp.where(same, 1.0 - 1.0 / 128.0, -1.0 / 128.0).astype(BF16)
        centre[128:256] = hi
        centre[256:384] = mid
        wb_s[...] = jnp.zeros_like(wb_s)
        wb_s[0:H] = wb_in[...].astype(F32)
        project = wb_s[...].astype(BF16)
        gains = gain[...]
        step = 8

        def prepare(k, carry):
            first = k * step
            centres = []
            for u in range(step):
                offset = jnp.clip(key_index - idx_b[pl.ds(first + u, 1), :], -64.0, 63.0)
                onehot = jnp.where(offset == lane, 1.0, 0.0).astype(BF16)
                both = jnp.concatenate([pair_v[first + u], onehot, onehot], axis=1)
                centres.append(mm(both, centre[...]))
            for u in range(step):
                spread = jnp.mean(centres[u] * centres[u], axis=-1, keepdims=True)
                normed = (centres[u] * lax.rsqrt(spread + NORM_EPSILON) * gains).astype(BF16)
                pair_v[first + u] = normed
                bias = lax.dot_general(
                    project, normed, (((1,), (1,)), ((), ())), preferred_element_type=F32
                )
                live = idx_b[pl.ds(ROWS + first + u, 1), :] > 0.5
                at = pl.multiple_of((first + u) * HP, HP)
                bias_v[pl.ds(at, HP), :] = jnp.where(live, bias * THIRD, DEAD)
            return carry

        lax.fori_loop(0, ROWS // step, prepare, 0)

    def mask_keys():
        live = unpack(col_recv[0])[1].T[13:14, :] > 0.5
        for k in range(4):
            part = pl.ds(k * 256, 256)
            bias_v[part, :] = jnp.where(live, bias_v[part, :], DEAD)

    def attend(it):
        with jax.named_scope("logits"):
            keys = kf[...]
            rows = 256
            for k in range(ROWS * HP // rows):
                part = pl.ds(k * rows, rows)
                acc = lax.dot_general(
                    qmask[part, :], keys, (((1,), (1,)), ((), ())), preferred_element_type=F32
                )
                bias = bias_v[part, :]
                logits = jnp.where(bias > -1e38, acc * (THIRD / math.sqrt(C)) + bias, MASKED_LOGIT)
                top = jnp.max(logits, axis=-1, keepdims=True)
                p = jnp.exp(logits - top).astype(BF16)
                m_b[part, :] = jnp.broadcast_to(top, (rows, 128))
                total = jnp.sum(p.astype(F32), axis=-1, keepdims=True)
                s_b[part, :] = jnp.broadcast_to(total, (rows, 128))
                p_s[part, 0:128] = p
                p_s[part, 128:256] = p

        with jax.named_scope("pack"):
            lane = lane_iota(8)
            for g in range(NC):
                tile = jnp.zeros((8, 128), F32)
                for h in range(H):
                    src = pl.ds(8 * HP * g + h, 8, stride=HP)
                    tile = jnp.where(lane == h, m_b[src, :], tile)
                    tile = jnp.where(lane == HP + h, s_b[src, :], tile)
                top_send[it, g] = tile
            for peer in row_peers:
                top_copy(it, peer, c).start()
        with jax.named_scope("pairs"):
            for i in range(ROWS):
                part = pl.ds(i * HP, HP)
                pair_s[part, :] = mm(p_s[part, 0:128], pair_v[i])
            for h in range(H):
                pair_send[it, :, :, 128 * h : 128 * h + 128] = (
                    pair_s[pl.ds(h, ROWS, stride=HP), :].astype(BF16).reshape(NC, OWN, 128)
                )
            for peer in row_peers:
                pair_copy(it, peer, c).start()
        with jax.named_scope("values"):
            value_features(it)
        with jax.named_scope("sums"):
            values = vcat[...]
            for k in range(4):
                part = pl.ds(k * 256, 256)
                y = mm(p_s[part, :], values)
                for t in range(5):
                    r_s[t, part, :] = y[:, 128 * t : 128 * t + 128]
        with jax.named_scope("select"):
            for t in range(5):
                val_send[it, :, :, 128 * t : 128 * t + 128] = by_head(
                    t, ROWS, lambda h: r_s[t, pl.ds(h, ROWS, stride=HP), :]
                ).reshape(NC, OWN, 128)
            for peer in row_peers:
                val_copy(it, peer, c).start()
            top_recv[it, c] = top_send[it, c]
            pair_recv[it, c] = pair_send[it, c]
            val_recv[it, c] = val_send[it, c]

            @pl.when(it == 0)
            def _():
                prepare_weights()

    def by_head(t, rows, piece):
        if t == 0:
            heads, first, size = range(0, 8), 0, C
        elif t == 1:
            heads, first, size = range(8, 12), 8, C
        else:
            heads, first, size = range(0, H), 0, PV
        lane = lane_iota(rows)
        out = jnp.zeros((rows, 128), F32)
        for h in heads:
            lo = (h - first) * size
            out = jnp.where((lane >= lo) & (lane < lo + size), piece(h), out)
        return out

    def advance(it):
        with jax.named_scope("wait_top"):
            for peer in row_peers:
                top_copy(it, peer, peer).wait_recv()
        tops = [top_recv[it, k] for k in range(NC)]
        top = functools.reduce(jnp.maximum, tops)
        scales = [jnp.exp(t - top) for t in tops]
        total = scales[0] * pltpu.roll(tops[0], 128 - HP, 1)
        for k in range(1, NC):
            total = total + scales[k] * pltpu.roll(tops[k], 128 - HP, 1)
        inverse = 1.0 / jnp.where(lane_iota(OWN) < H, total, 1.0)
        factor = [[column(e * inverse, h) for h in range(H)] for e in scales]
        with jax.named_scope("wait_pair"):
            for peer in row_peers:
                pair_copy(it, peer, peer).wait_recv()
        pairs = []
        for h in range(H):
            at = pl.ds(128 * h, 128)
            out = factor[0][h] * pair_recv[it, 0, :, at].astype(F32)
            for k in range(1, NC):
                out = out + factor[k][h] * pair_recv[it, k, :, at].astype(F32)
            pairs.append(out)
        mixed = dot3(jnp.concatenate(pairs, axis=1), wmix_hi[...], wmix_mid[...])
        spread = [[by_head(t, OWN, lambda h: factor[k][h]) for t in range(3)] for k in range(NC)]
        with jax.named_scope("wait_val"):
            for peer in row_peers:
                val_copy(it, peer, peer).wait_recv()
        tiles = []
        for t in range(5):
            at = pl.ds(128 * t, 128)
            out = spread[0][min(t, 2)] * val_recv[it, 0, :, at]
            for k in range(1, NC):
                out = out + spread[k][min(t, 2)] * val_recv[it, k, :, at]
            tiles.append(out)
        frames = state_f[:, D:]
        single = state_f[:, :D]
        moved = [tiles[2 + a] - column(frames, 9 + a) for a in range(3)]
        local = [
            column(frames, a) * moved[0]
            + column(frames, 3 + a) * moved[1]
            + column(frames, 6 + a) * moved[2]
            for a in range(3)
        ]
        lengths = jnp.sqrt(
            local[0] * local[0] + local[1] * local[1] + local[2] * local[2] + NORM_FLOOR
        )
        keep = lane_iota(OWN) < H * PV
        feats = tiles[:2] + [jnp.where(keep, x, 0.0) for x in local + [lengths]]
        feats = jnp.concatenate(feats, axis=1)
        single = single + mixed + dot3(feats, wloc_hi[...], wloc_mid[...])
        single = layer_norm(single)
        hidden = jnp.maximum(dot3(single, whid_hi[...], whid_mid[...]), 0.0)
        single = layer_norm(single + dot3(hidden, wback_hi[...], wback_mid[...]))
        update = dot3(single, wfr_hi[...], wfr_mid[...])
        turn = rotation_entries(column(update, 0), column(update, 1), column(update, 2))
        rot = [column(frames, k) for k in range(9)]
        step = [column(update, 3 + k) for k in range(3)]
        new = [
            rot[3 * left] * turn[right]
            + rot[3 * left + 1] * turn[3 + right]
            + rot[3 * left + 2] * turn[6 + right]
            for left in range(3)
            for right in range(3)
        ] + [
            rot[3 * left] * step[0]
            + rot[3 * left + 1] * step[1]
            + rot[3 * left + 2] * step[2]
            + column(frames, 9 + left)
            for left in range(3)
        ]
        lane = lax.rem(lane_iota(OWN), 16)
        out = frames
        for k, value in enumerate(new):
            out = jnp.where(lane == k, value, out)
        return single, out

    def iteration(it, carry):
        with jax.named_scope("start"):
            start_exchange(it)

            @pl.when(it == 0)
            def _():
                prepare_projection()

        with jax.named_scope("wait_swap"):
            swap_copy(it).wait_recv()
        with jax.named_scope("send_col"):
            for peer in col_peers:
                col_copy(it, peer, slot).start()
            col_recv[it, slot] = swap_recv[it]

        with jax.named_scope("wait_row"):
            for peer in row_peers:
                row_copy(it, peer, peer).wait_recv()
        with jax.named_scope("query"):

            @pl.when(it == 0)
            def _():
                send_numbers()

            query_features(it)
        with jax.named_scope("prep_pair"):

            @pl.when(it == 0)
            def _():
                key_numbers()
                prepare_pair()

        with jax.named_scope("wait_col"):
            for peer in col_peers:
                col_copy(it, peer, slot_of(peer)).wait_recv()
        with jax.named_scope("key"):
            key_features(it)

            @pl.when(it == 0)
            def _():
                mask_keys()

        attend(it)
        with jax.named_scope("advance"):
            single, frames = advance(it)

            @pl.when(it < ITERS - 1)
            def _():
                send_buf[it + 1] = pack(single, frames)
                state_f[:, 0:D] = single
                state_f[:, D:] = frames

            @pl.when(it == ITERS - 1)
            def _():
                single_out[...] = single
                frames_out[...] = frames[:, 0:12]

        with jax.named_scope("wait_send"):
            swap_copy(it).wait_send()
            for peer in row_peers:
                row_copy(it, peer, c).wait_send()
                top_copy(it, peer, c).wait_send()
                pair_copy(it, peer, c).wait_send()
                val_copy(it, peer, c).wait_send()
            for peer in col_peers:
                col_copy(it, peer, slot).wait_send()
        return carry

    lax.fori_loop(0, ITERS, iteration, 0)
    for k, (needed, peer) in enumerate(idx_targets):

        @pl.when(needed)
        def _(k=k, peer=peer):
            idx_copy(peer, k, core).wait_send()


def hand_over(state, frames, state_out, frames_out):
    state_out[...] = state[...]
    frames_out[...] = frames[...]


def body(
    pair, relpos, pair_gain, bias_weight, single, rotation_params, translation, residue_index,
    residue_mask, w_scalar, w_points, head_weights, w_out, w_hidden, w_back, w_frame,
):
    vmem = pl.BlockSpec(memory_space=pltpu.VMEM)
    anyspace = pl.BlockSpec(memory_space=pl.ANY)
    V = pltpu.VMEM
    dma = pltpu.SemaphoreType.DMA
    scratch = [
        V((OWN, D), F32),
        V((3, OWN), F32),
        V((3, OWN), F32),
        V((1, OWN), jnp.int32),
        V((1, OWN), jnp.int32),
        V((1, H), F32),
        V((128, 128), BF16),
        V((1, 128), F32),
        V((H, 128), BF16),
        V((6, D), F32),
        V((ROWS, COLS, 128), BF16),
        V((ROWS * HP, 128), F32),
        V((576, D), F32),
        V((576, D), F32),
        V((2112, D), F32),
        V((D, D), F32),
        V((D, D), F32),
        V((128, D), F32),
        V((D, 3 * QW), BF16),
        V((D, 3 * QW), BF16),
        V((H * 128, D), BF16),
        V((H * 128, D), BF16),
        V((768, D), BF16),
        V((768, D), BF16),
        V((D, D), BF16),
        V((D, D), BF16),
        V((D, D), BF16),
        V((D, D), BF16),
        V((D, 128), BF16),
        V((D, 128), BF16),
        V((HP, 128), F32),
        V((HP, 128), F32),
        V((1, 128), F32),
        V((HP, FW), F32),
        V((3 * 128, 128), BF16),
        V((OWN, SW), F32),
        V((ITERS, OWN, SW), BF16),
        V((ITERS, NC, OWN, SW), BF16),
        V((ITERS, OWN, SW), BF16),
        V((ITERS, NR, OWN, SW), BF16),
        V((ITERS, NC, OWN, 128), F32),
        V((ITERS, NC, OWN, 128), F32),
        V((ITERS, NC, OWN, H * 128), BF16),
        V((ITERS, NC, OWN, H * 128), BF16),
        V((ITERS, NC, OWN, QW), F32),
        V((ITERS, NC, OWN, QW), F32),
        V((2, NC, OWN, 128), BF16),
        V((COLS, 128), F32),
        V((ROWS, FW), F32),
        V((ROWS * HP, FW), BF16),
        V((COLS, FW), BF16),
        V((2 * COLS, QW), BF16),
        V((2 * ROWS, 128), F32),
        V((ROWS * HP, 256), BF16),
        V((ROWS * HP, 128), F32),
        V((ROWS * HP, 128), F32),
        V((5, ROWS * HP, 128), F32),
        V((ROWS * HP, 128), F32),
        dma((16,)),
        dma((NC,)),
        dma((ITERS, NC)),
        dma,
        dma((ITERS,)),
        dma((NR,)),
        dma((ITERS, NR)),
        dma((NC,)),
        dma((ITERS, NC)),
        dma((NC,)),
        dma((ITERS, NC)),
        dma((NC,)),
        dma((ITERS, NC)),
        dma((3,)),
        dma((2,)),
    ]
    state, frames = pl.pallas_call(
        kernel,
        out_shape=(
            jax.ShapeDtypeStruct((OWN, D), F32),
            jax.ShapeDtypeStruct((OWN, 12), F32),
        ),
        in_specs=[anyspace] * 16,
        out_specs=(vmem, vmem),
        scratch_shapes=scratch,
        compiler_params=pltpu.CompilerParams(
            collective_id=0, has_side_effects=True, vmem_limit_bytes=62 * 1024 * 1024
        ),
        name="structure",
    )(
        single, rotation_params, translation, residue_index.reshape(1, OWN),
        residue_mask.reshape(1, OWN), head_weights.reshape(1, H), relpos,
        pair_gain.reshape(1, 128), bias_weight.T, w_frame.T,
        pair, w_scalar.T, w_points.T, w_out, w_hidden, w_back,
    )
    state, frames = pl.pallas_call(
        hand_over,
        out_shape=(
            jax.ShapeDtypeStruct((OWN, D), F32),
            jax.ShapeDtypeStruct((OWN, 12), F32),
        ),
        in_specs=[vmem, vmem],
        out_specs=(vmem, vmem),
        compiler_params=pltpu.CompilerParams(vmem_limit_bytes=62 * 1024 * 1024),
        name="hand_over",
    )(state, frames)
    return state, frames.T


def solution(mesh):
    placed = (
        P("row", "col", None),
        P(),
        P(),
        P(),
        P(("row", "col"), None),
        P(None, ("row", "col")),
        P(None, ("row", "col")),
        P(("row", "col")),
        P(("row", "col")),
        P(),
        P(),
        P(),
        P(),
        P(),
        P(),
        P(),
    )
    return jax.shard_map(
        body,
        mesh=mesh,
        in_specs=placed,
        out_specs=(P(("row", "col"), None), P(None, ("row", "col"))),
        check_vma=False,
    )
```

```python
import functools
import math

import jax
import jax.numpy as jnp
from jax import lax
from jax.experimental import pallas as pl
from jax.experimental.pallas import tpu as pltpu
from jax.sharding import PartitionSpec as P

H = 12
C = 16
PQ = 4
PV = 8
BINS = 128
ITERS = 3
D = 384
HP = 16
PITCH = 24
ROWS = 64
COLS = 128
OWN = 8
NR = 16
NC = 8
SW = 512
QW = 640
VW = 512
FW = 1024

NORM_EPSILON = 1e-05
MASKED_LOGIT = -100000.0
DEAD = -3e38
NORM_FLOOR = 0.1
THIRD = math.sqrt(1.0 / 3.0)
MESH = pl.DeviceIdType.MESH
F32 = jnp.float32
BF16 = jnp.bfloat16


def rotation_entries(b, c, d):
    inverse = 1.0 / (1.0 + b * b + c * c + d * d)
    entries = [
        1.0 + b * b - c * c - d * d,
        2.0 * (b * c - d),
        2.0 * (b * d + c),
        2.0 * (b * c + d),
        1.0 - b * b + c * c - d * d,
        2.0 * (c * d - b),
        2.0 * (b * d - c),
        2.0 * (c * d + b),
        1.0 - b * b - c * c + d * d,
    ]
    return [e * inverse for e in entries]


def layer_norm(values):
    center = values - jnp.mean(values, axis=-1, keepdims=True)
    spread = jnp.mean(center * center, axis=-1, keepdims=True)
    return center * lax.rsqrt(spread + NORM_EPSILON)


def split2(x):
    hi = x.astype(BF16)
    return hi, (x - hi.astype(F32)).astype(BF16)


def mm(a, b):
    return jnp.dot(a, b, preferred_element_type=F32)


def dot3(x, w_hi, w_mid):
    hi, mid = split2(x)
    n = x.shape[0]
    both = mm(jnp.concatenate([hi, mid], axis=0), w_hi)
    return both[:n] + both[n:] + mm(hi, w_mid)


def lane_iota(rows):
    return lax.broadcasted_iota(jnp.int32, (rows, 128), 1)


def pad_lanes(x):
    return jnp.concatenate([x, jnp.zeros((x.shape[0], 128 - x.shape[1]), x.dtype)], axis=1)


def column(x, k):
    return jnp.broadcast_to(x[:, k : k + 1], (x.shape[0], 128))


def kernel(
    single_hbm, rotation_hbm, translation_hbm, index_hbm, live_hbm, head_hbm, relpos_hbm, gain_hbm,
    wb_hbm, wframe_hbm, pair_hbm, wsc_hbm, wpt_hbm, wout_hbm, whid_hbm, wback_hbm,
    single_out, frames_out,
    single_in, rotation_in, translation_in, index_in, live_in, head_in, relpos, gain, wb_in, wframe,
    pair_v, bias_v, wsc_f, wpt_f, wout_f, whid_f, wback_f, wfr_f,
    wp_hi, wp_mid, wmix_hi, wmix_mid, wloc_hi, wloc_mid, whid_hi, whid_mid, wback_hi, wback_mid,
    wfr_hi, wfr_mid, wb_s, small, gamma, hmask, centre,
    state_f, send_buf, row_recv, swap_recv, col_recv, top_send, top_recv, pair_send, pair_recv,
    val_send, val_recv, idx_recv, key_idx,
    qf, qmask, kf, vcat, idx_b, p_s, m_b, s_b, r_s, pair_s,
    copy_sem, row_ss, row_rs, swap_ss, swap_rs, col_ss, col_rs, top_ss, top_rs,
    pair_ss, pair_rs, val_ss, val_rs, idx_ss, idx_rs,
):
    r = lax.axis_index("row")
    c = lax.axis_index("col")
    core = lax.rem(r, 2)
    z = lax.rem(r // 2, 4)
    y_hi = r // 8
    x = lax.rem(c, 4)
    y_lo = c // 4
    to_row = y_lo * 8 + lax.rem(x + 2, 4) * 2 + core
    to_col = y_hi * 4 + z
    from_row = y_lo * 8 + x * 2 + core
    from_col = y_hi * 4 + lax.rem(z + 2, 4)

    def slot_of(row):
        return lax.rem(row, 2) * 8 + (row // 8) * 4 + lax.rem(row // 2 + 2, 4)

    slot = slot_of(r)
    near = (r >= 2 * c - 1) & (r <= 2 * c + 2)
    diagonal = r // 2 == c

    row_peers = [
        lax.rem(y_lo + dy, 2) * 4 + lax.rem(x + dx, 4)
        for dy, dx in ((1, 2), (1, 1), (1, 3), (0, 2), (1, 0), (0, 1), (0, 3))
    ]
    col_peers = [
        lax.rem(y_hi + dy, 2) * 8 + lax.rem(z + dz, 4) * 2 + lax.rem(core + dc, 2)
        for dy, dz in ((1, 2), (1, 1), (1, 3), (1, 0), (0, 2), (0, 1), (0, 3), (0, 0))
        for dc in (0, 1)
        if (dy, dz, dc) != (0, 0, 0)
    ]

    barrier = pltpu.get_barrier_semaphore()
    for peer in col_peers:
        pl.semaphore_signal(barrier, inc=1, device_id=(peer, c), device_id_type=MESH)
    for peer in row_peers:
        pl.semaphore_signal(barrier, inc=1, device_id=(r, peer), device_id_type=MESH)
    pl.semaphore_signal(barrier, inc=1, device_id=(from_row, from_col), device_id_type=MESH)

    small_copies = [
        pltpu.make_async_copy(src, dst, copy_sem.at[6 + k])
        for k, (src, dst) in enumerate(
            [
                (single_hbm, single_in),
                (rotation_hbm, rotation_in),
                (translation_hbm, translation_in),
                (index_hbm, index_in),
                (live_hbm, live_in),
                (head_hbm, head_in),
                (relpos_hbm, relpos),
                (gain_hbm, gain),
                (wb_hbm, wb_in),
                (wframe_hbm, wframe),
            ]
        )
    ]
    copies = [
        pltpu.make_async_copy(src, dst, copy_sem.at[k])
        for k, (src, dst) in enumerate(
            [
                (wsc_hbm, wsc_f),
                (wpt_hbm, wpt_f),
                (pair_hbm, pair_v),
                (wout_hbm, wout_f),
                (whid_hbm, whid_f),
                (wback_hbm, wback_f),
            ]
        )
    ]
    for cp in small_copies + copies:
        cp.start()
    for cp in small_copies:
        cp.wait()

    small[...] = jnp.zeros_like(small)
    entries = rotation_entries(rotation_in[0:1], rotation_in[1:2], rotation_in[2:3])
    for k, row in enumerate(
        entries
        + [translation_in[k : k + 1] for k in range(3)]
        + [index_in[...].astype(F32), jnp.where(live_in[...] == 1, 1.0, 0.0)]
    ):
        small[k : k + 1, 0:OWN] = row
    head = head_in[...]
    positive = jnp.maximum(head, 0.0) + jnp.log1p(jnp.exp(-jnp.abs(head)))
    small[14:15, 0:H] = positive * (math.sqrt(2.0 / (9.0 * PQ)) / 2.0)
    turned = small[...].T
    state_f[:, 0:D] = single_in[...]
    state_f[:, D:] = pad_lanes(jnp.concatenate([turned[0:OWN]] * 3, axis=1))

    def pack(single, frames):
        at = lane_iota(OWN)
        hi, mid = split2(frames)
        lo = (frames - hi.astype(F32) - mid.astype(F32)).astype(BF16)
        pieces = jnp.where(
            at < 16,
            hi.astype(F32),
            jnp.where(at < 32, mid.astype(F32), jnp.where(at < 48, lo.astype(F32), 0.0)),
        )
        return jnp.concatenate([single.astype(BF16), pieces.astype(BF16)], axis=1)

    def unpack(blocks):
        rows = blocks.astype(F32).reshape(blocks.shape[0] * OWN, SW)
        f = rows[:, D:]
        f = f + pltpu.roll(f, 112, 1) + pltpu.roll(f, 96, 1)
        return rows[:, :D].astype(BF16), f

    send_buf[0] = pack(state_f[:, 0:D], state_f[:, D:])

    lane = lane_iota(HP)
    head_row = lax.broadcasted_iota(jnp.int32, (HP, 128), 0)
    low = lane < 96
    owner = jnp.where(low, lax.rem(lane, 48) // PQ, lane - 96)
    own = (owner == head_row) & (lane < 96 + H)
    spread_scale = jnp.where(own, jnp.where(low, 8.0, -4.0), 0.0)
    gamma[...] = jnp.sum(
        jnp.broadcast_to(turned[0:HP, 14:15], (HP, 128)) * spread_scale, axis=0, keepdims=True
    )
    for t in range(2):
        own_scalar = (lane + 128 * t) // C == head_row
        hmask[:, 128 * t : 128 * t + 128] = jnp.where(own_scalar & (head_row < H), 1.0, 0.0)
    for t in range(2, 8):
        hmask[:, 128 * t : 128 * t + 128] = jnp.where(own & (head_row < H), 1.0, 0.0)

    with jax.named_scope("barrier"):
        pl.semaphore_wait(barrier, NC + NR - 1)

    def row_copy(it, peer, at):
        return pltpu.make_async_remote_copy(
            src_ref=send_buf.at[it],
            dst_ref=row_recv.at[it, at],
            send_sem=row_ss.at[peer],
            recv_sem=row_rs.at[it, at],
            device_id=(r, peer),
            device_id_type=MESH,
        )

    def swap_copy(it):
        return pltpu.make_async_remote_copy(
            src_ref=send_buf.at[it],
            dst_ref=swap_recv.at[it],
            send_sem=swap_ss,
            recv_sem=swap_rs.at[it],
            device_id=(to_row, to_col),
            device_id_type=MESH,
        )

    def col_copy(it, peer, at):
        return pltpu.make_async_remote_copy(
            src_ref=swap_recv.at[it],
            dst_ref=col_recv.at[it, at],
            send_sem=col_ss.at[peer],
            recv_sem=col_rs.at[it, at],
            device_id=(peer, c),
            device_id_type=MESH,
        )

    def idx_copy(peer, k, at):
        return pltpu.make_async_remote_copy(
            src_ref=row_recv.at[0, :, :, D:SW],
            dst_ref=idx_recv.at[at],
            send_sem=idx_ss.at[k],
            recv_sem=idx_rs.at[at],
            device_id=(peer, c),
            device_id_type=MESH,
        )

    idx_targets = (
        (diagonal, r + 1 - 2 * core),
        (diagonal & (c > 0), lax.rem(2 * c + 15, 16)),
        (diagonal & (c < NC - 1), lax.rem(2 * c + 2, 16)),
    )

    def send_numbers():
        for k, (needed, peer) in enumerate(idx_targets):

            @pl.when(needed)
            def _(k=k, peer=peer):
                idx_copy(peer, k, core).start()

        @pl.when(diagonal)
        def _():
            idx_recv[core] = row_recv[0, :, :, D:SW]

    def key_numbers():
        @pl.when(diagonal)
        def _():
            idx_copy(r, 0, 1 - core).wait_recv()

        @pl.when(near & jnp.logical_not(diagonal))
        def _():
            idx_copy(r, 0, 0).wait_recv()
            idx_copy(r, 0, 1).wait_recv()

        @pl.when(near)
        def _():
            f = idx_recv[...].astype(F32).reshape(COLS, 128)
            f = f + pltpu.roll(f, 112, 1) + pltpu.roll(f, 96, 1)
            key_idx[...] = column(f, 12)

        @pl.when(jnp.logical_not(near) & (c > r // 2))
        def _():
            key_idx[...] = jnp.full((COLS, 128), 1e6, F32)

        @pl.when(jnp.logical_not(near) & (c < r // 2))
        def _():
            key_idx[...] = jnp.full((COLS, 128), -1e6, F32)

    def top_copy(it, peer, at):
        return pltpu.make_async_remote_copy(
            src_ref=top_send.at[it, peer],
            dst_ref=top_recv.at[it, at],
            send_sem=top_ss.at[peer],
            recv_sem=top_rs.at[it, at],
            device_id=(r, peer),
            device_id_type=MESH,
        )

    def pair_copy(it, peer, at):
        return pltpu.make_async_remote_copy(
            src_ref=pair_send.at[it, peer],
            dst_ref=pair_recv.at[it, at],
            send_sem=pair_ss.at[peer],
            recv_sem=pair_rs.at[it, at],
            device_id=(r, peer),
            device_id_type=MESH,
        )

    def val_copy(it, peer, at):
        return pltpu.make_async_remote_copy(
            src_ref=val_send.at[it, peer],
            dst_ref=val_recv.at[it, at],
            send_sem=val_ss.at[peer],
            recv_sem=val_rs.at[it, at],
            device_id=(r, peer),
            device_id_type=MESH,
        )

    def start_exchange(it):
        swap_copy(it).start()
        for peer in row_peers:
            row_copy(it, peer, c).start()
        row_recv[it, c] = send_buf[it]

    def prepare_projection():
        for cp in copies[:2]:
            cp.wait()
        zeros64 = jnp.zeros((64, D), F32)
        zeros32 = jnp.zeros((32, D), F32)

        def place(block, rows):
            hi, mid = split2(rows.T)
            wp_hi[:, 128 * block : 128 * block + 128] = hi
            wp_mid[:, 128 * block : 128 * block + 128] = mid

        for g in range(2):
            at = g * H * C
            place(5 * g, wsc_f[at : at + 128])
            place(5 * g + 1, jnp.concatenate([wsc_f[at + 128 : at + 192], zeros64], axis=0))
            for a in range(3):
                first = g * 144 + 48 * a
                part = wpt_f[first : first + 48]
                place(5 * g + 2 + a, jnp.concatenate([part, part, zeros32], axis=0))
        at = 2 * H * C
        for a in range(3):
            part = wsc_f[at + 32 * a : at + 32 * a + 32]
            place(10 + a, jnp.concatenate([wpt_f[288 + 96 * a : 384 + 96 * a], part], axis=0))
        place(13, jnp.concatenate([wsc_f[at + 96 : at + 192], zeros32], axis=0))

    def prepare_weights():
        for cp in copies[3:]:
            cp.wait()
        zeros32 = jnp.zeros((32, D), BF16)
        for part, (dst_mix, dst_loc) in enumerate(((wmix_hi, wloc_hi), (wmix_mid, wloc_mid))):
            for k in range(4):
                dst_mix[384 * k : 384 * k + 384] = split2(wout_f[576 + 384 * k : 960 + 384 * k])[
                    part
                ]
            for k in range(3):
                dst_loc[128 * k : 128 * k + 96] = split2(wout_f[192 + 96 * k : 288 + 96 * k])[part]
                dst_loc[128 * k + 96 : 128 * k + 128] = split2(wout_f[32 * k : 32 * k + 32])[part]
            dst_loc[384:480] = split2(wout_f[96:192])[part]
            dst_loc[480:512] = zeros32
            dst_loc[512:608] = split2(wout_f[480:576])[part]
            dst_loc[608:640] = zeros32
        whid_hi[...], whid_mid[...] = split2(whid_f[...])
        wback_hi[...], wback_mid[...] = split2(wback_f[...])
        wfr_f[...] = jnp.zeros_like(wfr_f)
        wfr_f[0:6] = wframe[...]
        wfr_hi[...], wfr_mid[...] = split2(wfr_f[...].T)

    def to_global(f, y, width):
        comps = []
        x = [y[:, 128 * b : 128 * b + 128] for b in range(3)]
        keep = lane_iota(f.shape[0]) < width
        for a in range(3):
            g = (
                column(f, 3 * a) * x[0]
                + column(f, 3 * a + 1) * x[1]
                + column(f, 3 * a + 2) * x[2]
                + column(f, 9 + a)
            )
            comps.append(jnp.where(keep, g, 0.0))
        return comps

    def square_terms(comps):
        sq = comps[0] * comps[0] + comps[1] * comps[1] + comps[2] * comps[2]
        f = lax.broadcasted_iota(jnp.int32, (128, 128), 0)
        n = lax.broadcasted_iota(jnp.int32, (128, 128), 1)
        pick = jnp.where((f < 48) & (n == 96 + f // PQ), 1.0, 0.0).astype(BF16)
        hi, mid = split2(sq)
        lo = (sq - hi.astype(F32) - mid.astype(F32)).astype(BF16)
        total = (mm(hi, pick) + mm(mid, pick) + mm(lo, pick)) * gamma[...]
        hi, mid = split2(total)
        lo = (total - hi.astype(F32) - mid.astype(F32)).astype(BF16)
        return hi, mid, lo

    def query_features(it):
        s, f = unpack(row_recv[it])
        y = mm(s, wp_hi[:, :QW]) + mm(s, wp_mid[:, :QW])
        qf[:, 0:256] = y[:, :256]
        comps = to_global(f, y[:, 256:], 96)
        squares = square_terms(comps)
        lane = lane_iota(ROWS)
        for a in range(3):
            hi, mid = split2(comps[a] * gamma[...])
            ones = jnp.where(lane < 96 + H, 1.0, 0.0)
            qf[:, 256 + 128 * a : 384 + 128 * a] = jnp.where(lane < 96, hi.astype(F32), ones)
            qf[:, 640 + 128 * a : 768 + 128 * a] = jnp.where(
                lane < 48, mid.astype(F32), jnp.where(lane < 96, 0.0, squares[a].astype(F32))
            )

        mask = hmask[...]

        def spread(k, carry):
            for u in range(4):
                i = k * 4 + u
                row = jnp.broadcast_to(qf[pl.ds(i, 1), :], (HP, FW))
                at = pl.multiple_of(i * HP, HP)
                qmask[pl.ds(at, HP), :] = (row * mask).astype(BF16)
            return carry

        lax.fori_loop(0, ROWS // 4, spread, 0)

    def key_features(it):
        s, f = unpack(col_recv[it])
        y = mm(s, wp_hi[:, QW : 2 * QW]) + mm(s, wp_mid[:, QW : 2 * QW])
        kf[:, 0:256] = y[:, :256].astype(BF16)
        comps = to_global(f, y[:, 256:QW], 96)
        squares = square_terms(comps)
        lane = lane_iota(COLS)
        zero = jnp.zeros((COLS, 128), F32)
        for a in range(3):
            hi, mid = split2(comps[a])
            hi, mid = hi.astype(F32), mid.astype(F32)
            sq = squares[a].astype(F32)
            kf[:, 256 + 128 * a : 384 + 128 * a] = jnp.where(
                lane < 48, hi, jnp.where(lane < 96, mid, sq)
            ).astype(BF16)
            ones = jnp.where((lane >= 96) & (lane < 96 + H), 1.0, zero)
            kf[:, 640 + 128 * a : 768 + 128 * a] = jnp.where(lane < 48, hi, ones).astype(BF16)

    def value_features(it):
        s, f = unpack(col_recv[it])
        y = mm(s, wp_hi[:, 2 * QW :]) + mm(s, wp_mid[:, 2 * QW :])
        values = to_global(f, y, 96)
        lane = lane_iota(COLS)
        for a in range(3):
            at = 128 * a
            hi, mid = split2(jnp.where(lane < 96, values[a], y[:, at : at + 128]))
            vcat[0:COLS, at : at + 128] = hi
            vcat[COLS:, at : at + 128] = jnp.where(lane < 96, mid.astype(F32), 0.0).astype(BF16)
        vcat[0:COLS, 384:512] = y[:, 384:512].astype(BF16)
        vcat[COLS:, 384:512] = jnp.zeros((COLS, 128), BF16)

    def prepare_pair():
        copies[2].wait()
        fq = unpack(row_recv[0])[1]
        idx_b[0:ROWS] = column(fq, 12)
        idx_b[ROWS:] = column(fq, 13)
        key_index = key_idx[...]
        shape = (COLS, 128)
        lane = lax.broadcasted_iota(jnp.int32, shape, 1).astype(F32) - 64.0
        same = lax.broadcasted_iota(jnp.int32, shape, 0) == lax.broadcasted_iota(jnp.int32, shape, 1)
        table = relpos[...].astype(F32)
        hi, mid = split2(table - jnp.mean(table, axis=-1, keepdims=True))
        centre[0:128] = jnp.where(same, 1.0 - 1.0 / 128.0, -1.0 / 128.0).astype(BF16)
        centre[128:256] = hi
        centre[256:384] = mid
        wb_s[...] = jnp.zeros_like(wb_s)
        wb_s[0:H] = wb_in[...].astype(F32)
        project = wb_s[...].astype(BF16)
        gains = gain[...]
        step = 8

        def prepare(k, carry):
            first = k * step
            centres = []
            for u in range(step):
                offset = jnp.clip(key_index - idx_b[pl.ds(first + u, 1), :], -64.0, 63.0)
                onehot = jnp.where(offset == lane, 1.0, 0.0).astype(BF16)
                both = jnp.concatenate([pair_v[first + u], onehot, onehot], axis=1)
                centres.append(mm(both, centre[...]))
            for u in range(step):
                spread = jnp.mean(centres[u] * centres[u], axis=-1, keepdims=True)
                normed = (centres[u] * lax.rsqrt(spread + NORM_EPSILON) * gains).astype(BF16)
                pair_v[first + u] = normed
                bias = lax.dot_general(
                    project, normed, (((1,), (1,)), ((), ())), preferred_element_type=F32
                )
                live = idx_b[pl.ds(ROWS + first + u, 1), :] > 0.5
                at = pl.multiple_of((first + u) * HP, HP)
                bias_v[pl.ds(at, HP), :] = jnp.where(live, bias * THIRD, DEAD)
            return carry

        lax.fori_loop(0, ROWS // step, prepare, 0)

    def mask_keys():
        live = unpack(col_recv[0])[1].T[13:14, :] > 0.5
        for k in range(4):
            part = pl.ds(k * 256, 256)
            bias_v[part, :] = jnp.where(live, bias_v[part, :], DEAD)

    def store_queries(ref, first, rows):
        for k in range(rows.shape[0] // HP):
            ref[pl.ds((first + k) * PITCH, HP), :] = rows[HP * k : HP * k + HP]

    def attend(it):
        with jax.named_scope("logits"):
            keys = kf[...]
            rows = 256
            for k in range(ROWS * HP // rows):
                part = pl.ds(k * rows, rows)
                acc = lax.dot_general(
                    qmask[part, :], keys, (((1,), (1,)), ((), ())), preferred_element_type=F32
                )
                bias = bias_v[part, :]
                logits = jnp.where(bias > -1e38, acc * (THIRD / math.sqrt(C)) + bias, MASKED_LOGIT)
                top = jnp.max(logits, axis=-1, keepdims=True)
                p = jnp.exp(logits - top).astype(BF16)
                top = jnp.broadcast_to(top, (rows, 128))
                total = jnp.sum(p.astype(F32), axis=-1, keepdims=True)
                total = jnp.broadcast_to(total, (rows, 128))
                store_queries(m_b, k * rows // HP, top)
                store_queries(s_b, k * rows // HP, total)
                p_s[part, 0:128] = p
                p_s[part, 128:256] = p

        with jax.named_scope("pack"):
            lane = lane_iota(8)
            place = jnp.where(lane < 96, lax.rem(lane, 32), -1)
            for g in range(NC):
                tile = jnp.zeros((8, 128), F32)
                for h in range(H):
                    src = pl.ds(8 * PITCH * g + h, 8, stride=PITCH)
                    tile = jnp.where(place == h, m_b[src, :], tile)
                    tile = jnp.where(place == HP + h, s_b[src, :], tile)
                hi, mid = split2(tile)
                lo = tile - hi.astype(F32) - mid.astype(F32)
                tile = jnp.where(
                    lane < 32, hi.astype(F32), jnp.where(lane < 64, mid.astype(F32), lo)
                )
                top_send[it, g] = tile.astype(BF16)
            for peer in row_peers:
                top_copy(it, peer, c).start()
        with jax.named_scope("pairs"):
            for i in range(ROWS):
                part = pl.ds(i * HP, HP)
                store_queries(pair_s, i, mm(p_s[part, 0:128], pair_v[i]))
            for h in range(H):
                pair_send[it, :, :, 128 * h : 128 * h + 128] = (
                    pair_s[pl.ds(h, ROWS, stride=PITCH), :].astype(BF16).reshape(NC, OWN, 128)
                )
            for peer in row_peers:
                pair_copy(it, peer, c).start()
        with jax.named_scope("values"):
            value_features(it)
        with jax.named_scope("sums"):
            values = vcat[...]
            for k in range(4):
                part = pl.ds(k * 256, 256)
                y = mm(p_s[part, :], values)
                for t in range(4):
                    store_queries(r_s.at[t], 16 * k, y[:, 128 * t : 128 * t + 128])
        with jax.named_scope("select"):
            for t in range(4):
                val_send[it, :, :, 128 * t : 128 * t + 128] = by_head(
                    t, ROWS, lambda h: r_s[t, pl.ds(h, ROWS, stride=PITCH), :]
                ).reshape(NC, OWN, 128)
            for peer in row_peers:
                val_copy(it, peer, c).start()
            top_recv[it, c] = top_send[it, c]
            pair_recv[it, c] = pair_send[it, c]
            val_recv[it, c] = val_send[it, c]

            @pl.when(it == 0)
            def _():
                prepare_weights()

    def by_head(t, rows, piece):
        spans = [(h, PV * h, PV) for h in range(H)] if t < 3 else []
        at, heads = (96, range(2 * t, 2 * t + 2)) if t < 3 else (0, range(6, H))
        spans += [(h, at + C * (h - heads[0]), C) for h in heads]
        lane = lane_iota(rows)
        out = jnp.zeros((rows, 128), F32)
        for h, lo, size in spans:
            out = jnp.where((lane >= lo) & (lane < lo + size), piece(h), out)
        return out

    def advance(it):
        with jax.named_scope("wait_top"):
            for peer in row_peers:
                top_copy(it, peer, peer).wait_recv()
        tops = []
        for k in range(NC):
            tile = top_recv[it, k].astype(F32)
            tops.append(tile + pltpu.roll(tile, 96, 1) + pltpu.roll(tile, 64, 1))
        top = functools.reduce(jnp.maximum, tops)
        scales = [jnp.exp(t - top) for t in tops]
        total = scales[0] * pltpu.roll(tops[0], 128 - HP, 1)
        for k in range(1, NC):
            total = total + scales[k] * pltpu.roll(tops[k], 128 - HP, 1)
        inverse = 1.0 / jnp.where(lane_iota(OWN) < H, total, 1.0)
        factor = [[column(e * inverse, h) for h in range(H)] for e in scales]
        with jax.named_scope("wait_pair"):
            for peer in row_peers:
                pair_copy(it, peer, peer).wait_recv()
        pairs = []
        for h in range(H):
            at = pl.ds(128 * h, 128)
            out = factor[0][h] * pair_recv[it, 0, :, at].astype(F32)
            for k in range(1, NC):
                out = out + factor[k][h] * pair_recv[it, k, :, at].astype(F32)
            pairs.append(out)
        mixed = dot3(jnp.concatenate(pairs, axis=1), wmix_hi[...], wmix_mid[...])
        spread = [[by_head(t, OWN, lambda h: factor[k][h]) for t in range(4)] for k in range(NC)]
        with jax.named_scope("wait_val"):
            for peer in row_peers:
                val_copy(it, peer, peer).wait_recv()
        tiles = []
        for t in range(4):
            at = pl.ds(128 * t, 128)
            out = spread[0][t] * val_recv[it, 0, :, at]
            for k in range(1, NC):
                out = out + spread[k][t] * val_recv[it, k, :, at]
            tiles.append(out)
        frames = state_f[:, D:]
        single = state_f[:, :D]
        moved = [tiles[a] - column(frames, 9 + a) for a in range(3)]
        local = [
            column(frames, a) * moved[0]
            + column(frames, 3 + a) * moved[1]
            + column(frames, 6 + a) * moved[2]
            for a in range(3)
        ]
        lengths = jnp.sqrt(
            local[0] * local[0] + local[1] * local[1] + local[2] * local[2] + NORM_FLOOR
        )
        keep = lane_iota(OWN) < H * PV
        feats = [jnp.where(keep, local[a], tiles[a]) for a in range(3)]
        feats += [tiles[3], jnp.where(keep, lengths, 0.0)]
        feats = jnp.concatenate(feats, axis=1)
        single = single + mixed + dot3(feats, wloc_hi[...], wloc_mid[...])
        single = layer_norm(single)
        hidden = jnp.maximum(dot3(single, whid_hi[...], whid_mid[...]), 0.0)
        single = layer_norm(single + dot3(hidden, wback_hi[...], wback_mid[...]))
        update = dot3(single, wfr_hi[...], wfr_mid[...])
        turn = rotation_entries(column(update, 0), column(update, 1), column(update, 2))
        rot = [column(frames, k) for k in range(9)]
        step = [column(update, 3 + k) for k in range(3)]
        new = [
            rot[3 * left] * turn[right]
            + rot[3 * left + 1] * turn[3 + right]
            + rot[3 * left + 2] * turn[6 + right]
            for left in range(3)
            for right in range(3)
        ] + [
            rot[3 * left] * step[0]
            + rot[3 * left + 1] * step[1]
            + rot[3 * left + 2] * step[2]
            + column(frames, 9 + left)
            for left in range(3)
        ]
        lane = lax.rem(lane_iota(OWN), 16)
        out = frames
        for k, value in enumerate(new):
            out = jnp.where(lane == k, value, out)
        return single, out

    def iteration(it, carry):
        with jax.named_scope("start"):
            start_exchange(it)

            @pl.when(it == 0)
            def _():
                prepare_projection()

        with jax.named_scope("wait_swap"):
            swap_copy(it).wait_recv()
        with jax.named_scope("send_col"):
            for peer in col_peers:
                col_copy(it, peer, slot).start()
            col_recv[it, slot] = swap_recv[it]

        with jax.named_scope("wait_row"):
            for peer in row_peers:
                row_copy(it, peer, peer).wait_recv()
        with jax.named_scope("query"):

            @pl.when(it == 0)
            def _():
                send_numbers()

            query_features(it)
        with jax.named_scope("prep_pair"):

            @pl.when(it == 0)
            def _():
                key_numbers()
                prepare_pair()

        with jax.named_scope("wait_col"):
            for peer in col_peers:
                col_copy(it, peer, slot_of(peer)).wait_recv()
        with jax.named_scope("key"):
            key_features(it)

            @pl.when(it == 0)
            def _():
                mask_keys()

        attend(it)
        with jax.named_scope("advance"):
            single, frames = advance(it)

            @pl.when(it < ITERS - 1)
            def _():
                send_buf[it + 1] = pack(single, frames)
                state_f[:, 0:D] = single
                state_f[:, D:] = frames

            @pl.when(it == ITERS - 1)
            def _():
                single_out[...] = single
                frames_out[...] = frames[:, 0:12]

        with jax.named_scope("wait_send"):
            swap_copy(it).wait_send()
            for peer in row_peers:
                row_copy(it, peer, c).wait_send()
                top_copy(it, peer, c).wait_send()
                pair_copy(it, peer, c).wait_send()
                val_copy(it, peer, c).wait_send()
            for peer in col_peers:
                col_copy(it, peer, slot).wait_send()
        return carry

    lax.fori_loop(0, ITERS, iteration, 0)
    for k, (needed, peer) in enumerate(idx_targets):

        @pl.when(needed)
        def _(k=k, peer=peer):
            idx_copy(peer, k, core).wait_send()


def hand_over(state, frames, state_out, frames_out):
    state_out[...] = state[...]
    frames_out[...] = frames[...]


def body(
    pair, relpos, pair_gain, bias_weight, single, rotation_params, translation, residue_index,
    residue_mask, w_scalar, w_points, head_weights, w_out, w_hidden, w_back, w_frame,
):
    vmem = pl.BlockSpec(memory_space=pltpu.VMEM)
    anyspace = pl.BlockSpec(memory_space=pl.ANY)
    V = pltpu.VMEM
    dma = pltpu.SemaphoreType.DMA
    scratch = [
        V((OWN, D), F32),
        V((3, OWN), F32),
        V((3, OWN), F32),
        V((1, OWN), jnp.int32),
        V((1, OWN), jnp.int32),
        V((1, H), F32),
        V((128, 128), BF16),
        V((1, 128), F32),
        V((H, 128), BF16),
        V((6, D), F32),
        V((ROWS, COLS, 128), BF16),
        V((ROWS * HP, 128), F32),
        V((576, D), F32),
        V((576, D), F32),
        V((2112, D), F32),
        V((D, D), F32),
        V((D, D), F32),
        V((128, D), F32),
        V((D, 2 * QW + VW), BF16),
        V((D, 2 * QW + VW), BF16),
        V((H * 128, D), BF16),
        V((H * 128, D), BF16),
        V((QW, D), BF16),
        V((QW, D), BF16),
        V((D, D), BF16),
        V((D, D), BF16),
        V((D, D), BF16),
        V((D, D), BF16),
        V((D, 128), BF16),
        V((D, 128), BF16),
        V((HP, 128), F32),
        V((HP, 128), F32),
        V((1, 128), F32),
        V((HP, FW), F32),
        V((3 * 128, 128), BF16),
        V((OWN, SW), F32),
        V((ITERS, OWN, SW), BF16),
        V((ITERS, NC, OWN, SW), BF16),
        V((ITERS, OWN, SW), BF16),
        V((ITERS, NR, OWN, SW), BF16),
        V((ITERS, NC, OWN, 128), BF16),
        V((ITERS, NC, OWN, 128), BF16),
        V((ITERS, NC, OWN, H * 128), BF16),
        V((ITERS, NC, OWN, H * 128), BF16),
        V((ITERS, NC, OWN, VW), F32),
        V((ITERS, NC, OWN, VW), F32),
        V((2, NC, OWN, 128), BF16),
        V((COLS, 128), F32),
        V((ROWS, FW), F32),
        V((ROWS * HP, FW), BF16),
        V((COLS, FW), BF16),
        V((2 * COLS, VW), BF16),
        V((2 * ROWS, 128), F32),
        V((ROWS * HP, 256), BF16),
        V((ROWS * PITCH, 128), F32),
        V((ROWS * PITCH, 128), F32),
        V((4, ROWS * PITCH, 128), F32),
        V((ROWS * PITCH, 128), F32),
        dma((16,)),
        dma((NC,)),
        dma((ITERS, NC)),
        dma,
        dma((ITERS,)),
        dma((NR,)),
        dma((ITERS, NR)),
        dma((NC,)),
        dma((ITERS, NC)),
        dma((NC,)),
        dma((ITERS, NC)),
        dma((NC,)),
        dma((ITERS, NC)),
        dma((3,)),
        dma((2,)),
    ]
    state, frames = pl.pallas_call(
        kernel,
        out_shape=(
            jax.ShapeDtypeStruct((OWN, D), F32),
            jax.ShapeDtypeStruct((OWN, 12), F32),
        ),
        in_specs=[anyspace] * 16,
        out_specs=(vmem, vmem),
        scratch_shapes=scratch,
        compiler_params=pltpu.CompilerParams(
            collective_id=0, has_side_effects=True, vmem_limit_bytes=62 * 1024 * 1024
        ),
        name="structure",
    )(
        single, rotation_params, translation, residue_index.reshape(1, OWN),
        residue_mask.reshape(1, OWN), head_weights.reshape(1, H), relpos,
        pair_gain.reshape(1, 128), bias_weight.T, w_frame.T,
        pair, w_scalar.T, w_points.T, w_out, w_hidden, w_back,
    )
    state, frames = pl.pallas_call(
        hand_over,
        out_shape=(
            jax.ShapeDtypeStruct((OWN, D), F32),
            jax.ShapeDtypeStruct((OWN, 12), F32),
        ),
        in_specs=[vmem, vmem],
        out_specs=(vmem, vmem),
        compiler_params=pltpu.CompilerParams(vmem_limit_bytes=62 * 1024 * 1024),
        name="hand_over",
    )(state, frames)
    return state, frames.T


def solution(mesh):
    placed = (
        P("row", "col", None),
        P(),
        P(),
        P(),
        P(("row", "col"), None),
        P(None, ("row", "col")),
        P(None, ("row", "col")),
        P(("row", "col")),
        P(("row", "col")),
        P(),
        P(),
        P(),
        P(),
        P(),
        P(),
        P(),
    )
    return jax.shard_map(
        body,
        mesh=mesh,
        in_specs=placed,
        out_specs=(P(("row", "col"), None), P(None, ("row", "col"))),
        check_vma=False,
    )
```

```python
import functools
import math

import jax
import jax.numpy as jnp
from jax import lax
from jax.experimental import pallas as pl
from jax.experimental.pallas import tpu as pltpu
from jax.sharding import PartitionSpec as P

H = 12
C = 16
PQ = 4
PV = 8
BINS = 128
ITERS = 3
D = 384
HP = 16
PITCH = 24
ROWS = 64
COLS = 128
OWN = 8
NR = 16
NC = 8
SW = 512
QW = 640
VW = 512
FW = 1024

NORM_EPSILON = 1e-05
MASKED_LOGIT = -100000.0
DEAD = -3e38
NORM_FLOOR = 0.1
THIRD = math.sqrt(1.0 / 3.0)
MESH = pl.DeviceIdType.MESH
F32 = jnp.float32
BF16 = jnp.bfloat16


def rotation_entries(b, c, d):
    inverse = 1.0 / (1.0 + b * b + c * c + d * d)
    entries = [
        1.0 + b * b - c * c - d * d,
        2.0 * (b * c - d),
        2.0 * (b * d + c),
        2.0 * (b * c + d),
        1.0 - b * b + c * c - d * d,
        2.0 * (c * d - b),
        2.0 * (b * d - c),
        2.0 * (c * d + b),
        1.0 - b * b - c * c + d * d,
    ]
    return [e * inverse for e in entries]


def layer_norm(values):
    center = values - jnp.mean(values, axis=-1, keepdims=True)
    spread = jnp.mean(center * center, axis=-1, keepdims=True)
    return center * lax.rsqrt(spread + NORM_EPSILON)


def split2(x):
    hi = x.astype(BF16)
    return hi, (x - hi.astype(F32)).astype(BF16)


def mm(a, b):
    return jnp.dot(a, b, preferred_element_type=F32)


def dot3(x, w_hi, w_mid):
    hi, mid = split2(x)
    n = x.shape[0]
    both = mm(jnp.concatenate([hi, mid], axis=0), w_hi)
    return both[:n] + both[n:] + mm(hi, w_mid)


def lane_iota(rows):
    return lax.broadcasted_iota(jnp.int32, (rows, 128), 1)


def pad_lanes(x):
    return jnp.concatenate([x, jnp.zeros((x.shape[0], 128 - x.shape[1]), x.dtype)], axis=1)


def column(x, k):
    return jnp.broadcast_to(x[:, k : k + 1], (x.shape[0], 128))


def kernel(
    single_hbm, rotation_hbm, translation_hbm, index_hbm, live_hbm, head_hbm, relpos_hbm, gain_hbm,
    wb_hbm, wframe_hbm, pair_hbm, wsc_hbm, wpt_hbm, wout_hbm, whid_hbm, wback_hbm,
    single_out, frames_out,
    single_in, rotation_in, translation_in, index_in, live_in, head_in, relpos, gain, wb_in, wframe,
    pair_v, bias_v, wsc_f, wpt_f, wout_f, whid_f, wback_f, wfr_f,
    wp_hi, wp_mid, wmix_hi, wmix_mid, wloc_hi, wloc_mid, whid_hi, whid_mid, wback_hi, wback_mid,
    wfr_hi, wfr_mid, wb_s, small, gamma, hmask, centre,
    state_f, send_buf, row_recv, swap_recv, col_recv, top_send, top_recv, pair_send, pair_recv,
    val_send, val_recv, idx_recv, key_idx,
    qf, qmask, kf, vcat, idx_b, p_s, m_b, s_b, r_s, pair_s,
    copy_sem, row_ss, row_rs, swap_ss, swap_rs, col_ss, col_rs, top_ss, top_rs,
    pair_ss, pair_rs, val_ss, val_rs, idx_ss, idx_rs, far_ss,
):
    r = lax.axis_index("row")
    c = lax.axis_index("col")
    core = lax.rem(r, 2)
    z = lax.rem(r // 2, 4)
    y_hi = r // 8
    x = lax.rem(c, 4)
    y_lo = c // 4
    to_row = y_lo * 8 + lax.rem(x + 2, 4) * 2 + core
    to_col = y_hi * 4 + z
    from_row = y_lo * 8 + x * 2 + core
    from_col = y_hi * 4 + lax.rem(z + 2, 4)

    far_rows = [(1 - y_lo) * 8 + x * 2 + k for k in (0, 1)]
    far_sources = [(y_lo * 8 + x * 2 + k, (1 - y_hi) * 4 + z) for k in (0, 1)]

    def slot_of(row):
        return lax.rem(row, 2) * 8 + (row // 8) * 4 + lax.rem(row // 2 + 2, 4)

    slot = slot_of(r)
    near = (r >= 2 * c - 1) & (r <= 2 * c + 2)
    diagonal = r // 2 == c

    row_peers = [
        lax.rem(y_lo + dy, 2) * 4 + lax.rem(x + dx, 4)
        for dy, dx in ((1, 2), (1, 1), (1, 3), (0, 2), (1, 0), (0, 1), (0, 3))
    ]
    col_peers = [
        lax.rem(y_hi + dy, 2) * 8 + lax.rem(z + dz, 4) * 2 + lax.rem(core + dc, 2)
        for dy, dz in ((1, 2), (1, 1), (1, 3), (1, 0), (0, 2), (0, 1), (0, 3), (0, 0))
        for dc in (0, 1)
        if (dy, dz, dc) != (0, 0, 0)
    ]
    served = col_peers[2:]

    barrier = pltpu.get_barrier_semaphore()
    for peer in col_peers:
        pl.semaphore_signal(barrier, inc=1, device_id=(peer, c), device_id_type=MESH)
    for peer in row_peers:
        pl.semaphore_signal(barrier, inc=1, device_id=(r, peer), device_id_type=MESH)
    pl.semaphore_signal(barrier, inc=1, device_id=(from_row, from_col), device_id_type=MESH)
    for peer in far_sources:
        pl.semaphore_signal(barrier, inc=1, device_id=peer, device_id_type=MESH)

    small_copies = [
        pltpu.make_async_copy(src, dst, copy_sem.at[6 + k])
        for k, (src, dst) in enumerate(
            [
                (single_hbm, single_in),
                (rotation_hbm, rotation_in),
                (translation_hbm, translation_in),
                (index_hbm, index_in),
                (live_hbm, live_in),
                (head_hbm, head_in),
                (relpos_hbm, relpos),
                (gain_hbm, gain),
                (wb_hbm, wb_in),
                (wframe_hbm, wframe),
            ]
        )
    ]
    copies = [
        pltpu.make_async_copy(src, dst, copy_sem.at[k])
        for k, (src, dst) in enumerate(
            [
                (wsc_hbm, wsc_f),
                (wpt_hbm, wpt_f),
                (pair_hbm, pair_v),
                (wout_hbm, wout_f),
                (whid_hbm, whid_f),
                (wback_hbm, wback_f),
            ]
        )
    ]
    for cp in small_copies + copies:
        cp.start()
    for cp in small_copies:
        cp.wait()

    small[...] = jnp.zeros_like(small)
    entries = rotation_entries(rotation_in[0:1], rotation_in[1:2], rotation_in[2:3])
    for k, row in enumerate(
        entries
        + [translation_in[k : k + 1] for k in range(3)]
        + [index_in[...].astype(F32), jnp.where(live_in[...] == 1, 1.0, 0.0)]
    ):
        small[k : k + 1, 0:OWN] = row
    head = head_in[...]
    positive = jnp.maximum(head, 0.0) + jnp.log1p(jnp.exp(-jnp.abs(head)))
    small[14:15, 0:H] = positive * (math.sqrt(2.0 / (9.0 * PQ)) / 2.0)
    turned = small[...].T
    state_f[:, 0:D] = single_in[...]
    state_f[:, D:] = pad_lanes(jnp.concatenate([turned[0:OWN]] * 3, axis=1))

    def pack(single, frames):
        at = lane_iota(OWN)
        hi, mid = split2(frames)
        lo = (frames - hi.astype(F32) - mid.astype(F32)).astype(BF16)
        pieces = jnp.where(
            at < 16,
            hi.astype(F32),
            jnp.where(at < 32, mid.astype(F32), jnp.where(at < 48, lo.astype(F32), 0.0)),
        )
        return jnp.concatenate([single.astype(BF16), pieces.astype(BF16)], axis=1)

    def unpack(blocks):
        rows = blocks.astype(F32).reshape(blocks.shape[0] * OWN, SW)
        f = rows[:, D:]
        f = f + pltpu.roll(f, 112, 1) + pltpu.roll(f, 96, 1)
        return rows[:, :D].astype(BF16), f

    send_buf[0] = pack(state_f[:, 0:D], state_f[:, D:])

    lane = lane_iota(HP)
    head_row = lax.broadcasted_iota(jnp.int32, (HP, 128), 0)
    low = lane < 96
    owner = jnp.where(low, lax.rem(lane, 48) // PQ, lane - 96)
    own = (owner == head_row) & (lane < 96 + H)
    spread_scale = jnp.where(own, jnp.where(low, 8.0, -4.0), 0.0)
    gamma[...] = jnp.sum(
        jnp.broadcast_to(turned[0:HP, 14:15], (HP, 128)) * spread_scale, axis=0, keepdims=True
    )
    for t in range(2):
        own_scalar = (lane + 128 * t) // C == head_row
        hmask[:, 128 * t : 128 * t + 128] = jnp.where(own_scalar & (head_row < H), 1.0, 0.0)
    for t in range(2, 8):
        hmask[:, 128 * t : 128 * t + 128] = jnp.where(own & (head_row < H), 1.0, 0.0)

    with jax.named_scope("barrier"):
        pl.semaphore_wait(barrier, NC + NR + 1)

    def row_copy(it, peer, at):
        return pltpu.make_async_remote_copy(
            src_ref=send_buf.at[it],
            dst_ref=row_recv.at[it, at],
            send_sem=row_ss.at[peer],
            recv_sem=row_rs.at[it, at],
            device_id=(r, peer),
            device_id_type=MESH,
        )

    def swap_copy(it):
        return pltpu.make_async_remote_copy(
            src_ref=send_buf.at[it],
            dst_ref=swap_recv.at[it],
            send_sem=swap_ss,
            recv_sem=swap_rs.at[it],
            device_id=(to_row, to_col),
            device_id_type=MESH,
        )

    def far_copy(it, k, at):
        return pltpu.make_async_remote_copy(
            src_ref=send_buf.at[it],
            dst_ref=col_recv.at[it, at],
            send_sem=far_ss.at[k],
            recv_sem=col_rs.at[it, at],
            device_id=(far_rows[k], to_col),
            device_id_type=MESH,
        )

    def col_copy(it, peer, at):
        return pltpu.make_async_remote_copy(
            src_ref=swap_recv.at[it],
            dst_ref=col_recv.at[it, at],
            send_sem=col_ss.at[peer],
            recv_sem=col_rs.at[it, at],
            device_id=(peer, c),
            device_id_type=MESH,
        )

    def idx_copy(peer, k, at):
        return pltpu.make_async_remote_copy(
            src_ref=row_recv.at[0, :, :, D:SW],
            dst_ref=idx_recv.at[at],
            send_sem=idx_ss.at[k],
            recv_sem=idx_rs.at[at],
            device_id=(peer, c),
            device_id_type=MESH,
        )

    idx_targets = (
        (diagonal, r + 1 - 2 * core),
        (diagonal & (c > 0), lax.rem(2 * c + 15, 16)),
        (diagonal & (c < NC - 1), lax.rem(2 * c + 2, 16)),
    )

    def send_numbers():
        for k, (needed, peer) in enumerate(idx_targets):

            @pl.when(needed)
            def _(k=k, peer=peer):
                idx_copy(peer, k, core).start()

        @pl.when(diagonal)
        def _():
            idx_recv[core] = row_recv[0, :, :, D:SW]

    def key_numbers():
        @pl.when(diagonal)
        def _():
            idx_copy(r, 0, 1 - core).wait_recv()

        @pl.when(near & jnp.logical_not(diagonal))
        def _():
            idx_copy(r, 0, 0).wait_recv()
            idx_copy(r, 0, 1).wait_recv()

        @pl.when(near)
        def _():
            f = idx_recv[...].astype(F32).reshape(COLS, 128)
            f = f + pltpu.roll(f, 112, 1) + pltpu.roll(f, 96, 1)
            key_idx[...] = column(f, 12)

        @pl.when(jnp.logical_not(near) & (c > r // 2))
        def _():
            key_idx[...] = jnp.full((COLS, 128), 1e6, F32)

        @pl.when(jnp.logical_not(near) & (c < r // 2))
        def _():
            key_idx[...] = jnp.full((COLS, 128), -1e6, F32)

    def top_copy(it, peer, at):
        return pltpu.make_async_remote_copy(
            src_ref=top_send.at[it, peer],
            dst_ref=top_recv.at[it, at],
            send_sem=top_ss.at[peer],
            recv_sem=top_rs.at[it, at],
            device_id=(r, peer),
            device_id_type=MESH,
        )

    def pair_copy(it, peer, at):
        return pltpu.make_async_remote_copy(
            src_ref=pair_send.at[it, peer],
            dst_ref=pair_recv.at[it, at],
            send_sem=pair_ss.at[peer],
            recv_sem=pair_rs.at[it, at],
            device_id=(r, peer),
            device_id_type=MESH,
        )

    def val_copy(it, peer, at):
        return pltpu.make_async_remote_copy(
            src_ref=val_send.at[it, peer],
            dst_ref=val_recv.at[it, at],
            send_sem=val_ss.at[peer],
            recv_sem=val_rs.at[it, at],
            device_id=(r, peer),
            device_id_type=MESH,
        )

    def start_exchange(it):
        swap_copy(it).start()
        for k in (0, 1):
            far_copy(it, k, core * 8 + c).start()
        for peer in row_peers:
            row_copy(it, peer, c).start()
        row_recv[it, c] = send_buf[it]

    def prepare_projection():
        for cp in copies[:2]:
            cp.wait()
        zeros64 = jnp.zeros((64, D), F32)
        zeros32 = jnp.zeros((32, D), F32)

        def place(block, rows):
            hi, mid = split2(rows.T)
            wp_hi[:, 128 * block : 128 * block + 128] = hi
            wp_mid[:, 128 * block : 128 * block + 128] = mid

        for g in range(2):
            at = g * H * C
            place(5 * g, wsc_f[at : at + 128])
            place(5 * g + 1, jnp.concatenate([wsc_f[at + 128 : at + 192], zeros64], axis=0))
            for a in range(3):
                first = g * 144 + 48 * a
                part = wpt_f[first : first + 48]
                place(5 * g + 2 + a, jnp.concatenate([part, part, zeros32], axis=0))
        at = 2 * H * C
        for a in range(3):
            part = wsc_f[at + 32 * a : at + 32 * a + 32]
            place(10 + a, jnp.concatenate([wpt_f[288 + 96 * a : 384 + 96 * a], part], axis=0))
        place(13, jnp.concatenate([wsc_f[at + 96 : at + 192], zeros32], axis=0))

    def prepare_weights():
        for cp in copies[3:]:
            cp.wait()
        zeros32 = jnp.zeros((32, D), BF16)
        for part, (dst_mix, dst_loc) in enumerate(((wmix_hi, wloc_hi), (wmix_mid, wloc_mid))):
            for k in range(4):
                dst_mix[384 * k : 384 * k + 384] = split2(wout_f[576 + 384 * k : 960 + 384 * k])[
                    part
                ]
            for k in range(3):
                dst_loc[128 * k : 128 * k + 96] = split2(wout_f[192 + 96 * k : 288 + 96 * k])[part]
                dst_loc[128 * k + 96 : 128 * k + 128] = split2(wout_f[32 * k : 32 * k + 32])[part]
            dst_loc[384:480] = split2(wout_f[96:192])[part]
            dst_loc[480:512] = zeros32
            dst_loc[512:608] = split2(wout_f[480:576])[part]
            dst_loc[608:640] = zeros32
        whid_hi[...], whid_mid[...] = split2(whid_f[...])
        wback_hi[...], wback_mid[...] = split2(wback_f[...])
        wfr_f[...] = jnp.zeros_like(wfr_f)
        wfr_f[0:6] = wframe[...]
        wfr_hi[...], wfr_mid[...] = split2(wfr_f[...].T)

    def to_global(f, y, width):
        comps = []
        x = [y[:, 128 * b : 128 * b + 128] for b in range(3)]
        keep = lane_iota(f.shape[0]) < width
        for a in range(3):
            g = (
                column(f, 3 * a) * x[0]
                + column(f, 3 * a + 1) * x[1]
                + column(f, 3 * a + 2) * x[2]
                + column(f, 9 + a)
            )
            comps.append(jnp.where(keep, g, 0.0))
        return comps

    def square_terms(comps):
        sq = comps[0] * comps[0] + comps[1] * comps[1] + comps[2] * comps[2]
        f = lax.broadcasted_iota(jnp.int32, (128, 128), 0)
        n = lax.broadcasted_iota(jnp.int32, (128, 128), 1)
        pick = jnp.where((f < 48) & (n == 96 + f // PQ), 1.0, 0.0).astype(BF16)
        hi, mid = split2(sq)
        lo = (sq - hi.astype(F32) - mid.astype(F32)).astype(BF16)
        total = (mm(hi, pick) + mm(mid, pick) + mm(lo, pick)) * gamma[...]
        hi, mid = split2(total)
        lo = (total - hi.astype(F32) - mid.astype(F32)).astype(BF16)
        return hi, mid, lo

    def query_features(it):
        s, f = unpack(row_recv[it])
        y = mm(s, wp_hi[:, :QW]) + mm(s, wp_mid[:, :QW])
        qf[:, 0:256] = y[:, :256]
        comps = to_global(f, y[:, 256:], 96)
        squares = square_terms(comps)
        lane = lane_iota(ROWS)
        for a in range(3):
            hi, mid = split2(comps[a] * gamma[...])
            ones = jnp.where(lane < 96 + H, 1.0, 0.0)
            qf[:, 256 + 128 * a : 384 + 128 * a] = jnp.where(lane < 96, hi.astype(F32), ones)
            qf[:, 640 + 128 * a : 768 + 128 * a] = jnp.where(
                lane < 48, mid.astype(F32), jnp.where(lane < 96, 0.0, squares[a].astype(F32))
            )

        mask = hmask[...]

        def spread(k, carry):
            for u in range(4):
                i = k * 4 + u
                row = jnp.broadcast_to(qf[pl.ds(i, 1), :], (HP, FW))
                at = pl.multiple_of(i * HP, HP)
                qmask[pl.ds(at, HP), :] = (row * mask).astype(BF16)
            return carry

        lax.fori_loop(0, ROWS // 4, spread, 0)

    def key_features(it):
        s, f = unpack(col_recv[it])
        y = mm(s, wp_hi[:, QW : 2 * QW]) + mm(s, wp_mid[:, QW : 2 * QW])
        kf[:, 0:256] = y[:, :256].astype(BF16)
        comps = to_global(f, y[:, 256:QW], 96)
        squares = square_terms(comps)
        lane = lane_iota(COLS)
        zero = jnp.zeros((COLS, 128), F32)
        for a in range(3):
            hi, mid = split2(comps[a])
            hi, mid = hi.astype(F32), mid.astype(F32)
            sq = squares[a].astype(F32)
            kf[:, 256 + 128 * a : 384 + 128 * a] = jnp.where(
                lane < 48, hi, jnp.where(lane < 96, mid, sq)
            ).astype(BF16)
            ones = jnp.where((lane >= 96) & (lane < 96 + H), 1.0, zero)
            kf[:, 640 + 128 * a : 768 + 128 * a] = jnp.where(lane < 48, hi, ones).astype(BF16)

    def value_features(it):
        s, f = unpack(col_recv[it])
        y = mm(s, wp_hi[:, 2 * QW :]) + mm(s, wp_mid[:, 2 * QW :])
        values = to_global(f, y, 96)
        lane = lane_iota(COLS)
        for a in range(3):
            at = 128 * a
            hi, mid = split2(jnp.where(lane < 96, values[a], y[:, at : at + 128]))
            vcat[0:COLS, at : at + 128] = hi
            vcat[COLS:, at : at + 128] = jnp.where(lane < 96, mid.astype(F32), 0.0).astype(BF16)
        vcat[0:COLS, 384:512] = y[:, 384:512].astype(BF16)
        vcat[COLS:, 384:512] = jnp.zeros((COLS, 128), BF16)

    def prepare_pair():
        copies[2].wait()
        fq = unpack(row_recv[0])[1]
        idx_b[0:ROWS] = column(fq, 12)
        idx_b[ROWS:] = column(fq, 13)
        key_index = key_idx[...]
        shape = (COLS, 128)
        lane = lax.broadcasted_iota(jnp.int32, shape, 1).astype(F32) - 64.0
        same = lax.broadcasted_iota(jnp.int32, shape, 0) == lax.broadcasted_iota(jnp.int32, shape, 1)
        table = relpos[...].astype(F32)
        hi, mid = split2(table - jnp.mean(table, axis=-1, keepdims=True))
        centre[0:128] = jnp.where(same, 1.0 - 1.0 / 128.0, -1.0 / 128.0).astype(BF16)
        centre[128:256] = hi
        centre[256:384] = mid
        wb_s[...] = jnp.zeros_like(wb_s)
        wb_s[0:H] = wb_in[...].astype(F32)
        project = wb_s[...].astype(BF16)
        gains = gain[...]
        step = 8

        def prepare(k, carry):
            first = k * step
            centres = []
            for u in range(step):
                offset = jnp.clip(key_index - idx_b[pl.ds(first + u, 1), :], -64.0, 63.0)
                onehot = jnp.where(offset == lane, 1.0, 0.0).astype(BF16)
                both = jnp.concatenate([pair_v[first + u], onehot, onehot], axis=1)
                centres.append(mm(both, centre[...]))
            for u in range(step):
                spread = jnp.mean(centres[u] * centres[u], axis=-1, keepdims=True)
                normed = (centres[u] * lax.rsqrt(spread + NORM_EPSILON) * gains).astype(BF16)
                pair_v[first + u] = normed
                bias = lax.dot_general(
                    project, normed, (((1,), (1,)), ((), ())), preferred_element_type=F32
                )
                live = idx_b[pl.ds(ROWS + first + u, 1), :] > 0.5
                at = pl.multiple_of((first + u) * HP, HP)
                bias_v[pl.ds(at, HP), :] = jnp.where(live, bias * THIRD, DEAD)
            return carry

        lax.fori_loop(0, ROWS // step, prepare, 0)

    def mask_keys():
        live = unpack(col_recv[0])[1].T[13:14, :] > 0.5
        for k in range(4):
            part = pl.ds(k * 256, 256)
            bias_v[part, :] = jnp.where(live, bias_v[part, :], DEAD)

    def store_queries(ref, first, rows):
        for k in range(rows.shape[0] // HP):
            ref[pl.ds((first + k) * PITCH, HP), :] = rows[HP * k : HP * k + HP]

    def attend(it):
        with jax.named_scope("logits"):
            keys = kf[...]
            rows = 256
            for k in range(ROWS * HP // rows):
                part = pl.ds(k * rows, rows)
                acc = lax.dot_general(
                    qmask[part, :], keys, (((1,), (1,)), ((), ())), preferred_element_type=F32
                )
                bias = bias_v[part, :]
                logits = jnp.where(bias > -1e38, acc * (THIRD / math.sqrt(C)) + bias, MASKED_LOGIT)
                top = jnp.max(logits, axis=-1, keepdims=True)
                p = jnp.exp(logits - top).astype(BF16)
                top = jnp.broadcast_to(top, (rows, 128))
                total = jnp.sum(p.astype(F32), axis=-1, keepdims=True)
                total = jnp.broadcast_to(total, (rows, 128))
                store_queries(m_b, k * rows // HP, top)
                store_queries(s_b, k * rows // HP, total)
                p_s[part, 0:128] = p
                p_s[part, 128:256] = p

        with jax.named_scope("pack"):
            lane = lane_iota(8)
            place = jnp.where(lane < 96, lax.rem(lane, 32), -1)
            for g in range(NC):
                tile = jnp.zeros((8, 128), F32)
                for h in range(H):
                    src = pl.ds(8 * PITCH * g + h, 8, stride=PITCH)
                    tile = jnp.where(place == h, m_b[src, :], tile)
                    tile = jnp.where(place == HP + h, s_b[src, :], tile)
                hi, mid = split2(tile)
                lo = tile - hi.astype(F32) - mid.astype(F32)
                tile = jnp.where(
                    lane < 32, hi.astype(F32), jnp.where(lane < 64, mid.astype(F32), lo)
                )
                top_send[it, g] = tile.astype(BF16)
            for peer in row_peers:
                top_copy(it, peer, c).start()
        with jax.named_scope("pairs"):
            for i in range(ROWS):
                part = pl.ds(i * HP, HP)
                store_queries(pair_s, i, mm(p_s[part, 0:128], pair_v[i]))
            for h in range(H):
                pair_send[it, :, :, 128 * h : 128 * h + 128] = (
                    pair_s[pl.ds(h, ROWS, stride=PITCH), :].astype(BF16).reshape(NC, OWN, 128)
                )
            for peer in row_peers:
                pair_copy(it, peer, c).start()
        with jax.named_scope("values"):
            value_features(it)
        with jax.named_scope("sums"):
            values = vcat[...]
            for k in range(4):
                part = pl.ds(k * 256, 256)
                y = mm(p_s[part, :], values)
                for t in range(4):
                    store_queries(r_s.at[t], 16 * k, y[:, 128 * t : 128 * t + 128])
        with jax.named_scope("select"):
            for t in range(4):
                val_send[it, :, :, 128 * t : 128 * t + 128] = by_head(
                    t, ROWS, lambda h: r_s[t, pl.ds(h, ROWS, stride=PITCH), :]
                ).reshape(NC, OWN, 128)
            for peer in row_peers:
                val_copy(it, peer, c).start()
            top_recv[it, c] = top_send[it, c]
            pair_recv[it, c] = pair_send[it, c]
            val_recv[it, c] = val_send[it, c]

            @pl.when(it == 0)
            def _():
                prepare_weights()

    def by_head(t, rows, piece):
        spans = [(h, PV * h, PV) for h in range(H)] if t < 3 else []
        at, heads = (96, range(2 * t, 2 * t + 2)) if t < 3 else (0, range(6, H))
        spans += [(h, at + C * (h - heads[0]), C) for h in heads]
        lane = lane_iota(rows)
        out = jnp.zeros((rows, 128), F32)
        for h, lo, size in spans:
            out = jnp.where((lane >= lo) & (lane < lo + size), piece(h), out)
        return out

    def advance(it):
        with jax.named_scope("wait_top"):
            for peer in row_peers:
                top_copy(it, peer, peer).wait_recv()
        tops = []
        for k in range(NC):
            tile = top_recv[it, k].astype(F32)
            tops.append(tile + pltpu.roll(tile, 96, 1) + pltpu.roll(tile, 64, 1))
        top = functools.reduce(jnp.maximum, tops)
        scales = [jnp.exp(t - top) for t in tops]
        total = scales[0] * pltpu.roll(tops[0], 128 - HP, 1)
        for k in range(1, NC):
            total = total + scales[k] * pltpu.roll(tops[k], 128 - HP, 1)
        inverse = 1.0 / jnp.where(lane_iota(OWN) < H, total, 1.0)
        factor = [[column(e * inverse, h) for h in range(H)] for e in scales]
        with jax.named_scope("wait_pair"):
            for peer in row_peers:
                pair_copy(it, peer, peer).wait_recv()
        pairs = []
        for h in range(H):
            at = pl.ds(128 * h, 128)
            out = factor[0][h] * pair_recv[it, 0, :, at].astype(F32)
            for k in range(1, NC):
                out = out + factor[k][h] * pair_recv[it, k, :, at].astype(F32)
            pairs.append(out)
        mixed = dot3(jnp.concatenate(pairs, axis=1), wmix_hi[...], wmix_mid[...])
        spread = [[by_head(t, OWN, lambda h: factor[k][h]) for t in range(4)] for k in range(NC)]
        with jax.named_scope("wait_val"):
            for peer in row_peers:
                val_copy(it, peer, peer).wait_recv()
        tiles = []
        for t in range(4):
            at = pl.ds(128 * t, 128)
            out = spread[0][t] * val_recv[it, 0, :, at]
            for k in range(1, NC):
                out = out + spread[k][t] * val_recv[it, k, :, at]
            tiles.append(out)
        frames = state_f[:, D:]
        single = state_f[:, :D]
        moved = [tiles[a] - column(frames, 9 + a) for a in range(3)]
        local = [
            column(frames, a) * moved[0]
            + column(frames, 3 + a) * moved[1]
            + column(frames, 6 + a) * moved[2]
            for a in range(3)
        ]
        lengths = jnp.sqrt(
            local[0] * local[0] + local[1] * local[1] + local[2] * local[2] + NORM_FLOOR
        )
        keep = lane_iota(OWN) < H * PV
        feats = [jnp.where(keep, local[a], tiles[a]) for a in range(3)]
        feats += [tiles[3], jnp.where(keep, lengths, 0.0)]
        feats = jnp.concatenate(feats, axis=1)
        single = single + mixed + dot3(feats, wloc_hi[...], wloc_mid[...])
        single = layer_norm(single)
        hidden = jnp.maximum(dot3(single, whid_hi[...], whid_mid[...]), 0.0)
        single = layer_norm(single + dot3(hidden, wback_hi[...], wback_mid[...]))
        update = dot3(single, wfr_hi[...], wfr_mid[...])
        turn = rotation_entries(column(update, 0), column(update, 1), column(update, 2))
        rot = [column(frames, k) for k in range(9)]
        step = [column(update, 3 + k) for k in range(3)]
        new = [
            rot[3 * left] * turn[right]
            + rot[3 * left + 1] * turn[3 + right]
            + rot[3 * left + 2] * turn[6 + right]
            for left in range(3)
            for right in range(3)
        ] + [
            rot[3 * left] * step[0]
            + rot[3 * left + 1] * step[1]
            + rot[3 * left + 2] * step[2]
            + column(frames, 9 + left)
            for left in range(3)
        ]
        lane = lax.rem(lane_iota(OWN), 16)
        out = frames
        for k, value in enumerate(new):
            out = jnp.where(lane == k, value, out)
        return single, out

    def iteration(it, carry):
        with jax.named_scope("start"):
            start_exchange(it)

            @pl.when(it == 0)
            def _():
                prepare_projection()

        with jax.named_scope("wait_swap"):
            swap_copy(it).wait_recv()
        with jax.named_scope("send_col"):
            for peer in served:
                col_copy(it, peer, slot).start()
            col_recv[it, slot] = swap_recv[it]

        with jax.named_scope("wait_row"):
            for peer in row_peers:
                row_copy(it, peer, peer).wait_recv()
        with jax.named_scope("query"):

            @pl.when(it == 0)
            def _():
                send_numbers()

            query_features(it)
        with jax.named_scope("prep_pair"):

            @pl.when(it == 0)
            def _():
                key_numbers()
                prepare_pair()

        with jax.named_scope("wait_col"):
            for peer in served:
                col_copy(it, peer, slot_of(peer)).wait_recv()
            for k in (0, 1):
                far_copy(it, k, k * 8 + far_sources[k][1]).wait_recv()
        with jax.named_scope("key"):
            key_features(it)

            @pl.when(it == 0)
            def _():
                mask_keys()

        attend(it)
        with jax.named_scope("advance"):
            single, frames = advance(it)

            @pl.when(it < ITERS - 1)
            def _():
                send_buf[it + 1] = pack(single, frames)
                state_f[:, 0:D] = single
                state_f[:, D:] = frames

            @pl.when(it == ITERS - 1)
            def _():
                single_out[...] = single
                frames_out[...] = frames[:, 0:12]

        with jax.named_scope("wait_send"):
            swap_copy(it).wait_send()
            for peer in row_peers:
                row_copy(it, peer, c).wait_send()
                top_copy(it, peer, c).wait_send()
                pair_copy(it, peer, c).wait_send()
                val_copy(it, peer, c).wait_send()
            for peer in served:
                col_copy(it, peer, slot).wait_send()
            for k in (0, 1):
                far_copy(it, k, core * 8 + c).wait_send()
        return carry

    lax.fori_loop(0, ITERS, iteration, 0)
    for k, (needed, peer) in enumerate(idx_targets):

        @pl.when(needed)
        def _(k=k, peer=peer):
            idx_copy(peer, k, core).wait_send()


def hand_over(state, frames, state_out, frames_out):
    state_out[...] = state[...]
    frames_out[...] = frames[...]


def body(
    pair, relpos, pair_gain, bias_weight, single, rotation_params, translation, residue_index,
    residue_mask, w_scalar, w_points, head_weights, w_out, w_hidden, w_back, w_frame,
):
    vmem = pl.BlockSpec(memory_space=pltpu.VMEM)
    anyspace = pl.BlockSpec(memory_space=pl.ANY)
    V = pltpu.VMEM
    dma = pltpu.SemaphoreType.DMA
    scratch = [
        V((OWN, D), F32),
        V((3, OWN), F32),
        V((3, OWN), F32),
        V((1, OWN), jnp.int32),
        V((1, OWN), jnp.int32),
        V((1, H), F32),
        V((128, 128), BF16),
        V((1, 128), F32),
        V((H, 128), BF16),
        V((6, D), F32),
        V((ROWS, COLS, 128), BF16),
        V((ROWS * HP, 128), F32),
        V((576, D), F32),
        V((576, D), F32),
        V((2112, D), F32),
        V((D, D), F32),
        V((D, D), F32),
        V((128, D), F32),
        V((D, 2 * QW + VW), BF16),
        V((D, 2 * QW + VW), BF16),
        V((H * 128, D), BF16),
        V((H * 128, D), BF16),
        V((QW, D), BF16),
        V((QW, D), BF16),
        V((D, D), BF16),
        V((D, D), BF16),
        V((D, D), BF16),
        V((D, D), BF16),
        V((D, 128), BF16),
        V((D, 128), BF16),
        V((HP, 128), F32),
        V((HP, 128), F32),
        V((1, 128), F32),
        V((HP, FW), F32),
        V((3 * 128, 128), BF16),
        V((OWN, SW), F32),
        V((ITERS, OWN, SW), BF16),
        V((ITERS, NC, OWN, SW), BF16),
        V((ITERS, OWN, SW), BF16),
        V((ITERS, NR, OWN, SW), BF16),
        V((ITERS, NC, OWN, 128), BF16),
        V((ITERS, NC, OWN, 128), BF16),
        V((ITERS, NC, OWN, H * 128), BF16),
        V((ITERS, NC, OWN, H * 128), BF16),
        V((ITERS, NC, OWN, VW), F32),
        V((ITERS, NC, OWN, VW), F32),
        V((2, NC, OWN, 128), BF16),
        V((COLS, 128), F32),
        V((ROWS, FW), F32),
        V((ROWS * HP, FW), BF16),
        V((COLS, FW), BF16),
        V((2 * COLS, VW), BF16),
        V((2 * ROWS, 128), F32),
        V((ROWS * HP, 256), BF16),
        V((ROWS * PITCH, 128), F32),
        V((ROWS * PITCH, 128), F32),
        V((4, ROWS * PITCH, 128), F32),
        V((ROWS * PITCH, 128), F32),
        dma((16,)),
        dma((NC,)),
        dma((ITERS, NC)),
        dma,
        dma((ITERS,)),
        dma((NR,)),
        dma((ITERS, NR)),
        dma((NC,)),
        dma((ITERS, NC)),
        dma((NC,)),
        dma((ITERS, NC)),
        dma((NC,)),
        dma((ITERS, NC)),
        dma((3,)),
        dma((2,)),
        dma((2,)),
    ]
    state, frames = pl.pallas_call(
        kernel,
        out_shape=(
            jax.ShapeDtypeStruct((OWN, D), F32),
            jax.ShapeDtypeStruct((OWN, 12), F32),
        ),
        in_specs=[anyspace] * 16,
        out_specs=(vmem, vmem),
        scratch_shapes=scratch,
        compiler_params=pltpu.CompilerParams(
            collective_id=0, has_side_effects=True, vmem_limit_bytes=62 * 1024 * 1024
        ),
        name="structure",
    )(
        single, rotation_params, translation, residue_index.reshape(1, OWN),
        residue_mask.reshape(1, OWN), head_weights.reshape(1, H), relpos,
        pair_gain.reshape(1, 128), bias_weight.T, w_frame.T,
        pair, w_scalar.T, w_points.T, w_out, w_hidden, w_back,
    )
    state, frames = pl.pallas_call(
        hand_over,
        out_shape=(
            jax.ShapeDtypeStruct((OWN, D), F32),
            jax.ShapeDtypeStruct((OWN, 12), F32),
        ),
        in_specs=[vmem, vmem],
        out_specs=(vmem, vmem),
        compiler_params=pltpu.CompilerParams(vmem_limit_bytes=62 * 1024 * 1024),
        name="hand_over",
    )(state, frames)
    return state, frames.T


def solution(mesh):
    placed = (
        P("row", "col", None),
        P(),
        P(),
        P(),
        P(("row", "col"), None),
        P(None, ("row", "col")),
        P(None, ("row", "col")),
        P(("row", "col")),
        P(("row", "col")),
        P(),
        P(),
        P(),
        P(),
        P(),
        P(),
        P(),
    )
    return jax.shard_map(
        body,
        mesh=mesh,
        in_specs=placed,
        out_specs=(P(("row", "col"), None), P(None, ("row", "col"))),
        check_vma=False,
    )
```

```python
import functools
import math

import jax
import jax.numpy as jnp
from jax import lax
from jax.experimental import pallas as pl
from jax.experimental.pallas import tpu as pltpu
from jax.sharding import PartitionSpec as P

H = 12
C = 16
PQ = 4
PV = 8
BINS = 128
ITERS = 3
D = 384
HP = 16
PITCH = 24
ROWS = 64
COLS = 128
OWN = 8
NR = 16
NC = 8
SW = 512
QW = 640
VW = 512
FW = 1024

NORM_EPSILON = 1e-05
MASKED_LOGIT = -100000.0
DEAD = -3e38
NORM_FLOOR = 0.1
THIRD = math.sqrt(1.0 / 3.0)
MESH = pl.DeviceIdType.MESH
F32 = jnp.float32
BF16 = jnp.bfloat16


def rotation_entries(b, c, d):
    inverse = 1.0 / (1.0 + b * b + c * c + d * d)
    entries = [
        1.0 + b * b - c * c - d * d,
        2.0 * (b * c - d),
        2.0 * (b * d + c),
        2.0 * (b * c + d),
        1.0 - b * b + c * c - d * d,
        2.0 * (c * d - b),
        2.0 * (b * d - c),
        2.0 * (c * d + b),
        1.0 - b * b - c * c + d * d,
    ]
    return [e * inverse for e in entries]


def layer_norm(values):
    center = values - jnp.mean(values, axis=-1, keepdims=True)
    spread = jnp.mean(center * center, axis=-1, keepdims=True)
    return center * lax.rsqrt(spread + NORM_EPSILON)


def split2(x):
    hi = x.astype(BF16)
    return hi, (x - hi.astype(F32)).astype(BF16)


def mm(a, b):
    return jnp.dot(a, b, preferred_element_type=F32)


def dot3(x, w_hi, w_mid):
    hi, mid = split2(x)
    n = x.shape[0]
    both = mm(jnp.concatenate([hi, mid], axis=0), w_hi)
    return both[:n] + both[n:] + mm(hi, w_mid)


def lane_iota(rows):
    return lax.broadcasted_iota(jnp.int32, (rows, 128), 1)


def pad_lanes(x):
    return jnp.concatenate([x, jnp.zeros((x.shape[0], 128 - x.shape[1]), x.dtype)], axis=1)


def column(x, k):
    return jnp.broadcast_to(x[:, k : k + 1], (x.shape[0], 128))


def kernel(
    single_hbm, rotation_hbm, translation_hbm, index_hbm, live_hbm, head_hbm, relpos_hbm, gain_hbm,
    wb_hbm, wframe_hbm, pair_hbm, wsc_hbm, wpt_hbm, wout_hbm, whid_hbm, wback_hbm,
    single_out, frames_out,
    single_in, rotation_in, translation_in, index_in, live_in, head_in, relpos, gain, wb_in, wframe,
    pair_v, bias_v, wsc_f, wpt_f, wout_f, whid_f, wback_f, wfr_f,
    wp_hi, wp_mid, wmix_hi, wmix_mid, wloc_hi, wloc_mid, whid_hi, whid_mid, wback_hi, wback_mid,
    wfr_hi, wfr_mid, wb_s, small, gamma, hmask, centre,
    state_f, send_buf, row_recv, swap_recv, col_recv, top_send, top_recv, pair_send, pair_recv,
    val_send, val_recv, idx_recv, key_idx,
    qf, qmask, kf, vcat, idx_b, p_s, m_b, s_b, r_s, pair_s,
    copy_sem, row_ss, row_rs, swap_ss, swap_rs, col_ss, col_rs, top_ss, top_rs,
    pair_ss, pair_rs, val_ss, val_rs, idx_ss, idx_rs, far_ss,
):
    r = lax.axis_index("row")
    c = lax.axis_index("col")
    core = lax.rem(r, 2)
    z = lax.rem(r // 2, 4)
    y_hi = r // 8
    x = lax.rem(c, 4)
    y_lo = c // 4
    to_row = y_lo * 8 + lax.rem(x + 2, 4) * 2 + core
    to_col = y_hi * 4 + z
    from_row = y_lo * 8 + x * 2 + core
    from_col = y_hi * 4 + lax.rem(z + 2, 4)

    far_rows = [(1 - y_lo) * 8 + x * 2 + k for k in (0, 1)]
    far_sources = [(y_lo * 8 + x * 2 + k, (1 - y_hi) * 4 + z) for k in (0, 1)]

    def slot_of(row):
        return lax.rem(row, 2) * 8 + (row // 8) * 4 + lax.rem(row // 2 + 2, 4)

    slot = slot_of(r)
    near = (r >= 2 * c - 1) & (r <= 2 * c + 2)
    diagonal = r // 2 == c

    row_peers = [
        lax.rem(y_lo + dy, 2) * 4 + lax.rem(x + dx, 4)
        for dy, dx in ((1, 2), (1, 1), (1, 3), (0, 2), (1, 0), (0, 1), (0, 3))
    ]
    col_peers = [
        lax.rem(y_hi + dy, 2) * 8 + lax.rem(z + dz, 4) * 2 + lax.rem(core + dc, 2)
        for dy, dz in ((1, 2), (1, 1), (1, 3), (1, 0), (0, 2), (0, 1), (0, 3), (0, 0))
        for dc in (0, 1)
        if (dy, dz, dc) != (0, 0, 0)
    ]
    served = col_peers[2:]

    barrier = pltpu.get_barrier_semaphore()
    for peer in col_peers:
        pl.semaphore_signal(barrier, inc=1, device_id=(peer, c), device_id_type=MESH)
    for peer in row_peers:
        pl.semaphore_signal(barrier, inc=1, device_id=(r, peer), device_id_type=MESH)
    pl.semaphore_signal(barrier, inc=1, device_id=(from_row, from_col), device_id_type=MESH)
    for peer in far_sources:
        pl.semaphore_signal(barrier, inc=1, device_id=peer, device_id_type=MESH)

    small_copies = [
        pltpu.make_async_copy(src, dst, copy_sem.at[6 + k])
        for k, (src, dst) in enumerate(
            [
                (single_hbm, single_in),
                (rotation_hbm, rotation_in),
                (translation_hbm, translation_in),
                (index_hbm, index_in),
                (live_hbm, live_in),
                (head_hbm, head_in),
                (relpos_hbm, relpos),
                (gain_hbm, gain),
                (wb_hbm, wb_in),
                (wframe_hbm, wframe),
            ]
        )
    ]
    copies = [
        pltpu.make_async_copy(src, dst, copy_sem.at[k])
        for k, (src, dst) in enumerate(
            [
                (wsc_hbm, wsc_f),
                (wpt_hbm, wpt_f),
                (pair_hbm, pair_v),
                (wout_hbm, wout_f),
                (whid_hbm, whid_f),
                (wback_hbm, wback_f),
            ]
        )
    ]
    for cp in small_copies + copies:
        cp.start()
    for cp in small_copies:
        cp.wait()

    small[...] = jnp.zeros_like(small)
    entries = rotation_entries(rotation_in[0:1], rotation_in[1:2], rotation_in[2:3])
    for k, row in enumerate(
        entries
        + [translation_in[k : k + 1] for k in range(3)]
        + [index_in[...].astype(F32), jnp.where(live_in[...] == 1, 1.0, 0.0)]
    ):
        small[k : k + 1, 0:OWN] = row
    head = head_in[...]
    positive = jnp.maximum(head, 0.0) + jnp.log1p(jnp.exp(-jnp.abs(head)))
    small[14:15, 0:H] = positive * (math.sqrt(2.0 / (9.0 * PQ)) / 2.0)
    turned = small[...].T
    state_f[:, 0:D] = single_in[...]
    state_f[:, D:] = pad_lanes(jnp.concatenate([turned[0:OWN]] * 3, axis=1))

    def pack(single, frames):
        at = lane_iota(OWN)
        hi, mid = split2(frames)
        lo = (frames - hi.astype(F32) - mid.astype(F32)).astype(BF16)
        pieces = jnp.where(
            at < 16,
            hi.astype(F32),
            jnp.where(at < 32, mid.astype(F32), jnp.where(at < 48, lo.astype(F32), 0.0)),
        )
        return jnp.concatenate([single.astype(BF16), pieces.astype(BF16)], axis=1)

    def unpack(blocks):
        rows = blocks.astype(F32).reshape(blocks.shape[0] * OWN, SW)
        f = rows[:, D:]
        f = f + pltpu.roll(f, 112, 1) + pltpu.roll(f, 96, 1)
        return rows[:, :D].astype(BF16), f

    send_buf[0] = pack(state_f[:, 0:D], state_f[:, D:])

    lane = lane_iota(HP)
    head_row = lax.broadcasted_iota(jnp.int32, (HP, 128), 0)
    low = lane < 96
    owner = jnp.where(low, lax.rem(lane, 48) // PQ, lane - 96)
    own = (owner == head_row) & (lane < 96 + H)
    spread_scale = jnp.where(own, jnp.where(low, 8.0, -4.0), 0.0)
    gamma[...] = jnp.sum(
        jnp.broadcast_to(turned[0:HP, 14:15], (HP, 128)) * spread_scale, axis=0, keepdims=True
    )
    for t in range(2):
        own_scalar = (lane + 128 * t) // C == head_row
        hmask[:, 128 * t : 128 * t + 128] = jnp.where(own_scalar & (head_row < H), 1.0, 0.0)
    for t in range(2, 8):
        hmask[:, 128 * t : 128 * t + 128] = jnp.where(own & (head_row < H), 1.0, 0.0)

    with jax.named_scope("barrier"):
        pl.semaphore_wait(barrier, NC + NR + 1)

    def row_copy(it, peer, at):
        return pltpu.make_async_remote_copy(
            src_ref=send_buf.at[it],
            dst_ref=row_recv.at[it, at],
            send_sem=row_ss.at[peer],
            recv_sem=row_rs.at[it, at],
            device_id=(r, peer),
            device_id_type=MESH,
        )

    def swap_copy(it):
        return pltpu.make_async_remote_copy(
            src_ref=send_buf.at[it],
            dst_ref=swap_recv.at[it],
            send_sem=swap_ss,
            recv_sem=swap_rs.at[it],
            device_id=(to_row, to_col),
            device_id_type=MESH,
        )

    def far_copy(it, k, at):
        return pltpu.make_async_remote_copy(
            src_ref=send_buf.at[it],
            dst_ref=col_recv.at[it, at],
            send_sem=far_ss.at[k],
            recv_sem=col_rs.at[it, at],
            device_id=(far_rows[k], to_col),
            device_id_type=MESH,
        )

    def col_copy(it, peer, at):
        return pltpu.make_async_remote_copy(
            src_ref=swap_recv.at[it],
            dst_ref=col_recv.at[it, at],
            send_sem=col_ss.at[peer],
            recv_sem=col_rs.at[it, at],
            device_id=(peer, c),
            device_id_type=MESH,
        )

    def idx_copy(peer, k, at):
        return pltpu.make_async_remote_copy(
            src_ref=row_recv.at[0, :, :, D:SW],
            dst_ref=idx_recv.at[at],
            send_sem=idx_ss.at[k],
            recv_sem=idx_rs.at[at],
            device_id=(peer, c),
            device_id_type=MESH,
        )

    idx_targets = (
        (diagonal, r + 1 - 2 * core),
        (diagonal & (c > 0), lax.rem(2 * c + 15, 16)),
        (diagonal & (c < NC - 1), lax.rem(2 * c + 2, 16)),
    )

    def send_numbers():
        for k, (needed, peer) in enumerate(idx_targets):

            @pl.when(needed)
            def _(k=k, peer=peer):
                idx_copy(peer, k, core).start()

        @pl.when(diagonal)
        def _():
            idx_recv[core] = row_recv[0, :, :, D:SW]

    def key_numbers():
        @pl.when(diagonal)
        def _():
            idx_copy(r, 0, 1 - core).wait_recv()

        @pl.when(near & jnp.logical_not(diagonal))
        def _():
            idx_copy(r, 0, 0).wait_recv()
            idx_copy(r, 0, 1).wait_recv()

        @pl.when(near)
        def _():
            f = idx_recv[...].astype(F32).reshape(COLS, 128)
            f = f + pltpu.roll(f, 112, 1) + pltpu.roll(f, 96, 1)
            key_idx[...] = column(f, 12)

        @pl.when(jnp.logical_not(near) & (c > r // 2))
        def _():
            key_idx[...] = jnp.full((COLS, 128), 1e6, F32)

        @pl.when(jnp.logical_not(near) & (c < r // 2))
        def _():
            key_idx[...] = jnp.full((COLS, 128), -1e6, F32)

    def top_copy(it, peer, at):
        return pltpu.make_async_remote_copy(
            src_ref=top_send.at[it, peer],
            dst_ref=top_recv.at[it, at],
            send_sem=top_ss.at[peer],
            recv_sem=top_rs.at[it, at],
            device_id=(r, peer),
            device_id_type=MESH,
        )

    def pair_copy(it, peer, at):
        return pltpu.make_async_remote_copy(
            src_ref=pair_send.at[it, peer],
            dst_ref=pair_recv.at[it, at],
            send_sem=pair_ss.at[peer],
            recv_sem=pair_rs.at[it, at],
            device_id=(r, peer),
            device_id_type=MESH,
        )

    def val_copy(it, peer, at):
        return pltpu.make_async_remote_copy(
            src_ref=val_send.at[it, peer],
            dst_ref=val_recv.at[it, at],
            send_sem=val_ss.at[peer],
            recv_sem=val_rs.at[it, at],
            device_id=(r, peer),
            device_id_type=MESH,
        )

    def start_exchange(it):
        swap_copy(it).start()
        for k in (0, 1):
            far_copy(it, k, core * 8 + c).start()
        for peer in row_peers:
            row_copy(it, peer, c).start()
        row_recv[it, c] = send_buf[it]

    def prepare_projection():
        for cp in copies[:2]:
            cp.wait()
        zeros64 = jnp.zeros((64, D), F32)
        zeros32 = jnp.zeros((32, D), F32)

        def place(block, rows):
            hi, mid = split2(rows.T)
            wp_hi[:, 128 * block : 128 * block + 128] = hi
            wp_mid[:, 128 * block : 128 * block + 128] = mid

        for g in range(2):
            at = g * H * C
            place(5 * g, wsc_f[at : at + 128])
            place(5 * g + 1, jnp.concatenate([wsc_f[at + 128 : at + 192], zeros64], axis=0))
            for a in range(3):
                first = g * 144 + 48 * a
                part = wpt_f[first : first + 48]
                place(5 * g + 2 + a, jnp.concatenate([part, part, zeros32], axis=0))
        at = 2 * H * C
        for a in range(3):
            part = wsc_f[at + 32 * a : at + 32 * a + 32]
            place(10 + a, jnp.concatenate([wpt_f[288 + 96 * a : 384 + 96 * a], part], axis=0))
        place(13, jnp.concatenate([wsc_f[at + 96 : at + 192], zeros32], axis=0))

    def prepare_weights():
        for cp in copies[3:]:
            cp.wait()
        zeros32 = jnp.zeros((32, D), BF16)
        for part, (dst_mix, dst_loc) in enumerate(((wmix_hi, wloc_hi), (wmix_mid, wloc_mid))):
            for k in range(4):
                dst_mix[384 * k : 384 * k + 384] = split2(wout_f[576 + 384 * k : 960 + 384 * k])[
                    part
                ]
            for k in range(3):
                dst_loc[128 * k : 128 * k + 96] = split2(wout_f[192 + 96 * k : 288 + 96 * k])[part]
                dst_loc[128 * k + 96 : 128 * k + 128] = split2(wout_f[32 * k : 32 * k + 32])[part]
            dst_loc[384:480] = split2(wout_f[96:192])[part]
            dst_loc[480:512] = zeros32
            dst_loc[512:608] = split2(wout_f[480:576])[part]
            dst_loc[608:640] = zeros32
        whid_hi[...], whid_mid[...] = split2(whid_f[...])
        wback_hi[...], wback_mid[...] = split2(wback_f[...])
        wfr_f[...] = jnp.zeros_like(wfr_f)
        wfr_f[0:6] = wframe[...]
        wfr_hi[...], wfr_mid[...] = split2(wfr_f[...].T)

    def to_global(f, y, width):
        comps = []
        x = [y[:, 128 * b : 128 * b + 128] for b in range(3)]
        keep = lane_iota(f.shape[0]) < width
        for a in range(3):
            g = (
                column(f, 3 * a) * x[0]
                + column(f, 3 * a + 1) * x[1]
                + column(f, 3 * a + 2) * x[2]
                + column(f, 9 + a)
            )
            comps.append(jnp.where(keep, g, 0.0))
        return comps

    def square_terms(comps):
        sq = comps[0] * comps[0] + comps[1] * comps[1] + comps[2] * comps[2]
        f = lax.broadcasted_iota(jnp.int32, (128, 128), 0)
        n = lax.broadcasted_iota(jnp.int32, (128, 128), 1)
        pick = jnp.where((f < 48) & (n == 96 + f // PQ), 1.0, 0.0).astype(BF16)
        hi, mid = split2(sq)
        lo = (sq - hi.astype(F32) - mid.astype(F32)).astype(BF16)
        total = (mm(hi, pick) + mm(mid, pick) + mm(lo, pick)) * gamma[...]
        hi, mid = split2(total)
        lo = (total - hi.astype(F32) - mid.astype(F32)).astype(BF16)
        return hi, mid, lo

    def query_features(it):
        s, f = unpack(row_recv[it])
        y = mm(s, wp_hi[:, :QW]) + mm(s, wp_mid[:, :QW])
        qf[:, 0:256] = y[:, :256]
        comps = to_global(f, y[:, 256:], 96)
        squares = square_terms(comps)
        lane = lane_iota(ROWS)
        for a in range(3):
            hi, mid = split2(comps[a] * gamma[...])
            ones = jnp.where(lane < 96 + H, 1.0, 0.0)
            qf[:, 256 + 128 * a : 384 + 128 * a] = jnp.where(lane < 96, hi.astype(F32), ones)
            qf[:, 640 + 128 * a : 768 + 128 * a] = jnp.where(
                lane < 48, mid.astype(F32), jnp.where(lane < 96, 0.0, squares[a].astype(F32))
            )

        mask = hmask[...]

        def spread(k, carry):
            for u in range(4):
                i = k * 4 + u
                row = jnp.broadcast_to(qf[pl.ds(i, 1), :], (HP, FW))
                at = pl.multiple_of(i * HP, HP)
                qmask[pl.ds(at, HP), :] = (row * mask).astype(BF16)
            return carry

        lax.fori_loop(0, ROWS // 4, spread, 0)

    def key_features(it):
        s, f = unpack(col_recv[it])
        y = mm(s, wp_hi[:, QW : 2 * QW]) + mm(s, wp_mid[:, QW : 2 * QW])
        kf[:, 0:256] = y[:, :256].astype(BF16)
        comps = to_global(f, y[:, 256:QW], 96)
        squares = square_terms(comps)
        lane = lane_iota(COLS)
        zero = jnp.zeros((COLS, 128), F32)
        for a in range(3):
            hi, mid = split2(comps[a])
            hi, mid = hi.astype(F32), mid.astype(F32)
            sq = squares[a].astype(F32)
            kf[:, 256 + 128 * a : 384 + 128 * a] = jnp.where(
                lane < 48, hi, jnp.where(lane < 96, mid, sq)
            ).astype(BF16)
            ones = jnp.where((lane >= 96) & (lane < 96 + H), 1.0, zero)
            kf[:, 640 + 128 * a : 768 + 128 * a] = jnp.where(lane < 48, hi, ones).astype(BF16)

    def value_features(it):
        s, f = unpack(col_recv[it])
        y = mm(s, wp_hi[:, 2 * QW :]) + mm(s, wp_mid[:, 2 * QW :])
        values = to_global(f, y, 96)
        lane = lane_iota(COLS)
        for a in range(3):
            at = 128 * a
            hi, mid = split2(jnp.where(lane < 96, values[a], y[:, at : at + 128]))
            vcat[0:COLS, at : at + 128] = hi
            vcat[COLS:, at : at + 128] = jnp.where(lane < 96, mid.astype(F32), 0.0).astype(BF16)
        vcat[0:COLS, 384:512] = y[:, 384:512].astype(BF16)
        vcat[COLS:, 384:512] = jnp.zeros((COLS, 128), BF16)

    def prepare_pair():
        copies[2].wait()
        fq = unpack(row_recv[0])[1]
        idx_b[0:ROWS] = column(fq, 12)
        idx_b[ROWS:] = column(fq, 13)
        key_index = key_idx[...]
        shape = (COLS, 128)
        lane = lax.broadcasted_iota(jnp.int32, shape, 1).astype(F32) - 64.0
        same = lax.broadcasted_iota(jnp.int32, shape, 0) == lax.broadcasted_iota(jnp.int32, shape, 1)
        table = relpos[...].astype(F32)
        hi, mid = split2(table - jnp.mean(table, axis=-1, keepdims=True))
        centre[0:128] = jnp.where(same, 1.0 - 1.0 / 128.0, -1.0 / 128.0).astype(BF16)
        centre[128:256] = hi
        centre[256:384] = mid
        wb_s[...] = jnp.zeros_like(wb_s)
        wb_s[0:H] = wb_in[...].astype(F32)
        project = wb_s[...].astype(BF16)
        gains = gain[...]
        step = 8

        def prepare(k, carry):
            first = k * step
            centres = []
            for u in range(step):
                offset = jnp.clip(key_index - idx_b[pl.ds(first + u, 1), :], -64.0, 63.0)
                onehot = jnp.where(offset == lane, 1.0, 0.0).astype(BF16)
                both = jnp.concatenate([pair_v[first + u], onehot, onehot], axis=1)
                centres.append(mm(both, centre[...]))
            normed = []
            for u in range(step):
                spread = jnp.mean(centres[u] * centres[u], axis=-1, keepdims=True)
                normed.append((centres[u] * lax.rsqrt(spread + NORM_EPSILON) * gains).astype(BF16))
                pair_v[first + u] = normed[u]
            for u in range(0, step, 2):
                two = jnp.concatenate(normed[u : u + 2], axis=0)
                bias = lax.dot_general(
                    project, two, (((1,), (1,)), ((), ())), preferred_element_type=F32
                )
                for v in range(2):
                    live = idx_b[pl.ds(ROWS + first + u + v, 1), :] > 0.5
                    at = pl.multiple_of((first + u + v) * HP, HP)
                    bias_v[pl.ds(at, HP), :] = jnp.where(
                        live, bias[:, 128 * v : 128 * v + 128] * THIRD, DEAD
                    )
            return carry

        lax.fori_loop(0, ROWS // step, prepare, 0)

    def mask_keys():
        live = unpack(col_recv[0])[1].T[13:14, :] > 0.5
        for k in range(4):
            part = pl.ds(k * 256, 256)
            bias_v[part, :] = jnp.where(live, bias_v[part, :], DEAD)

    def store_queries(ref, first, rows):
        for k in range(rows.shape[0] // HP):
            ref[pl.ds((first + k) * PITCH, HP), :] = rows[HP * k : HP * k + HP]

    def attend(it):
        with jax.named_scope("logits"):
            keys = kf[...]
            rows = 256
            for k in range(ROWS * HP // rows):
                part = pl.ds(k * rows, rows)
                acc = lax.dot_general(
                    qmask[part, :], keys, (((1,), (1,)), ((), ())), preferred_element_type=F32
                )
                bias = bias_v[part, :]
                logits = jnp.where(bias > -1e38, acc * (THIRD / math.sqrt(C)) + bias, MASKED_LOGIT)
                top = jnp.max(logits, axis=-1, keepdims=True)
                p = jnp.exp(logits - top).astype(BF16)
                top = jnp.broadcast_to(top, (rows, 128))
                total = jnp.sum(p.astype(F32), axis=-1, keepdims=True)
                total = jnp.broadcast_to(total, (rows, 128))
                store_queries(m_b, k * rows // HP, top)
                store_queries(s_b, k * rows // HP, total)
                p_s[part, 0:128] = p
                p_s[part, 128:256] = p

        with jax.named_scope("pack"):
            lane = lane_iota(8)
            place = jnp.where(lane < 96, lax.rem(lane, 32), -1)
            for g in range(NC):
                tile = jnp.zeros((8, 128), F32)
                for h in range(H):
                    src = pl.ds(8 * PITCH * g + h, 8, stride=PITCH)
                    tile = jnp.where(place == h, m_b[src, :], tile)
                    tile = jnp.where(place == HP + h, s_b[src, :], tile)
                hi, mid = split2(tile)
                lo = tile - hi.astype(F32) - mid.astype(F32)
                tile = jnp.where(
                    lane < 32, hi.astype(F32), jnp.where(lane < 64, mid.astype(F32), lo)
                )
                top_send[it, g] = tile.astype(BF16)
            for peer in row_peers:
                top_copy(it, peer, c).start()
        with jax.named_scope("pairs"):
            for i in range(0, ROWS, 2):
                part = pl.ds(i * HP, 2 * HP)
                two = jnp.concatenate([pair_v[i], pair_v[i + 1]], axis=1)
                y = mm(p_s[part, 0:128], two)
                store_queries(pair_s, i, y[0:HP, 0:128])
                store_queries(pair_s, i + 1, y[HP:, 128:256])
            for h in range(H):
                pair_send[it, :, :, 128 * h : 128 * h + 128] = (
                    pair_s[pl.ds(h, ROWS, stride=PITCH), :].astype(BF16).reshape(NC, OWN, 128)
                )
            for peer in row_peers:
                pair_copy(it, peer, c).start()
        with jax.named_scope("values"):
            value_features(it)
        with jax.named_scope("sums"):
            values = vcat[...]
            for k in range(4):
                part = pl.ds(k * 256, 256)
                y = mm(p_s[part, :], values)
                for t in range(4):
                    store_queries(r_s.at[t], 16 * k, y[:, 128 * t : 128 * t + 128])
        with jax.named_scope("select"):
            for t in range(4):
                val_send[it, :, :, 128 * t : 128 * t + 128] = by_head(
                    t, ROWS, lambda h: r_s[t, pl.ds(h, ROWS, stride=PITCH), :]
                ).reshape(NC, OWN, 128)
            for peer in row_peers:
                val_copy(it, peer, c).start()
            top_recv[it, c] = top_send[it, c]
            pair_recv[it, c] = pair_send[it, c]
            val_recv[it, c] = val_send[it, c]

            @pl.when(it == 0)
            def _():
                prepare_weights()

    def by_head(t, rows, piece):
        spans = [(h, PV * h, PV) for h in range(H)] if t < 3 else []
        at, heads = (96, range(2 * t, 2 * t + 2)) if t < 3 else (0, range(6, H))
        spans += [(h, at + C * (h - heads[0]), C) for h in heads]
        lane = lane_iota(rows)
        out = jnp.zeros((rows, 128), F32)
        for h, lo, size in spans:
            out = jnp.where((lane >= lo) & (lane < lo + size), piece(h), out)
        return out

    def advance(it):
        with jax.named_scope("wait_top"):
            for peer in row_peers:
                top_copy(it, peer, peer).wait_recv()
        tops = []
        for k in range(NC):
            tile = top_recv[it, k].astype(F32)
            tops.append(tile + pltpu.roll(tile, 96, 1) + pltpu.roll(tile, 64, 1))
        top = functools.reduce(jnp.maximum, tops)
        scales = [jnp.exp(t - top) for t in tops]
        total = scales[0] * pltpu.roll(tops[0], 128 - HP, 1)
        for k in range(1, NC):
            total = total + scales[k] * pltpu.roll(tops[k], 128 - HP, 1)
        inverse = 1.0 / jnp.where(lane_iota(OWN) < H, total, 1.0)
        factor = [[column(e * inverse, h) for h in range(H)] for e in scales]
        with jax.named_scope("wait_pair"):
            for peer in row_peers:
                pair_copy(it, peer, peer).wait_recv()
        pairs = []
        for h in range(H):
            at = pl.ds(128 * h, 128)
            out = factor[0][h] * pair_recv[it, 0, :, at].astype(F32)
            for k in range(1, NC):
                out = out + factor[k][h] * pair_recv[it, k, :, at].astype(F32)
            pairs.append(out)
        mixed = dot3(jnp.concatenate(pairs, axis=1), wmix_hi[...], wmix_mid[...])
        spread = [[by_head(t, OWN, lambda h: factor[k][h]) for t in range(4)] for k in range(NC)]
        with jax.named_scope("wait_val"):
            for peer in row_peers:
                val_copy(it, peer, peer).wait_recv()
        tiles = []
        for t in range(4):
            at = pl.ds(128 * t, 128)
            out = spread[0][t] * val_recv[it, 0, :, at]
            for k in range(1, NC):
                out = out + spread[k][t] * val_recv[it, k, :, at]
            tiles.append(out)
        frames = state_f[:, D:]
        single = state_f[:, :D]
        moved = [tiles[a] - column(frames, 9 + a) for a in range(3)]
        local = [
            column(frames, a) * moved[0]
            + column(frames, 3 + a) * moved[1]
            + column(frames, 6 + a) * moved[2]
            for a in range(3)
        ]
        lengths = jnp.sqrt(
            local[0] * local[0] + local[1] * local[1] + local[2] * local[2] + NORM_FLOOR
        )
        keep = lane_iota(OWN) < H * PV
        feats = [jnp.where(keep, local[a], tiles[a]) for a in range(3)]
        feats += [tiles[3], jnp.where(keep, lengths, 0.0)]
        feats = jnp.concatenate(feats, axis=1)
        single = single + mixed + dot3(feats, wloc_hi[...], wloc_mid[...])
        single = layer_norm(single)
        hidden = jnp.maximum(dot3(single, whid_hi[...], whid_mid[...]), 0.0)
        single = layer_norm(single + dot3(hidden, wback_hi[...], wback_mid[...]))
        update = dot3(single, wfr_hi[...], wfr_mid[...])
        turn = rotation_entries(column(update, 0), column(update, 1), column(update, 2))
        rot = [column(frames, k) for k in range(9)]
        step = [column(update, 3 + k) for k in range(3)]
        new = [
            rot[3 * left] * turn[right]
            + rot[3 * left + 1] * turn[3 + right]
            + rot[3 * left + 2] * turn[6 + right]
            for left in range(3)
            for right in range(3)
        ] + [
            rot[3 * left] * step[0]
            + rot[3 * left + 1] * step[1]
            + rot[3 * left + 2] * step[2]
            + column(frames, 9 + left)
            for left in range(3)
        ]
        lane = lax.rem(lane_iota(OWN), 16)
        out = frames
        for k, value in enumerate(new):
            out = jnp.where(lane == k, value, out)
        return single, out

    def iteration(it, carry):
        with jax.named_scope("start"):
            start_exchange(it)

            @pl.when(it == 0)
            def _():
                prepare_projection()

        with jax.named_scope("wait_swap"):
            swap_copy(it).wait_recv()
        with jax.named_scope("send_col"):
            for peer in served:
                col_copy(it, peer, slot).start()
            col_recv[it, slot] = swap_recv[it]

        with jax.named_scope("wait_row"):
            for peer in row_peers:
                row_copy(it, peer, peer).wait_recv()
        with jax.named_scope("query"):

            @pl.when(it == 0)
            def _():
                send_numbers()

            query_features(it)
        with jax.named_scope("prep_pair"):

            @pl.when(it == 0)
            def _():
                key_numbers()
                prepare_pair()

        with jax.named_scope("wait_col"):
            for peer in served:
                col_copy(it, peer, slot_of(peer)).wait_recv()
            for k in (0, 1):
                far_copy(it, k, k * 8 + far_sources[k][1]).wait_recv()
        with jax.named_scope("key"):
            key_features(it)

            @pl.when(it == 0)
            def _():
                mask_keys()

        attend(it)
        with jax.named_scope("advance"):
            single, frames = advance(it)

            @pl.when(it < ITERS - 1)
            def _():
                send_buf[it + 1] = pack(single, frames)
                state_f[:, 0:D] = single
                state_f[:, D:] = frames

            @pl.when(it == ITERS - 1)
            def _():
                single_out[...] = single
                frames_out[...] = frames[:, 0:12]

        with jax.named_scope("wait_send"):
            swap_copy(it).wait_send()
            for peer in row_peers:
                row_copy(it, peer, c).wait_send()
                top_copy(it, peer, c).wait_send()
                pair_copy(it, peer, c).wait_send()
                val_copy(it, peer, c).wait_send()
            for peer in served:
                col_copy(it, peer, slot).wait_send()
            for k in (0, 1):
                far_copy(it, k, core * 8 + c).wait_send()
        return carry

    lax.fori_loop(0, ITERS, iteration, 0)
    for k, (needed, peer) in enumerate(idx_targets):

        @pl.when(needed)
        def _(k=k, peer=peer):
            idx_copy(peer, k, core).wait_send()


def hand_over(state, frames, state_out, frames_out):
    state_out[...] = state[...]
    frames_out[...] = frames[...]


def body(
    pair, relpos, pair_gain, bias_weight, single, rotation_params, translation, residue_index,
    residue_mask, w_scalar, w_points, head_weights, w_out, w_hidden, w_back, w_frame,
):
    vmem = pl.BlockSpec(memory_space=pltpu.VMEM)
    anyspace = pl.BlockSpec(memory_space=pl.ANY)
    V = pltpu.VMEM
    dma = pltpu.SemaphoreType.DMA
    scratch = [
        V((OWN, D), F32),
        V((3, OWN), F32),
        V((3, OWN), F32),
        V((1, OWN), jnp.int32),
        V((1, OWN), jnp.int32),
        V((1, H), F32),
        V((128, 128), BF16),
        V((1, 128), F32),
        V((H, 128), BF16),
        V((6, D), F32),
        V((ROWS, COLS, 128), BF16),
        V((ROWS * HP, 128), F32),
        V((576, D), F32),
        V((576, D), F32),
        V((2112, D), F32),
        V((D, D), F32),
        V((D, D), F32),
        V((128, D), F32),
        V((D, 2 * QW + VW), BF16),
        V((D, 2 * QW + VW), BF16),
        V((H * 128, D), BF16),
        V((H * 128, D), BF16),
        V((QW, D), BF16),
        V((QW, D), BF16),
        V((D, D), BF16),
        V((D, D), BF16),
        V((D, D), BF16),
        V((D, D), BF16),
        V((D, 128), BF16),
        V((D, 128), BF16),
        V((HP, 128), F32),
        V((HP, 128), F32),
        V((1, 128), F32),
        V((HP, FW), F32),
        V((3 * 128, 128), BF16),
        V((OWN, SW), F32),
        V((ITERS, OWN, SW), BF16),
        V((ITERS, NC, OWN, SW), BF16),
        V((ITERS, OWN, SW), BF16),
        V((ITERS, NR, OWN, SW), BF16),
        V((ITERS, NC, OWN, 128), BF16),
        V((ITERS, NC, OWN, 128), BF16),
        V((ITERS, NC, OWN, H * 128), BF16),
        V((ITERS, NC, OWN, H * 128), BF16),
        V((ITERS, NC, OWN, VW), F32),
        V((ITERS, NC, OWN, VW), F32),
        V((2, NC, OWN, 128), BF16),
        V((COLS, 128), F32),
        V((ROWS, FW), F32),
        V((ROWS * HP, FW), BF16),
        V((COLS, FW), BF16),
        V((2 * COLS, VW), BF16),
        V((2 * ROWS, 128), F32),
        V((ROWS * HP, 256), BF16),
        V((ROWS * PITCH, 128), F32),
        V((ROWS * PITCH, 128), F32),
        V((4, ROWS * PITCH, 128), F32),
        V((ROWS * PITCH, 128), F32),
        dma((16,)),
        dma((NC,)),
        dma((ITERS, NC)),
        dma,
        dma((ITERS,)),
        dma((NR,)),
        dma((ITERS, NR)),
        dma((NC,)),
        dma((ITERS, NC)),
        dma((NC,)),
        dma((ITERS, NC)),
        dma((NC,)),
        dma((ITERS, NC)),
        dma((3,)),
        dma((2,)),
        dma((2,)),
    ]
    state, frames = pl.pallas_call(
        kernel,
        out_shape=(
            jax.ShapeDtypeStruct((OWN, D), F32),
            jax.ShapeDtypeStruct((OWN, 12), F32),
        ),
        in_specs=[anyspace] * 16,
        out_specs=(vmem, vmem),
        scratch_shapes=scratch,
        compiler_params=pltpu.CompilerParams(
            collective_id=0, has_side_effects=True, vmem_limit_bytes=62 * 1024 * 1024
        ),
        name="structure",
    )(
        single, rotation_params, translation, residue_index.reshape(1, OWN),
        residue_mask.reshape(1, OWN), head_weights.reshape(1, H), relpos,
        pair_gain.reshape(1, 128), bias_weight.T, w_frame.T,
        pair, w_scalar.T, w_points.T, w_out, w_hidden, w_back,
    )
    state, frames = pl.pallas_call(
        hand_over,
        out_shape=(
            jax.ShapeDtypeStruct((OWN, D), F32),
            jax.ShapeDtypeStruct((OWN, 12), F32),
        ),
        in_specs=[vmem, vmem],
        out_specs=(vmem, vmem),
        compiler_params=pltpu.CompilerParams(vmem_limit_bytes=62 * 1024 * 1024),
        name="hand_over",
    )(state, frames)
    return state, frames.T


def solution(mesh):
    placed = (
        P("row", "col", None),
        P(),
        P(),
        P(),
        P(("row", "col"), None),
        P(None, ("row", "col")),
        P(None, ("row", "col")),
        P(("row", "col")),
        P(("row", "col")),
        P(),
        P(),
        P(),
        P(),
        P(),
        P(),
        P(),
    )
    return jax.shard_map(
        body,
        mesh=mesh,
        in_specs=placed,
        out_specs=(P(("row", "col"), None), P(None, ("row", "col"))),
        check_vma=False,
    )
```

```python
import functools
import math

import jax
import jax.numpy as jnp
from jax import lax
from jax.experimental import pallas as pl
from jax.experimental.pallas import tpu as pltpu
from jax.sharding import PartitionSpec as P

H = 12
C = 16
PQ = 4
PV = 8
BINS = 128
ITERS = 3
D = 384
HP = 16
PITCH = 24
ROWS = 64
COLS = 128
OWN = 8
NR = 16
NC = 8
SW = 512
QW = 640
VW = 512
FW = 1024

NORM_EPSILON = 1e-05
MASKED_LOGIT = -100000.0
DEAD = -3e38
NORM_FLOOR = 0.1
THIRD = math.sqrt(1.0 / 3.0)
MESH = pl.DeviceIdType.MESH
F32 = jnp.float32
BF16 = jnp.bfloat16


def rotation_entries(b, c, d):
    inverse = 1.0 / (1.0 + b * b + c * c + d * d)
    entries = [
        1.0 + b * b - c * c - d * d,
        2.0 * (b * c - d),
        2.0 * (b * d + c),
        2.0 * (b * c + d),
        1.0 - b * b + c * c - d * d,
        2.0 * (c * d - b),
        2.0 * (b * d - c),
        2.0 * (c * d + b),
        1.0 - b * b - c * c + d * d,
    ]
    return [e * inverse for e in entries]


def layer_norm(values):
    center = values - jnp.mean(values, axis=-1, keepdims=True)
    spread = jnp.mean(center * center, axis=-1, keepdims=True)
    return center * lax.rsqrt(spread + NORM_EPSILON)


def split2(x):
    hi = x.astype(BF16)
    return hi, (x - hi.astype(F32)).astype(BF16)


def mm(a, b):
    return jnp.dot(a, b, preferred_element_type=F32)


def dot3(x, w_hi, w_mid):
    hi, mid = split2(x)
    n = x.shape[0]
    both = mm(jnp.concatenate([hi, mid], axis=0), w_hi)
    return both[:n] + both[n:] + mm(hi, w_mid)


def lane_iota(rows):
    return lax.broadcasted_iota(jnp.int32, (rows, 128), 1)


def pad_lanes(x):
    return jnp.concatenate([x, jnp.zeros((x.shape[0], 128 - x.shape[1]), x.dtype)], axis=1)


def column(x, k):
    return jnp.broadcast_to(x[:, k : k + 1], (x.shape[0], 128))


def kernel(
    single_hbm, rotation_hbm, translation_hbm, index_hbm, live_hbm, head_hbm, relpos_hbm, gain_hbm,
    wb_hbm, wframe_hbm, pair_hbm, wsc_hbm, wpt_hbm, wout_hbm, whid_hbm, wback_hbm,
    single_out, frames_out,
    single_in, rotation_in, translation_in, index_in, live_in, head_in, relpos, gain, wb_in, wframe,
    pair_v, bias_v, wsc_f, wpt_f, wout_f, whid_f, wback_f, wfr_f,
    wp_hi, wp_mid, wmix_hi, wmix_mid, wloc_hi, wloc_mid, whid_hi, whid_mid, wback_hi, wback_mid,
    wfr_hi, wfr_mid, wb_s, small, gamma, hmask, centre,
    state_f, send_buf, row_recv, swap_recv, col_recv, top_send, top_recv, pair_send, pair_recv,
    val_send, val_recv, idx_recv, key_idx,
    qf, qmask, kf, vcat, idx_b, p_s, m_b, s_b, r_s, pair_s,
    copy_sem, row_ss, row_rs, swap_ss, swap_rs, col_ss, col_rs, top_ss, top_rs,
    pair_ss, pair_rs, val_ss, val_rs, idx_ss, idx_rs, far_ss,
):
    r = lax.axis_index("row")
    c = lax.axis_index("col")
    core = lax.rem(r, 2)
    z = lax.rem(r // 2, 4)
    y_hi = r // 8
    x = lax.rem(c, 4)
    y_lo = c // 4
    to_row = y_lo * 8 + lax.rem(x + 2, 4) * 2 + core
    to_col = y_hi * 4 + z
    from_row = y_lo * 8 + x * 2 + core
    from_col = y_hi * 4 + lax.rem(z + 2, 4)

    far_rows = [(1 - y_lo) * 8 + x * 2 + k for k in (0, 1)]
    far_sources = [(y_lo * 8 + x * 2 + k, (1 - y_hi) * 4 + z) for k in (0, 1)]

    def slot_of(row):
        return lax.rem(row, 2) * 8 + (row // 8) * 4 + lax.rem(row // 2 + 2, 4)

    slot = slot_of(r)
    near = (r >= 2 * c - 1) & (r <= 2 * c + 2)
    diagonal = r // 2 == c

    row_peers = [
        lax.rem(y_lo + dy, 2) * 4 + lax.rem(x + dx, 4)
        for dy, dx in ((1, 2), (1, 1), (1, 3), (0, 2), (1, 0), (0, 1), (0, 3))
    ]
    col_peers = [
        lax.rem(y_hi + dy, 2) * 8 + lax.rem(z + dz, 4) * 2 + lax.rem(core + dc, 2)
        for dy, dz in ((1, 2), (1, 1), (1, 3), (1, 0), (0, 2), (0, 1), (0, 3), (0, 0))
        for dc in (0, 1)
        if (dy, dz, dc) != (0, 0, 0)
    ]
    served = col_peers[2:]

    barrier = pltpu.get_barrier_semaphore()
    for peer in col_peers:
        pl.semaphore_signal(barrier, inc=1, device_id=(peer, c), device_id_type=MESH)
    for peer in row_peers:
        pl.semaphore_signal(barrier, inc=1, device_id=(r, peer), device_id_type=MESH)
    pl.semaphore_signal(barrier, inc=1, device_id=(from_row, from_col), device_id_type=MESH)
    for peer in far_sources:
        pl.semaphore_signal(barrier, inc=1, device_id=peer, device_id_type=MESH)

    small_copies = [
        pltpu.make_async_copy(src, dst, copy_sem.at[6 + k])
        for k, (src, dst) in enumerate(
            [
                (single_hbm, single_in),
                (rotation_hbm, rotation_in),
                (translation_hbm, translation_in),
                (index_hbm, index_in),
                (live_hbm, live_in),
                (head_hbm, head_in),
                (relpos_hbm, relpos),
                (gain_hbm, gain),
                (wb_hbm, wb_in),
                (wframe_hbm, wframe),
            ]
        )
    ]
    copies = [
        pltpu.make_async_copy(src, dst, copy_sem.at[k])
        for k, (src, dst) in enumerate(
            [
                (wsc_hbm, wsc_f),
                (wpt_hbm, wpt_f),
                (pair_hbm, pair_v),
                (wout_hbm, wout_f),
                (whid_hbm, whid_f),
                (wback_hbm, wback_f),
            ]
        )
    ]
    for cp in small_copies + copies:
        cp.start()
    for cp in small_copies:
        cp.wait()

    small[...] = jnp.zeros_like(small)
    entries = rotation_entries(rotation_in[0:1], rotation_in[1:2], rotation_in[2:3])
    for k, row in enumerate(
        entries
        + [translation_in[k : k + 1] for k in range(3)]
        + [index_in[...].astype(F32), jnp.where(live_in[...] == 1, 1.0, 0.0)]
    ):
        small[k : k + 1, 0:OWN] = row
    head = head_in[...]
    positive = jnp.maximum(head, 0.0) + jnp.log1p(jnp.exp(-jnp.abs(head)))
    small[14:15, 0:H] = positive * (math.sqrt(2.0 / (9.0 * PQ)) / 2.0)
    turned = small[...].T
    state_f[:, 0:D] = single_in[...]
    state_f[:, D:] = pad_lanes(jnp.concatenate([turned[0:OWN]] * 3, axis=1))

    def pack(single, frames):
        at = lane_iota(OWN)
        hi, mid = split2(frames)
        lo = (frames - hi.astype(F32) - mid.astype(F32)).astype(BF16)
        pieces = jnp.where(
            at < 16,
            hi.astype(F32),
            jnp.where(at < 32, mid.astype(F32), jnp.where(at < 48, lo.astype(F32), 0.0)),
        )
        return jnp.concatenate([single.astype(BF16), pieces.astype(BF16)], axis=1)

    def unpack(blocks):
        rows = blocks.astype(F32).reshape(blocks.shape[0] * OWN, SW)
        f = rows[:, D:]
        f = f + pltpu.roll(f, 112, 1) + pltpu.roll(f, 96, 1)
        return rows[:, :D].astype(BF16), f

    send_buf[0] = pack(state_f[:, 0:D], state_f[:, D:])

    lane = lane_iota(HP)
    head_row = lax.broadcasted_iota(jnp.int32, (HP, 128), 0)
    low = lane < 96
    owner = jnp.where(low, lax.rem(lane, 48) // PQ, lane - 96)
    own = (owner == head_row) & (lane < 96 + H)
    spread_scale = jnp.where(own, jnp.where(low, 8.0, -4.0), 0.0)
    gamma[...] = jnp.sum(
        jnp.broadcast_to(turned[0:HP, 14:15], (HP, 128)) * spread_scale, axis=0, keepdims=True
    )
    for t in range(2):
        own_scalar = (lane + 128 * t) // C == head_row
        hmask[:, 128 * t : 128 * t + 128] = jnp.where(own_scalar & (head_row < H), 1.0, 0.0)
    for t in range(2, 8):
        hmask[:, 128 * t : 128 * t + 128] = jnp.where(own & (head_row < H), 1.0, 0.0)

    with jax.named_scope("barrier"):
        pl.semaphore_wait(barrier, NC + NR + 1)

    def row_copy(it, peer, at):
        return pltpu.make_async_remote_copy(
            src_ref=send_buf.at[it],
            dst_ref=row_recv.at[it, at],
            send_sem=row_ss.at[peer],
            recv_sem=row_rs.at[it, at],
            device_id=(r, peer),
            device_id_type=MESH,
        )

    def swap_copy(it):
        return pltpu.make_async_remote_copy(
            src_ref=send_buf.at[it],
            dst_ref=swap_recv.at[it],
            send_sem=swap_ss,
            recv_sem=swap_rs.at[it],
            device_id=(to_row, to_col),
            device_id_type=MESH,
        )

    def far_copy(it, k, at):
        return pltpu.make_async_remote_copy(
            src_ref=send_buf.at[it],
            dst_ref=col_recv.at[it, at],
            send_sem=far_ss.at[k],
            recv_sem=col_rs.at[it, at],
            device_id=(far_rows[k], to_col),
            device_id_type=MESH,
        )

    def col_copy(it, peer, at):
        return pltpu.make_async_remote_copy(
            src_ref=swap_recv.at[it],
            dst_ref=col_recv.at[it, at],
            send_sem=col_ss.at[peer],
            recv_sem=col_rs.at[it, at],
            device_id=(peer, c),
            device_id_type=MESH,
        )

    def idx_copy(peer, k, at):
        return pltpu.make_async_remote_copy(
            src_ref=row_recv.at[0, :, :, D:SW],
            dst_ref=idx_recv.at[at],
            send_sem=idx_ss.at[k],
            recv_sem=idx_rs.at[at],
            device_id=(peer, c),
            device_id_type=MESH,
        )

    idx_targets = (
        (diagonal, r + 1 - 2 * core),
        (diagonal & (c > 0), lax.rem(2 * c + 15, 16)),
        (diagonal & (c < NC - 1), lax.rem(2 * c + 2, 16)),
    )

    def send_numbers():
        for k, (needed, peer) in enumerate(idx_targets):

            @pl.when(needed)
            def _(k=k, peer=peer):
                idx_copy(peer, k, core).start()

        @pl.when(diagonal)
        def _():
            idx_recv[core] = row_recv[0, :, :, D:SW]

    def key_numbers():
        @pl.when(diagonal)
        def _():
            idx_copy(r, 0, 1 - core).wait_recv()

        @pl.when(near & jnp.logical_not(diagonal))
        def _():
            idx_copy(r, 0, 0).wait_recv()
            idx_copy(r, 0, 1).wait_recv()

        @pl.when(near)
        def _():
            f = idx_recv[...].astype(F32).reshape(COLS, 128)
            f = f + pltpu.roll(f, 112, 1) + pltpu.roll(f, 96, 1)
            key_idx[...] = column(f, 12)

        @pl.when(jnp.logical_not(near) & (c > r // 2))
        def _():
            key_idx[...] = jnp.full((COLS, 128), 1e6, F32)

        @pl.when(jnp.logical_not(near) & (c < r // 2))
        def _():
            key_idx[...] = jnp.full((COLS, 128), -1e6, F32)

    def top_copy(it, peer, at):
        return pltpu.make_async_remote_copy(
            src_ref=top_send.at[it, peer],
            dst_ref=top_recv.at[it, at],
            send_sem=top_ss.at[peer],
            recv_sem=top_rs.at[it, at],
            device_id=(r, peer),
            device_id_type=MESH,
        )

    def pair_copy(it, peer, at):
        return pltpu.make_async_remote_copy(
            src_ref=pair_send.at[it, peer],
            dst_ref=pair_recv.at[it, at],
            send_sem=pair_ss.at[peer],
            recv_sem=pair_rs.at[it, at],
            device_id=(r, peer),
            device_id_type=MESH,
        )

    def val_copy(it, peer, at):
        return pltpu.make_async_remote_copy(
            src_ref=val_send.at[it, peer],
            dst_ref=val_recv.at[it, at],
            send_sem=val_ss.at[peer],
            recv_sem=val_rs.at[it, at],
            device_id=(r, peer),
            device_id_type=MESH,
        )

    def start_exchange(it):
        swap_copy(it).start()
        for k in (0, 1):
            far_copy(it, k, core * 8 + c).start()
        for peer in row_peers:
            row_copy(it, peer, c).start()
        row_recv[it, c] = send_buf[it]

    def prepare_projection():
        for cp in copies[:2]:
            cp.wait()
        zeros64 = jnp.zeros((64, D), F32)
        zeros32 = jnp.zeros((32, D), F32)

        def place(block, rows):
            hi, mid = split2(rows.T)
            wp_hi[:, 128 * block : 128 * block + 128] = hi
            wp_mid[:, 128 * block : 128 * block + 128] = mid

        for g in range(2):
            at = g * H * C
            place(5 * g, wsc_f[at : at + 128])
            place(5 * g + 1, jnp.concatenate([wsc_f[at + 128 : at + 192], zeros64], axis=0))
            for a in range(3):
                first = g * 144 + 48 * a
                part = wpt_f[first : first + 48]
                place(5 * g + 2 + a, jnp.concatenate([part, part, zeros32], axis=0))
        at = 2 * H * C
        for a in range(3):
            part = wsc_f[at + 32 * a : at + 32 * a + 32]
            place(10 + a, jnp.concatenate([wpt_f[288 + 96 * a : 384 + 96 * a], part], axis=0))
        place(13, jnp.concatenate([wsc_f[at + 96 : at + 192], zeros32], axis=0))

    def prepare_weights():
        for cp in copies[3:]:
            cp.wait()
        zeros32 = jnp.zeros((32, D), BF16)
        for part, (dst_mix, dst_loc) in enumerate(((wmix_hi, wloc_hi), (wmix_mid, wloc_mid))):
            for k in range(4):
                dst_mix[384 * k : 384 * k + 384] = split2(wout_f[576 + 384 * k : 960 + 384 * k])[
                    part
                ]
            for k in range(3):
                dst_loc[128 * k : 128 * k + 96] = split2(wout_f[192 + 96 * k : 288 + 96 * k])[part]
                dst_loc[128 * k + 96 : 128 * k + 128] = split2(wout_f[32 * k : 32 * k + 32])[part]
            dst_loc[384:480] = split2(wout_f[96:192])[part]
            dst_loc[480:512] = zeros32
            dst_loc[512:608] = split2(wout_f[480:576])[part]
            dst_loc[608:640] = zeros32
        whid_hi[...], whid_mid[...] = split2(whid_f[...])
        wback_hi[...], wback_mid[...] = split2(wback_f[...])
        wfr_f[...] = jnp.zeros_like(wfr_f)
        wfr_f[0:6] = wframe[...]
        wfr_hi[...], wfr_mid[...] = split2(wfr_f[...].T)

    def to_global(f, y, width):
        comps = []
        x = [y[:, 128 * b : 128 * b + 128] for b in range(3)]
        keep = lane_iota(f.shape[0]) < width
        for a in range(3):
            g = (
                column(f, 3 * a) * x[0]
                + column(f, 3 * a + 1) * x[1]
                + column(f, 3 * a + 2) * x[2]
                + column(f, 9 + a)
            )
            comps.append(jnp.where(keep, g, 0.0))
        return comps

    def square_terms(comps):
        sq = comps[0] * comps[0] + comps[1] * comps[1] + comps[2] * comps[2]
        f = lax.broadcasted_iota(jnp.int32, (128, 128), 0)
        n = lax.broadcasted_iota(jnp.int32, (128, 128), 1)
        pick = jnp.where((f < 48) & (n == 96 + f // PQ), 1.0, 0.0).astype(BF16)
        hi, mid = split2(sq)
        lo = (sq - hi.astype(F32) - mid.astype(F32)).astype(BF16)
        total = (mm(hi, pick) + mm(mid, pick) + mm(lo, pick)) * gamma[...]
        hi, mid = split2(total)
        lo = (total - hi.astype(F32) - mid.astype(F32)).astype(BF16)
        return hi, mid, lo

    def query_features(it):
        s, f = unpack(row_recv[it])
        y = mm(s, wp_hi[:, :QW]) + mm(s, wp_mid[:, :QW])
        qf[:, 0:256] = y[:, :256]
        comps = to_global(f, y[:, 256:], 96)
        squares = square_terms(comps)
        lane = lane_iota(ROWS)
        for a in range(3):
            hi, mid = split2(comps[a] * gamma[...])
            ones = jnp.where(lane < 96 + H, 1.0, 0.0)
            qf[:, 256 + 128 * a : 384 + 128 * a] = jnp.where(lane < 96, hi.astype(F32), ones)
            qf[:, 640 + 128 * a : 768 + 128 * a] = jnp.where(
                lane < 48, mid.astype(F32), jnp.where(lane < 96, 0.0, squares[a].astype(F32))
            )

        mask = hmask[...]

        def spread(k, carry):
            for u in range(4):
                i = k * 4 + u
                row = jnp.broadcast_to(qf[pl.ds(i, 1), :], (HP, FW))
                at = pl.multiple_of(i * HP, HP)
                qmask[pl.ds(at, HP), :] = (row * mask).astype(BF16)
            return carry

        lax.fori_loop(0, ROWS // 4, spread, 0)

    def key_features(it):
        s, f = unpack(col_recv[it])
        y = mm(s, wp_hi[:, QW : 2 * QW]) + mm(s, wp_mid[:, QW : 2 * QW])
        kf[:, 0:256] = y[:, :256].astype(BF16)
        comps = to_global(f, y[:, 256:QW], 96)
        squares = square_terms(comps)
        lane = lane_iota(COLS)
        zero = jnp.zeros((COLS, 128), F32)
        for a in range(3):
            hi, mid = split2(comps[a])
            hi, mid = hi.astype(F32), mid.astype(F32)
            sq = squares[a].astype(F32)
            kf[:, 256 + 128 * a : 384 + 128 * a] = jnp.where(
                lane < 48, hi, jnp.where(lane < 96, mid, sq)
            ).astype(BF16)
            ones = jnp.where((lane >= 96) & (lane < 96 + H), 1.0, zero)
            kf[:, 640 + 128 * a : 768 + 128 * a] = jnp.where(lane < 48, hi, ones).astype(BF16)

    def value_features(it):
        s, f = unpack(col_recv[it])
        y = mm(s, wp_hi[:, 2 * QW :]) + mm(s, wp_mid[:, 2 * QW :])
        values = to_global(f, y, 96)
        lane = lane_iota(COLS)
        for a in range(3):
            at = 128 * a
            hi, mid = split2(jnp.where(lane < 96, values[a], y[:, at : at + 128]))
            vcat[0:COLS, at : at + 128] = hi
            vcat[COLS:, at : at + 128] = jnp.where(lane < 96, mid.astype(F32), 0.0).astype(BF16)
        vcat[0:COLS, 384:512] = y[:, 384:512].astype(BF16)
        vcat[COLS:, 384:512] = jnp.zeros((COLS, 128), BF16)

    def prepare_pair():
        copies[2].wait()
        fq = unpack(row_recv[0])[1]
        idx_b[0:ROWS] = column(fq, 12)
        idx_b[ROWS:] = column(fq, 13)
        key_index = key_idx[...]
        shape = (COLS, 128)
        lane = lax.broadcasted_iota(jnp.int32, shape, 1).astype(F32) - 64.0
        same = lax.broadcasted_iota(jnp.int32, shape, 0) == lax.broadcasted_iota(jnp.int32, shape, 1)
        table = relpos[...].astype(F32)
        hi, mid = split2(table - jnp.mean(table, axis=-1, keepdims=True))
        centre[0:128] = jnp.where(same, 1.0 - 1.0 / 128.0, -1.0 / 128.0).astype(BF16)
        centre[128:256] = hi
        centre[256:384] = mid
        wb_s[...] = jnp.zeros_like(wb_s)
        wb_s[0:H] = wb_in[...].astype(F32)
        project = wb_s[...].astype(BF16)
        gains = gain[...]
        step = 16

        def prepare(k, carry):
            first = k * step
            centres = []
            for u in range(step):
                offset = jnp.clip(key_index - idx_b[pl.ds(first + u, 1), :], -64.0, 63.0)
                onehot = jnp.where(offset == lane, 1.0, 0.0).astype(BF16)
                both = jnp.concatenate([pair_v[first + u], onehot, onehot], axis=1)
                centres.append(mm(both, centre[...]))
            normed = []
            for u in range(step):
                spread = jnp.mean(centres[u] * centres[u], axis=-1, keepdims=True)
                normed.append((centres[u] * lax.rsqrt(spread + NORM_EPSILON) * gains).astype(BF16))
                pair_v[first + u] = normed[u]
            for u in range(0, step, 2):
                two = jnp.concatenate(normed[u : u + 2], axis=0)
                bias = lax.dot_general(
                    project, two, (((1,), (1,)), ((), ())), preferred_element_type=F32
                )
                for v in range(2):
                    live = idx_b[pl.ds(ROWS + first + u + v, 1), :] > 0.5
                    at = pl.multiple_of((first + u + v) * HP, HP)
                    bias_v[pl.ds(at, HP), :] = jnp.where(
                        live, bias[:, 128 * v : 128 * v + 128] * THIRD, DEAD
                    )
            return carry

        lax.fori_loop(0, ROWS // step, prepare, 0)

    def mask_keys():
        live = unpack(col_recv[0])[1].T[13:14, :] > 0.5
        for k in range(4):
            part = pl.ds(k * 256, 256)
            bias_v[part, :] = jnp.where(live, bias_v[part, :], DEAD)

    def store_queries(ref, first, rows):
        for k in range(rows.shape[0] // HP):
            ref[pl.ds((first + k) * PITCH, HP), :] = rows[HP * k : HP * k + HP]

    def attend(it):
        with jax.named_scope("logits"):
            keys = kf[...]
            rows = 256
            for k in range(ROWS * HP // rows):
                part = pl.ds(k * rows, rows)
                acc = lax.dot_general(
                    qmask[part, :], keys, (((1,), (1,)), ((), ())), preferred_element_type=F32
                )
                bias = bias_v[part, :]
                logits = jnp.where(bias > -1e38, acc * (THIRD / math.sqrt(C)) + bias, MASKED_LOGIT)
                top = jnp.max(logits, axis=-1, keepdims=True)
                p = jnp.exp(logits - top).astype(BF16)
                top = jnp.broadcast_to(top, (rows, 128))
                total = jnp.sum(p.astype(F32), axis=-1, keepdims=True)
                total = jnp.broadcast_to(total, (rows, 128))
                store_queries(m_b, k * rows // HP, top)
                store_queries(s_b, k * rows // HP, total)
                p_s[part, 0:128] = p
                p_s[part, 128:256] = p

        with jax.named_scope("pack"):
            lane = lane_iota(8)
            place = jnp.where(lane < 96, lax.rem(lane, 32), -1)
            for g in range(NC):
                tile = jnp.zeros((8, 128), F32)
                for h in range(H):
                    src = pl.ds(8 * PITCH * g + h, 8, stride=PITCH)
                    tile = jnp.where(place == h, m_b[src, :], tile)
                    tile = jnp.where(place == HP + h, s_b[src, :], tile)
                hi, mid = split2(tile)
                lo = tile - hi.astype(F32) - mid.astype(F32)
                tile = jnp.where(
                    lane < 32, hi.astype(F32), jnp.where(lane < 64, mid.astype(F32), lo)
                )
                top_send[it, g] = tile.astype(BF16)
            for peer in row_peers:
                top_copy(it, peer, c).start()
        with jax.named_scope("pairs"):
            for i in range(0, ROWS, 2):
                part = pl.ds(i * HP, 2 * HP)
                two = jnp.concatenate([pair_v[i], pair_v[i + 1]], axis=1)
                y = mm(p_s[part, 0:128], two)
                store_queries(pair_s, i, y[0:HP, 0:128])
                store_queries(pair_s, i + 1, y[HP:, 128:256])
            for h in range(H):
                pair_send[it, :, :, 128 * h : 128 * h + 128] = (
                    pair_s[pl.ds(h, ROWS, stride=PITCH), :].astype(BF16).reshape(NC, OWN, 128)
                )
            for peer in row_peers:
                pair_copy(it, peer, c).start()
        with jax.named_scope("values"):
            value_features(it)
        with jax.named_scope("sums"):
            values = vcat[...]
            for k in range(4):
                part = pl.ds(k * 256, 256)
                y = mm(p_s[part, :], values)
                for t in range(4):
                    store_queries(r_s.at[t], 16 * k, y[:, 128 * t : 128 * t + 128])
        with jax.named_scope("select"):
            for t in range(4):
                val_send[it, :, :, 128 * t : 128 * t + 128] = by_head(
                    t, ROWS, lambda h: r_s[t, pl.ds(h, ROWS, stride=PITCH), :]
                ).reshape(NC, OWN, 128)
            for peer in row_peers:
                val_copy(it, peer, c).start()
            top_recv[it, c] = top_send[it, c]
            pair_recv[it, c] = pair_send[it, c]
            val_recv[it, c] = val_send[it, c]

            @pl.when(it == 0)
            def _():
                prepare_weights()

    def by_head(t, rows, piece):
        spans = [(h, PV * h, PV) for h in range(H)] if t < 3 else []
        at, heads = (96, range(2 * t, 2 * t + 2)) if t < 3 else (0, range(6, H))
        spans += [(h, at + C * (h - heads[0]), C) for h in heads]
        lane = lane_iota(rows)
        out = jnp.zeros((rows, 128), F32)
        for h, lo, size in spans:
            out = jnp.where((lane >= lo) & (lane < lo + size), piece(h), out)
        return out

    def advance(it):
        with jax.named_scope("wait_top"):
            for peer in row_peers:
                top_copy(it, peer, peer).wait_recv()
        tops = []
        for k in range(NC):
            tile = top_recv[it, k].astype(F32)
            tops.append(tile + pltpu.roll(tile, 96, 1) + pltpu.roll(tile, 64, 1))
        top = functools.reduce(jnp.maximum, tops)
        scales = [jnp.exp(t - top) for t in tops]
        total = scales[0] * pltpu.roll(tops[0], 128 - HP, 1)
        for k in range(1, NC):
            total = total + scales[k] * pltpu.roll(tops[k], 128 - HP, 1)
        inverse = 1.0 / jnp.where(lane_iota(OWN) < H, total, 1.0)
        factor = [[column(e * inverse, h) for h in range(H)] for e in scales]
        with jax.named_scope("wait_pair"):
            for peer in row_peers:
                pair_copy(it, peer, peer).wait_recv()
        pairs = []
        for h in range(H):
            at = pl.ds(128 * h, 128)
            out = factor[0][h] * pair_recv[it, 0, :, at].astype(F32)
            for k in range(1, NC):
                out = out + factor[k][h] * pair_recv[it, k, :, at].astype(F32)
            pairs.append(out)
        mixed = dot3(jnp.concatenate(pairs, axis=1), wmix_hi[...], wmix_mid[...])
        spread = [[by_head(t, OWN, lambda h: factor[k][h]) for t in range(4)] for k in range(NC)]
        with jax.named_scope("wait_val"):
            for peer in row_peers:
                val_copy(it, peer, peer).wait_recv()
        tiles = []
        for t in range(4):
            at = pl.ds(128 * t, 128)
            out = spread[0][t] * val_recv[it, 0, :, at]
            for k in range(1, NC):
                out = out + spread[k][t] * val_recv[it, k, :, at]
            tiles.append(out)
        frames = state_f[:, D:]
        single = state_f[:, :D]
        moved = [tiles[a] - column(frames, 9 + a) for a in range(3)]
        local = [
            column(frames, a) * moved[0]
            + column(frames, 3 + a) * moved[1]
            + column(frames, 6 + a) * moved[2]
            for a in range(3)
        ]
        lengths = jnp.sqrt(
            local[0] * local[0] + local[1] * local[1] + local[2] * local[2] + NORM_FLOOR
        )
        keep = lane_iota(OWN) < H * PV
        feats = [jnp.where(keep, local[a], tiles[a]) for a in range(3)]
        feats += [tiles[3], jnp.where(keep, lengths, 0.0)]
        feats = jnp.concatenate(feats, axis=1)
        single = single + mixed + dot3(feats, wloc_hi[...], wloc_mid[...])
        single = layer_norm(single)
        hidden = jnp.maximum(dot3(single, whid_hi[...], whid_mid[...]), 0.0)
        single = layer_norm(single + dot3(hidden, wback_hi[...], wback_mid[...]))
        update = dot3(single, wfr_hi[...], wfr_mid[...])
        turn = rotation_entries(column(update, 0), column(update, 1), column(update, 2))
        rot = [column(frames, k) for k in range(9)]
        step = [column(update, 3 + k) for k in range(3)]
        new = [
            rot[3 * left] * turn[right]
            + rot[3 * left + 1] * turn[3 + right]
            + rot[3 * left + 2] * turn[6 + right]
            for left in range(3)
            for right in range(3)
        ] + [
            rot[3 * left] * step[0]
            + rot[3 * left + 1] * step[1]
            + rot[3 * left + 2] * step[2]
            + column(frames, 9 + left)
            for left in range(3)
        ]
        lane = lax.rem(lane_iota(OWN), 16)
        out = frames
        for k, value in enumerate(new):
            out = jnp.where(lane == k, value, out)
        return single, out

    def iteration(it, carry):
        with jax.named_scope("start"):
            start_exchange(it)

            @pl.when(it == 0)
            def _():
                prepare_projection()

        with jax.named_scope("wait_swap"):
            swap_copy(it).wait_recv()
        with jax.named_scope("send_col"):
            for peer in served:
                col_copy(it, peer, slot).start()
            col_recv[it, slot] = swap_recv[it]

        with jax.named_scope("wait_row"):
            for peer in row_peers:
                row_copy(it, peer, peer).wait_recv()
        with jax.named_scope("query"):

            @pl.when(it == 0)
            def _():
                send_numbers()

            query_features(it)
        with jax.named_scope("prep_pair"):

            @pl.when(it == 0)
            def _():
                key_numbers()
                prepare_pair()

        with jax.named_scope("wait_col"):
            for peer in served:
                col_copy(it, peer, slot_of(peer)).wait_recv()
            for k in (0, 1):
                far_copy(it, k, k * 8 + far_sources[k][1]).wait_recv()
        with jax.named_scope("key"):
            key_features(it)

            @pl.when(it == 0)
            def _():
                mask_keys()

        attend(it)
        with jax.named_scope("advance"):
            single, frames = advance(it)

            @pl.when(it < ITERS - 1)
            def _():
                send_buf[it + 1] = pack(single, frames)
                state_f[:, 0:D] = single
                state_f[:, D:] = frames

            @pl.when(it == ITERS - 1)
            def _():
                single_out[...] = single
                frames_out[...] = frames[:, 0:12]

        with jax.named_scope("wait_send"):
            swap_copy(it).wait_send()
            for peer in row_peers:
                row_copy(it, peer, c).wait_send()
                top_copy(it, peer, c).wait_send()
                pair_copy(it, peer, c).wait_send()
                val_copy(it, peer, c).wait_send()
            for peer in served:
                col_copy(it, peer, slot).wait_send()
            for k in (0, 1):
                far_copy(it, k, core * 8 + c).wait_send()
        return carry

    lax.fori_loop(0, ITERS, iteration, 0)
    for k, (needed, peer) in enumerate(idx_targets):

        @pl.when(needed)
        def _(k=k, peer=peer):
            idx_copy(peer, k, core).wait_send()


def hand_over(state, frames, state_out, frames_out):
    state_out[...] = state[...]
    frames_out[...] = frames[...]


def body(
    pair, relpos, pair_gain, bias_weight, single, rotation_params, translation, residue_index,
    residue_mask, w_scalar, w_points, head_weights, w_out, w_hidden, w_back, w_frame,
):
    vmem = pl.BlockSpec(memory_space=pltpu.VMEM)
    anyspace = pl.BlockSpec(memory_space=pl.ANY)
    V = pltpu.VMEM
    dma = pltpu.SemaphoreType.DMA
    scratch = [
        V((OWN, D), F32),
        V((3, OWN), F32),
        V((3, OWN), F32),
        V((1, OWN), jnp.int32),
        V((1, OWN), jnp.int32),
        V((1, H), F32),
        V((128, 128), BF16),
        V((1, 128), F32),
        V((H, 128), BF16),
        V((6, D), F32),
        V((ROWS, COLS, 128), BF16),
        V((ROWS * HP, 128), F32),
        V((576, D), F32),
        V((576, D), F32),
        V((2112, D), F32),
        V((D, D), F32),
        V((D, D), F32),
        V((128, D), F32),
        V((D, 2 * QW + VW), BF16),
        V((D, 2 * QW + VW), BF16),
        V((H * 128, D), BF16),
        V((H * 128, D), BF16),
        V((QW, D), BF16),
        V((QW, D), BF16),
        V((D, D), BF16),
        V((D, D), BF16),
        V((D, D), BF16),
        V((D, D), BF16),
        V((D, 128), BF16),
        V((D, 128), BF16),
        V((HP, 128), F32),
        V((HP, 128), F32),
        V((1, 128), F32),
        V((HP, FW), F32),
        V((3 * 128, 128), BF16),
        V((OWN, SW), F32),
        V((ITERS, OWN, SW), BF16),
        V((ITERS, NC, OWN, SW), BF16),
        V((ITERS, OWN, SW), BF16),
        V((ITERS, NR, OWN, SW), BF16),
        V((ITERS, NC, OWN, 128), BF16),
        V((ITERS, NC, OWN, 128), BF16),
        V((ITERS, NC, OWN, H * 128), BF16),
        V((ITERS, NC, OWN, H * 128), BF16),
        V((ITERS, NC, OWN, VW), F32),
        V((ITERS, NC, OWN, VW), F32),
        V((2, NC, OWN, 128), BF16),
        V((COLS, 128), F32),
        V((ROWS, FW), F32),
        V((ROWS * HP, FW), BF16),
        V((COLS, FW), BF16),
        V((2 * COLS, VW), BF16),
        V((2 * ROWS, 128), F32),
        V((ROWS * HP, 256), BF16),
        V((ROWS * PITCH, 128), F32),
        V((ROWS * PITCH, 128), F32),
        V((4, ROWS * PITCH, 128), F32),
        V((ROWS * PITCH, 128), F32),
        dma((16,)),
        dma((NC,)),
        dma((ITERS, NC)),
        dma,
        dma((ITERS,)),
        dma((NR,)),
        dma((ITERS, NR)),
        dma((NC,)),
        dma((ITERS, NC)),
        dma((NC,)),
        dma((ITERS, NC)),
        dma((NC,)),
        dma((ITERS, NC)),
        dma((3,)),
        dma((2,)),
        dma((2,)),
    ]
    state, frames = pl.pallas_call(
        kernel,
        out_shape=(
            jax.ShapeDtypeStruct((OWN, D), F32),
            jax.ShapeDtypeStruct((OWN, 12), F32),
        ),
        in_specs=[anyspace] * 16,
        out_specs=(vmem, vmem),
        scratch_shapes=scratch,
        compiler_params=pltpu.CompilerParams(
            collective_id=0, has_side_effects=True, vmem_limit_bytes=62 * 1024 * 1024
        ),
        name="structure",
    )(
        single, rotation_params, translation, residue_index.reshape(1, OWN),
        residue_mask.reshape(1, OWN), head_weights.reshape(1, H), relpos,
        pair_gain.reshape(1, 128), bias_weight.T, w_frame.T,
        pair, w_scalar.T, w_points.T, w_out, w_hidden, w_back,
    )
    state, frames = pl.pallas_call(
        hand_over,
        out_shape=(
            jax.ShapeDtypeStruct((OWN, D), F32),
            jax.ShapeDtypeStruct((OWN, 12), F32),
        ),
        in_specs=[vmem, vmem],
        out_specs=(vmem, vmem),
        compiler_params=pltpu.CompilerParams(vmem_limit_bytes=62 * 1024 * 1024),
        name="hand_over",
    )(state, frames)
    return state, frames.T


def solution(mesh):
    placed = (
        P("row", "col", None),
        P(),
        P(),
        P(),
        P(("row", "col"), None),
        P(None, ("row", "col")),
        P(None, ("row", "col")),
        P(("row", "col")),
        P(("row", "col")),
        P(),
        P(),
        P(),
        P(),
        P(),
        P(),
        P(),
    )
    return jax.shard_map(
        body,
        mesh=mesh,
        in_specs=placed,
        out_specs=(P(("row", "col"), None), P(None, ("row", "col"))),
        check_vma=False,
    )
```
